16 devices in a mesh: data: 16 (over z, y, x, core).
Axes of the slice: x: 2, y: 2, z: 2, core: 2. Of those that a mesh axis runs over, the one named last changes fastest.
Arguments:
- x_in: bfloat16 [16, 8, 256, 2304], P('data')
- dy_out: bfloat16 [16, 8, 256, 2304], P('data')
- w_up: bfloat16 [1, 2304, 9216], P(None, 'data')
- w_down: bfloat16 [1, 9216, 2304], P(None, 'data')
Outputs:
- output 1: bfloat16 [1, 2304, 9216], P(None, 'data')
- output 2: bfloat16 [1, 9216, 2304], P(None, 'data')
- output 3: bfloat16 [16, 8, 256, 2304], P('data')
All inputs are finite; a program needn't handle non-finite values.
Results may differ from the reference program's by a relative error of at most 0.0128372.
Values are sent between devices in bfloat16 or wider.
A program may use at most 1 GiB of HBM per device.

```python
import jax
import jax.numpy as jnp
from jax import lax

D = 2304
FF = 9216
LAYERS = 1
BATCH = 8
SEQ = 256
MBS = 16


def setup_inputs(seed: int = 0) -> dict:
    key = jax.random.key(seed)
    key_x, key_dy, key_up, key_down = jax.random.split(key, 4)
    x_in = jax.random.normal(key_x, (MBS, BATCH, SEQ, D), jnp.float32).astype(jnp.bfloat16)
    dy_out = jax.random.normal(key_dy, (MBS, BATCH, SEQ, D), jnp.float32).astype(jnp.bfloat16)
    w_up = (jax.random.normal(key_up, (LAYERS, D, FF), jnp.float32) * D ** -0.5).astype(jnp.bfloat16)
    w_down = (jax.random.normal(key_down, (LAYERS, FF, D), jnp.float32) * (FF * LAYERS) ** -0.5).astype(jnp.bfloat16)
    return {"x_in": x_in, "dy_out": dy_out, "w_up": w_up, "w_down": w_down}


def gelu_fn(pre_act):
    return jax.nn.gelu(pre_act, approximate=True)


def micro_grads(w_up, w_down, x_blk, dy_blk):
    def fwd_layer(h_cur, weights):
        w_one, w_two = weights
        u_pre = jnp.dot(h_cur, w_one, preferred_element_type=jnp.float32).astype(jnp.bfloat16)
        a_act = gelu_fn(u_pre.astype(jnp.float32)).astype(jnp.bfloat16)
        h_next = (h_cur.astype(jnp.float32) + jnp.dot(a_act, w_two, preferred_element_type=jnp.float32)).astype(jnp.bfloat16)
        return h_next, (h_cur, u_pre, a_act)

    _, saved_acts = lax.scan(fwd_layer, x_blk, (w_up, w_down))

    def bwd_layer(g_cur, stacked):
        h_cur, u_pre, a_act, w_one, w_two = stacked
        d_two = jnp.dot(a_act.T, g_cur, preferred_element_type=jnp.float32)
        da_act = jnp.dot(g_cur, w_two.T, preferred_element_type=jnp.float32)
        _, gelu_back = jax.vjp(gelu_fn, u_pre.astype(jnp.float32))
        du_pre = gelu_back(da_act)[0].astype(jnp.bfloat16)
        d_one = jnp.dot(h_cur.T, du_pre, preferred_element_type=jnp.float32)
        g_next = (g_cur.astype(jnp.float32) + jnp.dot(du_pre, w_one.T, preferred_element_type=jnp.float32)).astype(jnp.bfloat16)
        return g_next, (d_one, d_two)

    h_all, u_all, a_all = saved_acts
    dx_blk, (d_up, d_down) = lax.scan(bwd_layer, dy_blk, (h_all, u_all, a_all, w_up, w_down), reverse=True)
    return dx_blk, d_up, d_down


def reference(x_in, dy_out, w_up, w_down):
    x_blocks = x_in.reshape(MBS, BATCH * SEQ, D)
    dy_blocks = dy_out.reshape(MBS, BATCH * SEQ, D)

    def micro_step(acc_pair, blk_pair):
        acc_up, acc_down = acc_pair
        dx_blk, d_up, d_down = micro_grads(w_up, w_down, blk_pair[0], blk_pair[1])
        return (acc_up + d_up, acc_down + d_down), dx_blk

    acc_init = (jnp.zeros((LAYERS, D, FF), jnp.float32), jnp.zeros((LAYERS, FF, D), jnp.float32))
    (acc_up, acc_down), dx_blocks = lax.scan(micro_step, acc_init, (x_blocks, dy_blocks))
    return acc_up.astype(jnp.bfloat16), acc_down.astype(jnp.bfloat16), dx_blocks.reshape(MBS, BATCH, SEQ, D)
```

```python
import functools
import math

import jax
import jax.numpy as jnp
from jax import lax
from jax.experimental import pallas as pl
from jax.experimental.pallas import tpu as pltpu
from jax.sharding import PartitionSpec as P

MESH = pl.DeviceIdType.MESH
F32, BF16 = jnp.float32, jnp.bfloat16
CHIPS, COLOURS, CORES = 8, 3, 2
DX_TILES = 8
UP_TILES = 8


def copy(src, dst, sem):
    return pltpu.make_async_copy(src, dst, sem)


def wait_for(ref, sem):
    pltpu.make_async_copy(ref, ref, sem).wait()


def gelu_both(u):
    scale = math.sqrt(2.0 / math.pi)
    square = u * u
    th = jnp.tanh(scale * (u + 0.044715 * (square * u)))
    cdf = 0.5 * (1.0 + th)
    slope = cdf + (0.5 * u) * (1.0 - th * th) * (scale * (1.0 + 0.134145 * square))
    return u * cdf, slope


def kernel(nc, x_hbm, dy_hbm, up_hbm, down_hbm,
           gup_hbm, gdown_hbm, dx_hbm,
           xr_hbm, dyr_hbm, upr_hbm, a1, a2, p1, p2, ra1, ra2, rb1, rb2, rc1, rc2, du_hbm, dxr_hbm,
           ag_send, ag_recv, rs_send, rs_recv, pair_send, pair_recv, dx_send, dx_recv, gup_send, gup_recv, local):
    me = lax.axis_index("data")
    core = me % 2
    bits = [(me // 2) % 2, (me // 4) % 2, (me // 8) % 2]
    partner = me + 1 - 2 * core
    near = [me + (2 << d) * (1 - 2 * bits[d]) for d in range(3)]

    tokens, width = x_hbm.shape
    both = 2 * tokens
    rows = a1.shape[3]
    fc = a1.shape[4]
    units = a2.shape[3]
    cols = a2.shape[4]
    half = up_hbm.shape[2]

    def chip(colour, m, order):
        total = 0
        for i in range(3):
            d = (colour + i) % 3
            flipped = (m >> order[i]) & 1
            total = total + (1 << d) * ((1 - bits[d]) if flipped else bits[d])
        return total

    GATHER, REDUCE = (0, 1, 2), (2, 1, 0)

    def up_rows(colour, m, order):
        return pl.ds(pl.multiple_of(chip(colour, m, order) * (3 * rows) + colour * rows, 16), rows)

    def down_rows(colour, m, order):
        return pl.ds(pl.multiple_of(chip(colour, m, order) * units, 16), units)

    def down_cols(colour):
        return pl.ds(colour * cols, cols)

    def ag_start(n, s):
        have = 1 << s
        for k in range(COLOURS):
            for buf in (a1, a2):
                pltpu.make_async_remote_copy(
                    src_ref=buf.at[n, k, pl.ds(0, have)], dst_ref=buf.at[n, k, pl.ds(have, have)],
                    send_sem=ag_send.at[s, n], recv_sem=ag_recv.at[s, n],
                    device_id=(near[(k + s) % 3],), device_id_type=MESH).start()

    sized = (rb1, ra1, p1)

    def ag_wait(n, s):
        wait_for(sized[s].at[n], ag_recv.at[s, n])

    def rs_start(n, s, k, src1, src2):
        dst1, dst2 = ((ra1, ra2), (rb1, rb2), (rc1, rc2))[s]
        for src, dst in ((src1, dst1), (src2, dst2)):
            pltpu.make_async_remote_copy(
                src_ref=src, dst_ref=dst.at[n, k], send_sem=rs_send.at[s, n], recv_sem=rs_recv.at[s, n],
                device_id=(near[(k + s) % 3],), device_id_type=MESH).start()

    def rs_wait(n, s):
        wait_for(sized[2 - s].at[n], rs_recv.at[s, n])

    barrier = pltpu.get_barrier_semaphore()
    for other in (partner, *near):
        pl.semaphore_signal(barrier, inc=1, device_id=(other,), device_id_type=MESH)
    pl.semaphore_wait(barrier, 4)

    def to_partner(src, dst, i):
        pltpu.make_async_remote_copy(
            src_ref=src, dst_ref=dst, send_sem=pair_send.at[i], recv_sem=pair_recv.at[i],
            device_id=(partner,), device_id_type=MESH).start()

    to_partner(up_hbm.at[1 - core], upr_hbm, 0)
    to_partner(x_hbm, xr_hbm, 1)
    to_partner(dy_hbm, dyr_hbm, 2)
    mine = pl.ds(pl.multiple_of(core * tokens, 16), tokens)
    theirs = pl.ds(pl.multiple_of((1 - core) * tokens, 16), tokens)

    def main(x, dy, w1, w2, ud, at, s1, s2):
        for n in range(nc):
            copy(up_hbm.at[core, n], ud.at[pl.ds(pl.multiple_of(n * 3 * rows + core * half, 16), half)], local.at[0]).start()
        own_down = x.at[pl.ds(0, nc * units)]
        copy(down_hbm, own_down, local.at[1]).start()
        wait_for(down_hbm, local.at[1])
        for n in range(nc):
            for k in range(COLOURS):
                copy(x.at[pl.ds(n * units, units), down_cols(k)], a2.at[n, k, 0], local.at[1]).start()
        wait_for(upr_hbm, pair_recv.at[0])
        for n in range(nc):
            copy(upr_hbm.at[n], ud.at[pl.ds(pl.multiple_of(n * 3 * rows + (1 - core) * half, 16), half)], local.at[0]).start()
        wait_for(up_hbm, local.at[0])
        for n in range(nc):
            for k in range(COLOURS):
                copy(ud.at[pl.ds((n * 3 + k) * rows, rows)], a1.at[n, k, 0], local.at[0]).start()
        wait_for(up_hbm, local.at[0])
        wait_for(down_hbm, local.at[1])
        ag_start(0, 0)
        copy(x_hbm, x.at[mine], local.at[1]).start()
        copy(dy_hbm, dy.at[mine], local.at[2]).start()
        ag_wait(0, 0)
        ag_start(0, 1)
        wait_for(xr_hbm, pair_recv.at[1])
        copy(xr_hbm, x.at[theirs], local.at[1]).start()
        ag_wait(0, 1)
        ag_start(0, 2)
        ag_start(1, 0)
        ag_start(2, 0)
        ag_start(3, 0)
        wait_for(dyr_hbm, pair_recv.at[2])
        copy(dyr_hbm, dy.at[theirs], local.at[2]).start()

        def load_weights(n):
            for k in range(COLOURS):
                for m in range(CHIPS):
                    copy(a1.at[n, k, m], w1.at[up_rows(k, m, GATHER)], local.at[3]).start()
                    copy(a2.at[n, k, m], w2.at[down_rows(k, m, GATHER), down_cols(k)], local.at[4]).start()

        ag_wait(0, 2)
        load_weights(0)
        wait_for(x, local.at[1])
        wait_for(dy, local.at[2])

        def send_up(n):
            for k in range(COLOURS):
                pltpu.make_async_remote_copy(
                    src_ref=p1.at[n, k, pl.ds(4, 4)], dst_ref=ra1.at[n, k], send_sem=rs_send.at[0, n],
                    recv_sem=rs_recv.at[0, n], device_id=(near[k],), device_id_type=MESH).start()

        def send_down(n):
            for k in range(COLOURS):
                pltpu.make_async_remote_copy(
                    src_ref=p2.at[n, k, pl.ds(4, 4)], dst_ref=ra2.at[n, k], send_sem=rs_send.at[0, n],
                    recv_sem=rs_recv.at[0, n], device_id=(near[k],), device_id_type=MESH).start()

        up_tile = both // UP_TILES

        def chunk(n, carry):
            wait_for(w1, local.at[3])
            wait_for(w2, local.at[4])

            def up_step(t, carry):
                at_t = pl.ds(pl.multiple_of(t * up_tile, up_tile), up_tile)
                u = jnp.dot(x[at_t, :], w1[...], preferred_element_type=F32).astype(BF16).astype(F32)
                da = lax.dot_general(dy[at_t, :], w2[...], (((1,), (1,)), ((), ())), preferred_element_type=F32)
                a, slope = gelu_both(u)
                ud[at_t, :] = (da * slope).astype(BF16)
                at[:, at_t] = a.astype(BF16).T

                @pl.when((t == 1) & (n == 0))
                def _():
                    ag_wait(1, 0)
                    ag_start(1, 1)
                    ag_wait(2, 0)
                    ag_start(2, 1)

                @pl.when((t == 1) & (n > 0))
                def _():
                    wait_for(p1.at[0], local.at[5])
                    send_up(n - 1)

                return carry

            lax.fori_loop(0, UP_TILES, up_step, 0)
            copy(ud, du_hbm.at[n], local.at[7]).start()

            @pl.when(n == 0)
            def _():
                ag_wait(1, 1)
                ag_start(1, 2)

            def down_grad(k, carry):
                part = pl.ds(pl.multiple_of(k * cols, cols), cols)
                s2[:, part] = jnp.dot(at[...], dy[:, part], preferred_element_type=F32).astype(BF16)
                return carry

            lax.fori_loop(0, 3, down_grad, 0)
            for k in range(COLOURS):
                for m in range(CHIPS):
                    copy(s2.at[down_rows(k, m, REDUCE), down_cols(k)], p2.at[n, k, m], local.at[6]).start()

            @pl.when(n + 1 < nc)
            def _():
                ag_wait(n + 1, 2)
                load_weights(n + 1)

            def up_grad(k, carry):
                part = pl.ds(pl.multiple_of(k * cols, cols), cols)
                s1[part, :] = lax.dot_general(
                    x[:, part], ud[...], (((0,), (0,)), ((), ())), preferred_element_type=F32).astype(BF16)
                return carry

            lax.fori_loop(0, 3, up_grad, 0)
            for k in range(COLOURS):
                for m in range(CHIPS):
                    copy(s1.at[up_rows(k, m, REDUCE)], p1.at[n, k, m], local.at[5]).start()

            @pl.when(n + 2 < nc)
            def _():
                ag_wait(n + 2, 1)
                ag_start(n + 2, 2)

            @pl.when(n + 3 < nc)
            def _():
                ag_wait(n + 3, 0)
                ag_start(n + 3, 1)

            @pl.when(n + 4 < nc)
            def _():
                ag_start(n + 4, 0)

            wait_for(p2.at[0], local.at[6])
            send_down(n)
            wait_for(ud, local.at[7])
            return carry

        lax.fori_loop(0, nc, chunk, 0)
        wait_for(p1.at[0], local.at[5])
        send_up(nc - 1)

    pl.run_scoped(
        main,
        pltpu.VMEM((both, width), BF16), pltpu.VMEM((both, width), BF16),
        pltpu.VMEM((width, fc), BF16), pltpu.VMEM((fc, width), BF16),
        pltpu.VMEM((both, fc), BF16), pltpu.VMEM((fc, both), BF16),
        pltpu.VMEM((width, fc), BF16), pltpu.VMEM((fc, width), BF16))

    dx_tile = both // DX_TILES
    half_tiles = DX_TILES // 2
    steps = 3 * DX_TILES
    hidden = nc * fc

    def last(w, du, out32, out16, got, res,
             c1, c2, cr1, cr2, co1, co2, d1, d2, do1, do2, e1, e2, eo1, eo2):
        def load_w(n, carry):
            for k in range(COLOURS):
                for m in range(CHIPS):
                    copy(a1.at[n, k, m], w.at[up_rows(k, m, GATHER), pl.ds(pl.multiple_of(n * fc, fc), fc)], local.at[0]).start()
            return carry

        lax.fori_loop(0, nc, load_w, 0)

        def tokens_at(q):
            later = q // half_tiles
            owner = (1 - later) * (1 - core) + later * core
            return pl.multiple_of(owner * tokens + (q % half_tiles) * dx_tile, dx_tile)

        def load_du(q):
            slot = q % 2
            for n in range(nc):
                copy(du_hbm.at[n, pl.ds(tokens_at(q), dx_tile)], du.at[slot, :, pl.ds(n * fc, fc)], local.at[1 + slot]).start()

        load_du(0)

        def own_at(q, n):
            return (pl.ds(pl.multiple_of((q % half_tiles) * dx_tile, dx_tile), dx_tile), pl.ds(pl.multiple_of(n * cols, cols), cols))

        def c_load(n):
            rs_wait(n, 0)
            copy(p1.at[n, :, pl.ds(2, 2)], c1, local.at[5]).start()
            copy(p2.at[n, :, pl.ds(2, 2)], c2, local.at[5]).start()
            copy(ra1.at[n, :, pl.ds(2, 2)], cr1, local.at[5]).start()
            copy(ra2.at[n, :, pl.ds(2, 2)], cr2, local.at[5]).start()

        def c_send(n):
            wait_for(p1.at[0], local.at[5])

            @pl.when(n > 0)
            def _():
                wait_for(sized[1].at[0], rs_send.at[1, n - 1])

            for k in range(COLOURS):
                co1[k] = (c1[k].astype(F32) + cr1[k].astype(F32)).astype(BF16)
                co2[k] = (c2[k].astype(F32) + cr2[k].astype(F32)).astype(BF16)
                rs_start(n, 1, k, co1.at[k], co2.at[k])

        def d_load(n):
            rs_wait(n, 1)
            for i, (b1, b2) in enumerate(((p1, p2), (ra1, ra2), (rb1, rb2))):
                copy(b1.at[n, :, 1], d1.at[i], local.at[6]).start()
                copy(b2.at[n, :, 1], d2.at[i], local.at[6]).start()

        def d_send(n):
            wait_for(d1, local.at[6])
            wait_for(d2, local.at[6])

            @pl.when(n > 0)
            def _():
                wait_for(sized[0].at[0], rs_send.at[2, n - 1])

            for k in range(COLOURS):
                do1[k] = (d1[0, k].astype(F32) + d1[1, k].astype(F32) + d1[2, k].astype(F32)).astype(BF16)
                do2[k] = (d2[0, k].astype(F32) + d2[1, k].astype(F32) + d2[2, k].astype(F32)).astype(BF16)
                rs_start(n, 2, k, do1.at[k], do2.at[k])

        def e_load(n):
            rs_wait(n, 2)
            for i, (b1, b2) in enumerate(((p1, p2), (ra1, ra2), (rb1, rb2))):
                copy(b1.at[n, :, 0], e1.at[i], local.at[7]).start()
                copy(b2.at[n, :, 0], e2.at[i], local.at[7]).start()
            copy(rc1.at[n], e1.at[3], local.at[7]).start()
            copy(rc2.at[n], e2.at[3], local.at[7]).start()

        keep = pl.ds(pl.multiple_of(core * half, 16), half)
        give = pl.ds(pl.multiple_of((1 - core) * half, 16), half)

        def e_wait_out(n):
            wait_for(gup_hbm.at[0, 0], local.at[8])
            wait_for(gdown_hbm.at[pl.ds(0, units)], local.at[9])
            wait_for(gup_hbm.at[0, 0], gup_send.at[n])

        def e_store(n):
            wait_for(e1, local.at[7])
            wait_for(e2, local.at[7])

            @pl.when(n > 0)
            def _():
                e_wait_out(n - 1)

            for k in range(COLOURS):
                eo1[k * rows:(k + 1) * rows, :] = (
                    e1[0, k].astype(F32) + e1[1, k].astype(F32) + e1[2, k].astype(F32) + e1[3, k].astype(F32)).astype(BF16)
                eo2[:, k * cols:(k + 1) * cols] = (
                    e2[0, k].astype(F32) + e2[1, k].astype(F32) + e2[2, k].astype(F32) + e2[3, k].astype(F32)).astype(BF16)
            copy(eo1.at[keep], gup_hbm.at[core, n], local.at[8]).start()
            copy(eo2, gdown_hbm.at[pl.ds(pl.multiple_of(n * units, 16), units)], local.at[9]).start()
            pltpu.make_async_remote_copy(
                src_ref=eo1.at[give], dst_ref=gup_hbm.at[core, n], send_sem=gup_send.at[n], recv_sem=gup_recv.at[n],
                device_id=(partner,), device_id_type=MESH).start()

        def pump(i):
            for first, every, load, finish in ((0, 1, c_load, c_send), (4, 2, d_load, d_send), (7, 2, e_load, e_store)):
                at = i - first
                n = at // every

                if every == 1:
                    @pl.when((at > 0) & (at <= nc))
                    def _(finish=finish, n=n):
                        finish(n - 1)

                    @pl.when((at >= 0) & (at < nc))
                    def _(load=load, n=n):
                        load(n)
                else:
                    @pl.when((at >= 0) & (at % 2 == 0) & (n < nc))
                    def _(load=load, n=n):
                        load(n)

                    @pl.when((at >= 0) & (at % 2 == 1) & (n < nc))
                    def _(finish=finish, n=n):
                        finish(n)

        def step(i, carry):
            q, n = i // 3, i % 3
            slot = i % 2

            @pl.when((i < steps) & (n == 0))
            def _():
                @pl.when(q + 1 < DX_TILES)
                def _():
                    load_du(q + 1)

                wait_for(du.at[0], local.at[1 + q % 2])

                @pl.when(i == 0)
                def _():
                    wait_for(w, local.at[0])

            @pl.when((i >= 3 * half_tiles) & (i < steps))
            def _():
                here = own_at(q, n)
                wait_for(dxr_hbm.at[here], dx_recv.at[i - 3 * half_tiles])
                copy(dxr_hbm.at[here], got, local.at[3]).start()
                copy(dy_hbm.at[here], res, local.at[4]).start()

            @pl.when((i >= 2) & (i < 3 * half_tiles + 2))
            def _():
                wait_for(out32.at[0], dx_send.at[i - 2])

            @pl.when((i >= 3 * half_tiles + 2) & (i < steps))
            def _():
                wait_for(out16.at[0], local.at[10 + slot])

            @pl.when(i < steps)
            def _():
                part = pl.ds(pl.multiple_of(n * cols, cols), cols)
                acc = lax.dot_general(du[q % 2], w[part, :], (((1,), (1,)), ((), ())), preferred_element_type=F32)

                out32[slot] = acc

            @pl.when(i < 3 * half_tiles)
            def _():
                pltpu.make_async_remote_copy(
                    src_ref=out32.at[slot], dst_ref=dxr_hbm.at[own_at(q, n)], send_sem=dx_send.at[i], recv_sem=dx_recv.at[i],
                    device_id=(partner,), device_id_type=MESH).start()

            @pl.when((i >= 3 * half_tiles) & (i < steps))
            def _():
                wait_for(got, local.at[3])
                wait_for(res, local.at[4])
                out16[slot] = (res[...].astype(F32) + (out32[slot] + got[...])).astype(BF16)
                copy(out16.at[slot], dx_hbm.at[own_at(q, n)], local.at[10 + slot]).start()

            pump(i)
            return carry

        lax.fori_loop(0, max(steps, 2 * nc + 7), step, 0)
        wait_for(out16.at[0], local.at[10])
        wait_for(out16.at[0], local.at[11])
        wait_for(sized[1].at[0], rs_send.at[1, nc - 1])
        wait_for(sized[0].at[0], rs_send.at[2, nc - 1])
        e_wait_out(nc - 1)

    pl.run_scoped(
        last,
        pltpu.VMEM((width, hidden), BF16), pltpu.VMEM((2, dx_tile, hidden), BF16),
        pltpu.VMEM((2, dx_tile, cols), F32), pltpu.VMEM((2, dx_tile, cols), BF16),
        pltpu.VMEM((dx_tile, cols), F32), pltpu.VMEM((dx_tile, cols), BF16),
        *[pltpu.VMEM((3, 2, *s), BF16) for _ in range(3) for s in ((rows, fc), (units, cols))],
        pltpu.VMEM((3, 3, rows, fc), BF16), pltpu.VMEM((3, 3, units, cols), BF16),
        pltpu.VMEM((3, rows, fc), BF16), pltpu.VMEM((3, units, cols), BF16),
        pltpu.VMEM((4, 3, rows, fc), BF16), pltpu.VMEM((4, 3, units, cols), BF16),
        pltpu.VMEM((3 * rows, fc), BF16), pltpu.VMEM((units, width), BF16))

    def drain(n, carry):
        for s in range(3):
            wait_for(sized[s].at[n], ag_send.at[s, n])
        wait_for(sized[2].at[n], rs_send.at[0, n])
        wait_for(gup_hbm.at[0, 0], gup_recv.at[n])
        return carry

    lax.fori_loop(0, nc, drain, 0)
    wait_for(upr_hbm, pair_send.at[0])
    wait_for(xr_hbm, pair_send.at[1])
    wait_for(dyr_hbm, pair_send.at[2])


def chunks_of(units):
    return 9 if units % 144 == 0 else 1


def solution(mesh):
    def device_fn(x_loc, dy_loc, up_loc, down_loc):
        width = x_loc.shape[-1]
        x = x_loc.reshape(-1, width)
        dy = dy_loc.reshape(-1, width)
        tokens = x.shape[0]
        down = down_loc[0]
        half, units_all = up_loc.shape[1], down.shape[0]
        nc = chunks_of(units_all)
        units = units_all // nc
        fc = CHIPS * units
        rows, cols = 2 * half // 3, width // 3
        up = up_loc.reshape(half, CHIPS, CORES, nc, units).transpose(2, 3, 0, 1, 4).reshape(CORES, nc, half, fc)

        def hbm(*shape, dtype=BF16):
            return jax.ShapeDtypeStruct(shape, dtype)

        one, two = (rows, fc), (units, cols)
        outs = [
            hbm(CORES, nc, half, fc), hbm(units_all, width), hbm(tokens, width),
            hbm(tokens, width), hbm(tokens, width), hbm(nc, half, fc),
            *[hbm(nc, 3, blocks, *s) for blocks in (8, 8, 4, 2) for s in (one, two)],
            hbm(nc, 3, *one), hbm(nc, 3, *two),
            hbm(nc, 2 * tokens, fc), hbm(tokens, width, dtype=F32),
        ]
        dma = pltpu.SemaphoreType.DMA
        half_steps = 3 * DX_TILES // 2
        got = pl.pallas_call(
            functools.partial(kernel, nc),
            out_shape=outs,
            in_specs=[pl.BlockSpec(memory_space=pl.ANY)] * 4,
            out_specs=[pl.BlockSpec(memory_space=pl.ANY)] * len(outs),
            scratch_shapes=[
                dma((3, nc)), dma((3, nc)), dma((3, nc)), dma((3, nc)), dma((3,)), dma((3,)),
                dma((half_steps,)), dma((half_steps,)), dma((nc,)), dma((nc,)), dma((12,)),
            ],
            compiler_params=pltpu.CompilerParams(
                collective_id=0, has_side_effects=True, vmem_limit_bytes=67_000_000),
        )(x, dy, up, down)
        g_up = got[0].reshape(CORES, nc, half, CHIPS, units).transpose(2, 3, 0, 1, 4).reshape(1, half, -1)
        return g_up, got[1][None], got[2].reshape(x_loc.shape)

    return jax.shard_map(
        device_fn, mesh=mesh, in_specs=(P("data"), P("data"), P(None, "data"), P(None, "data")),
        out_specs=(P(None, "data"), P(None, "data"), P("data")), check_vma=False)
```

```python
import functools
import math

import jax
import jax.numpy as jnp
from jax import lax
from jax.experimental import pallas as pl
from jax.experimental.pallas import tpu as pltpu
from jax.sharding import PartitionSpec as P

MESH = pl.DeviceIdType.MESH
F32, BF16 = jnp.float32, jnp.bfloat16
CHIPS, COLOURS, CORES = 8, 3, 2
DX_TILES = 8
UP_TILES = 8
PARTS = 2
UP_IN, X_IN, DY_IN, W1_IN, W2_IN, G1_OUT, G2_OUT, DU_OUT, SUM_IN, SUM_OUT, OWN_0, OWN_1, OWN_2 = range(13)
TILE_IN, _, GOT_IN, RES_IN, C_IN, D_IN, E_IN, GUP_OUT, GDOWN_OUT, DX_OUT = range(10)
EARLY = 4


def copy(src, dst, sem):
    return pltpu.make_async_copy(src, dst, sem)


def wait_for(ref, sem):
    pltpu.make_async_copy(ref, ref, sem).wait()


def gelu_both(u):
    scale = math.sqrt(2.0 / math.pi)
    square = u * u
    th = jnp.tanh(u * (scale + (0.044715 * scale) * square))
    half = 0.5 * th
    cdf = 0.5 + half
    slope = cdf + (u * (0.5 - th * half)) * (scale + (0.134145 * scale) * square)
    return u * cdf, slope


def kernel(nc, x_hbm, dy_hbm, up_hbm, down_hbm,
           gup_hbm, gdown_hbm, dx_hbm,
           xr_hbm, dyr_hbm, a1, a2, p1, p2, ra1, ra2, rb1, rb2, rc1, rc2, cb1, cb2, du_hbm, dxr_hbm,
           ag_send, ag_recv, rs_send, rs_recv, pair_send, pair_recv, dx_send, dx_recv, gup_send, gup_recv, w_sem, local):
    me = lax.axis_index("data")
    core = me % 2
    bits = [(me // 2) % 2, (me // 4) % 2, (me // 8) % 2]
    partner = me + 1 - 2 * core
    near = [me + (2 << d) * (1 - 2 * bits[d]) for d in range(3)]

    tokens, width = x_hbm.shape
    both = 2 * tokens
    rows = a1.shape[3]
    fc = a1.shape[4]
    units = a2.shape[3]
    cols = a2.shape[4]
    half = up_hbm.shape[0]
    third = half // 3

    def chip(colour, m, order):
        total = 0
        for i in range(3):
            d = (colour + i) % 3
            flipped = (m >> order[i]) & 1
            total = total + (1 << d) * ((1 - bits[d]) if flipped else bits[d])
        return total

    GATHER, REDUCE = (0, 1, 2), (2, 1, 0)

    def up_rows(colour, m, order):
        return pl.ds(pl.multiple_of(chip(colour, m, order) * (3 * rows) + colour * rows, 16), rows)

    def down_rows(colour, m, order):
        return pl.ds(pl.multiple_of(chip(colour, m, order) * units, 16), units)

    def down_cols(colour):
        return pl.ds(colour * cols, cols)

    def ag_start(n, s, arrays=(0, 1)):
        have = 1 << s
        for k in range(COLOURS):
            for i in arrays:
                buf = (a1, a2)[i]
                pltpu.make_async_remote_copy(
                    src_ref=buf.at[n, k, pl.ds(0, have)], dst_ref=buf.at[n, k, pl.ds(have, have)],
                    send_sem=ag_send.at[i, s, n], recv_sem=ag_recv.at[i, s, n],
                    device_id=(near[(k + s) % 3],), device_id_type=MESH).start()

    one_array = (rc1, rb1, ra1)
    sized = (rb1, ra1, p1)

    def ag_wait(n, s, arrays=(0, 1)):
        for i in arrays:
            wait_for(one_array[s].at[n], ag_recv.at[i, s, n])

    def rs_start(n, s, k, src1, src2):
        dst1, dst2 = ((ra1, ra2), (rb1, rb2), (rc1, rc2))[s]
        for src, dst in ((src1, dst1), (src2, dst2)):
            pltpu.make_async_remote_copy(
                src_ref=src, dst_ref=dst.at[n, k], send_sem=rs_send.at[s, n], recv_sem=rs_recv.at[s, n],
                device_id=(near[(k + s) % 3],), device_id_type=MESH).start()

    def rs_wait(n, s):
        wait_for(sized[2 - s].at[n], rs_recv.at[s, n])

    barrier = pltpu.get_barrier_semaphore()
    for other in (partner, *near):
        pl.semaphore_signal(barrier, inc=1, device_id=(other,), device_id_type=MESH)

    def to_partner(src, dst, i):
        pltpu.make_async_remote_copy(
            src_ref=src, dst_ref=dst, send_sem=pair_send.at[i], recv_sem=pair_recv.at[i],
            device_id=(partner,), device_id_type=MESH).start()

    mine = pl.ds(pl.multiple_of(core * tokens, 16), tokens)
    theirs = pl.ds(pl.multiple_of((1 - core) * tokens, 16), tokens)

    def c_load(n, c1, c2, sem):
        with jax.named_scope("wait_rs0"):
            rs_wait(n, 0)
        for i, (b1, b2) in enumerate(((p1, p2), (ra1, ra2))):
            for j in range(2):
                copy(b1.at[n, :, 2 + j], c1.at[2 * i + j], sem).start()
                copy(b2.at[n, :, 2 + j], c2.at[2 * i + j], sem).start()

    def c_sum(c1, c2, to1, to2, sem):
        wait_for(p1.at[0], sem)
        for k in range(COLOURS):
            for j in range(2):
                to1[k, j] = (c1[j, k].astype(F32) + c1[2 + j, k].astype(F32)).astype(BF16)
                to2[k, j] = (c2[j, k].astype(F32) + c2[2 + j, k].astype(F32)).astype(BF16)

    def main(x, dy, w1, w2, ud, at, s1, s2, c1, c2, co1, co2):
        own_down = x.at[pl.ds(0, nc * units)]
        blocks = up_hbm.shape[1] // width
        for b in range(blocks):
            copy(up_hbm.at[:, pl.ds(b * width, width)], x.at[pl.ds(nc * units + b * half, half)], local.at[UP_IN]).start()
        copy(down_hbm, own_down, local.at[X_IN]).start()
        wait_for(up_hbm, local.at[UP_IN])

        def unit(chip_, core_, n):
            first = ((chip_ * CORES + core_) * nc + n) * units
            b, c = first // width, first % width
            return x[nc * units + b * half:nc * units + (b + 1) * half, c:c + units]

        whole = pl.ds(pl.multiple_of(core * third, 16), 2 * third)
        rest = pl.ds(pl.multiple_of((1 - core) * 2 * third, 16), third)
        to_rest = pl.ds(pl.multiple_of(core * third, 16), third)

        def permute(n):
            for c in range(CORES):
                first = (n * CORES + c) * half
                ud[first:first + half, :] = jnp.concatenate([unit(r, c, n) for r in range(CHIPS)], axis=1)

        def own_up(n):
            def part(c, which):
                return ud.at[pl.ds(pl.multiple_of((n * CORES + c) * half + which.start, 16), which.size)]

            sem = min(n, 1)
            for which, dst in ((whole, a1.at[n, 2 * core, 0]), (rest, a1.at[n, 1, 0, to_rest])):
                pltpu.make_async_remote_copy(
                    src_ref=part(1 - core, which), dst_ref=dst, send_sem=pair_send.at[0], recv_sem=pair_recv.at[3 * sem],
                    device_id=(partner,), device_id_type=MESH).start()
                copy(part(core, which), dst, local.at[OWN_0 + sem]).start()

        def down_own(n):
            for k in range(COLOURS):
                copy(x.at[pl.ds(n * units, units), down_cols(k)], a2.at[n, k, 0], local.at[OWN_2 if n else X_IN]).start()

        permute(0)
        with jax.named_scope("entry"):
            pl.semaphore_wait(barrier, 4)
        own_up(0)
        wait_for(down_hbm, local.at[X_IN])
        down_own(0)
        for n in range(1, nc):
            permute(n)
        for n in range(1, nc):
            down_own(n)
            own_up(n)
        to_partner(x_hbm, xr_hbm, 1)
        to_partner(dy_hbm, dyr_hbm, 2)
        with jax.named_scope("own_wait"):
            wait_for(down_hbm.at[pl.ds(0, units)], local.at[X_IN])
            ag_start(0, 0, (1,))
            wait_for(du_hbm.at[0, pl.ds(0, half)], local.at[OWN_0])
            wait_for(du_hbm.at[0, pl.ds(0, half)], pair_recv.at[0])
        ag_start(0, 0, (0,))
        wait_for(down_hbm.at[pl.ds(0, (nc - 1) * units)], local.at[OWN_2])
        copy(x_hbm, x.at[mine], local.at[X_IN]).start()
        copy(dy_hbm, dy.at[mine], local.at[DY_IN]).start()
        for s in range(2):
            for i in range(2):
                with jax.named_scope(f"ag0{s}{i}"):
                    ag_wait(0, s, (i,))
                ag_start(0, s + 1, (i,))
        wait_for(du_hbm.at[0, pl.ds(0, (nc - 1) * half)], local.at[OWN_1])
        wait_for(du_hbm.at[0, pl.ds(0, (nc - 1) * half)], pair_recv.at[3])
        ag_start(1, 0)
        with jax.named_scope("xr"):
            wait_for(xr_hbm, pair_recv.at[1])
        copy(xr_hbm, x.at[theirs], local.at[X_IN]).start()

        def load_up(n):
            for k in range(COLOURS):
                for m in range(CHIPS):
                    copy(a1.at[n, k, m], w1.at[up_rows(k, m, GATHER)], local.at[W1_IN]).start()

        def load_down(n):
            for k in range(COLOURS):
                for m in range(CHIPS):
                    copy(a2.at[n, k, m], w2.at[down_rows(k, m, GATHER), down_cols(k)], local.at[W2_IN]).start()

        with jax.named_scope("ag020"):
            ag_wait(0, 2, (0,))
        load_up(0)
        with jax.named_scope("dyr"):
            wait_for(dyr_hbm, pair_recv.at[2])
        copy(dyr_hbm, dy.at[theirs], local.at[DY_IN]).start()
        with jax.named_scope("ag021"):
            ag_wait(0, 2, (1,))
        load_down(0)
        with jax.named_scope("tokens"):
            wait_for(x, local.at[X_IN])
            wait_for(dy, local.at[DY_IN])
            wait_for(du_hbm.at[0, pl.ds(0, nc * half)], pair_send.at[0])

        def send_first(src, dst, n):
            for k in range(COLOURS):
                pltpu.make_async_remote_copy(
                    src_ref=src.at[n, k, pl.ds(4, 4)], dst_ref=dst.at[n, k], send_sem=rs_send.at[0, n],
                    recv_sem=rs_recv.at[0, n], device_id=(near[k],), device_id_type=MESH).start()

        def send_both(n):
            wait_for(p2.at[0], local.at[G2_OUT])
            send_first(p2, ra2, n)
            wait_for(p1.at[0], local.at[G1_OUT])
            send_first(p1, ra1, n)

        def c_in(n):
            c_load(n, c1, c2, local.at[SUM_IN])

        def c_add(n):
            c_sum(c1, c2, co1, co2, local.at[SUM_IN])
            copy(co1, cb1.at[n], local.at[SUM_OUT]).start()
            copy(co2, cb2.at[n], local.at[SUM_OUT]).start()

        def c_go(n):
            wait_for(sized[1].at[0], local.at[SUM_OUT])
            for k in range(COLOURS):
                rs_start(n, 1, k, cb1.at[n, k], cb2.at[n, k])

        up_tile = both // UP_TILES

        def chunk(n, carry):
            with jax.named_scope("wait_w"):
                wait_for(w1, local.at[W1_IN])
                wait_for(w2, local.at[W2_IN])

            def up_step(t, carry):
                for part in range(PARTS):
                    size = up_tile // PARTS
                    first = t * up_tile + part * size
                    at_t = pl.ds(pl.multiple_of(first, size), size)
                    u = jnp.dot(x[at_t, :], w1[...], preferred_element_type=F32).astype(BF16)
                    da = lax.dot_general(dy[at_t, :], w2[...], (((1,), (1,)), ((), ())), preferred_element_type=F32)
                    strip = min(128, size)
                    for c in range(0, fc, 128):
                        for r in range(0, size, strip):
                            at_r = pl.ds(pl.multiple_of(first + r, strip), strip)
                            a, slope = gelu_both(u[r:r + strip, c:c + 128].astype(F32))
                            ud[at_r, c:c + 128] = (da[r:r + strip, c:c + 128] * slope).astype(BF16)
                            at[c:c + 128, at_r] = a.astype(BF16).T

                @pl.when((t == 1) & (n == 0))
                def _():
                    with jax.named_scope("wait_10"):
                        ag_wait(1, 0)
                    ag_start(1, 1)
                    ag_start(2, 0)

                @pl.when((t == 6) & (n == 0))
                def _():
                    with jax.named_scope("wait_11"):
                        ag_wait(1, 1)
                    ag_start(1, 2)
                    ag_start(3, 0)

                @pl.when((t == 2) & (n > 0))
                def _():
                    @pl.when(n + 1 < nc)
                    def _():
                        with jax.named_scope("wait_ag1"):
                            ag_wait(n + 1, 1)
                        ag_start(n + 1, 2)

                    @pl.when(n + 2 < nc)
                    def _():
                        with jax.named_scope("wait_ag0"):
                            ag_wait(n + 2, 0)
                        ag_start(n + 2, 1)

                    @pl.when(n + 3 < nc)
                    def _():
                        ag_start(n + 3, 0)

                    send_both(n - 1)

                @pl.when((t == 4) & (n == nc - 1))
                def _():
                    c_go(0)
                    c_add(1)
                    c_in(2)

                return carry

            with jax.named_scope("up"):
                lax.fori_loop(0, UP_TILES, up_step, 0)
            copy(ud, du_hbm.at[n], local.at[DU_OUT]).start()

            @pl.when(n == 0)
            def _():
                with jax.named_scope("wait_20"):
                    ag_wait(2, 0)
                ag_start(2, 1)

            @pl.when(n == nc - 1)
            def _():
                c_go(1)
                c_add(2)
                c_in(3)

            def down_grad(k, carry):
                part = pl.ds(pl.multiple_of(k * cols, cols), cols)
                s2[:, part] = jnp.dot(at[...], dy[:, part], preferred_element_type=F32).astype(BF16)
                return carry

            with jax.named_scope("down_grad"):
                lax.fori_loop(0, 3, down_grad, 0)
            for k in range(COLOURS):
                for m in range(CHIPS):
                    copy(s2.at[down_rows(k, m, REDUCE), down_cols(k)], p2.at[n, k, m], local.at[G2_OUT]).start()

            @pl.when(n == nc - 2)
            def _():
                c_in(0)

            @pl.when(n == nc - 1)
            def _():
                c_go(2)
                c_add(3)

            def up_grad(k, carry):
                part = pl.ds(pl.multiple_of(k * cols, cols), cols)

                @pl.when((k == 2) & (n + 1 < nc))
                def _():
                    with jax.named_scope("wait_ag2"):
                        ag_wait(n + 1, 2)
                    load_up(n + 1)
                    load_down(n + 1)

                s1[part, :] = lax.dot_general(
                    x[:, part], ud[...], (((0,), (0,)), ((), ())), preferred_element_type=F32).astype(BF16)
                return carry

            with jax.named_scope("up_grad"):
                lax.fori_loop(0, 3, up_grad, 0)
            for k in range(COLOURS):
                for m in range(CHIPS):
                    copy(s1.at[up_rows(k, m, REDUCE)], p1.at[n, k, m], local.at[G1_OUT]).start()

            @pl.when(n == nc - 2)
            def _():
                c_add(0)
                c_in(1)

            @pl.when(n == nc - 1)
            def _():
                c_go(3)

            wait_for(ud, local.at[DU_OUT])
            return carry

        lax.fori_loop(0, nc, chunk, 0)
        send_both(nc - 1)

    pl.run_scoped(
        main,
        pltpu.VMEM((both, width), BF16), pltpu.VMEM((both, width), BF16),
        pltpu.VMEM((width, fc), BF16), pltpu.VMEM((fc, width), BF16),
        pltpu.VMEM((both, fc), BF16), pltpu.VMEM((fc, both), BF16),
        pltpu.VMEM((width, fc), BF16), pltpu.VMEM((fc, width), BF16),
        pltpu.VMEM((4, 3, rows, fc), BF16), pltpu.VMEM((4, 3, units, cols), BF16),
        pltpu.VMEM((3, 2, rows, fc), BF16), pltpu.VMEM((3, 2, units, cols), BF16))

    dx_tile = both // DX_TILES
    half_tiles = DX_TILES // 2
    steps = 3 * DX_TILES
    hidden = nc * fc

    def last(w, du, out32, out16, got, res,
             co1, co2, d1, d2, do1, do2, e1, e2, eo1, eo2):
        def load_w(n, third_):
            for p in range(8):
                r, k = divmod(8 * third_ + p, 3)
                m = 0
                for i in range(3):
                    d = (k + i) % 3
                    m = m + (1 << i) * ((1 - bits[d]) if (r >> d) & 1 else bits[d])
                copy(a1.at[n, k, m], w.at[pl.ds((8 * third_ + p) * rows, rows), pl.ds(pl.multiple_of(n * fc, fc), fc)],
                     w_sem.at[third_]).start()

        def tokens_at(q):
            later = q // half_tiles
            owner = (1 - later) * (1 - core) + later * core
            return pl.multiple_of(owner * tokens + (q % half_tiles) * dx_tile, dx_tile)

        def load_du(q):
            slot = q % 2
            for n in range(nc):
                copy(du_hbm.at[n, pl.ds(tokens_at(q), dx_tile)], du.at[slot, :, pl.ds(n * fc, fc)], local.at[TILE_IN + slot]).start()

        for third_ in range(3):
            lax.fori_loop(0, nc, lambda n, carry, third_=third_: (load_w(n, third_), carry)[1], 0)
            if third_ == 0:
                load_du(0)

        def own_at(q, n):
            return (pl.ds(pl.multiple_of((q % half_tiles) * dx_tile, dx_tile), dx_tile), pl.ds(pl.multiple_of(n * cols, cols), cols))

        def c_in(n):
            c_load(n, e1, e2, local.at[C_IN])

        def c_send(n):
            to1, to2 = co1.at[n - EARLY], co2.at[n - EARLY]
            c_sum(e1, e2, to1, to2, local.at[C_IN])
            for k in range(COLOURS):
                rs_start(n, 1, k, to1.at[k], to2.at[k])

        def d_load(n):
            with jax.named_scope("wait_rs1"):
                rs_wait(n, 1)
            for i, (b1, b2) in enumerate(((p1, p2), (ra1, ra2), (rb1, rb2))):
                copy(b1.at[n, :, 1], d1.at[i], local.at[D_IN]).start()
                copy(b2.at[n, :, 1], d2.at[i], local.at[D_IN]).start()

        def d_send(n):
            wait_for(d1, local.at[D_IN])
            wait_for(d2, local.at[D_IN])

            for k in range(COLOURS):
                do1[n, k] = (d1[0, k].astype(F32) + d1[1, k].astype(F32) + d1[2, k].astype(F32)).astype(BF16)
                do2[n, k] = (d2[0, k].astype(F32) + d2[1, k].astype(F32) + d2[2, k].astype(F32)).astype(BF16)
                rs_start(n, 2, k, do1.at[n, k], do2.at[n, k])

        def e_load(n):
            with jax.named_scope("wait_rs2"):
                rs_wait(n, 2)
            for i, (b1, b2) in enumerate(((p1, p2), (ra1, ra2), (rb1, rb2))):
                copy(b1.at[n, :, 0], e1.at[i], local.at[E_IN]).start()
                copy(b2.at[n, :, 0], e2.at[i], local.at[E_IN]).start()
            copy(rc1.at[n], e1.at[3], local.at[E_IN]).start()
            copy(rc2.at[n], e2.at[3], local.at[E_IN]).start()

        keep = pl.ds(pl.multiple_of(core * half, 16), half)
        give = pl.ds(pl.multiple_of((1 - core) * half, 16), half)

        def e_wait_out(n):
            wait_for(gup_hbm.at[0, 0], local.at[GUP_OUT])
            wait_for(gdown_hbm.at[pl.ds(0, units)], local.at[GDOWN_OUT])
            wait_for(gup_hbm.at[0, 0], gup_send.at[n])

        def e_store(n):
            wait_for(e1, local.at[E_IN])
            wait_for(e2, local.at[E_IN])

            @pl.when(n > 0)
            def _():
                e_wait_out(n - 1)

            for k in range(COLOURS):
                eo1[k * rows:(k + 1) * rows, :] = (
                    e1[0, k].astype(F32) + e1[1, k].astype(F32) + e1[2, k].astype(F32) + e1[3, k].astype(F32)).astype(BF16)
                eo2[:, k * cols:(k + 1) * cols] = (
                    e2[0, k].astype(F32) + e2[1, k].astype(F32) + e2[2, k].astype(F32) + e2[3, k].astype(F32)).astype(BF16)
            copy(eo1.at[keep], gup_hbm.at[core, n], local.at[GUP_OUT]).start()
            copy(eo2, gdown_hbm.at[pl.ds(pl.multiple_of(n * units, 16), units)], local.at[GDOWN_OUT]).start()
            pltpu.make_async_remote_copy(
                src_ref=eo1.at[give], dst_ref=gup_hbm.at[core, n], send_sem=gup_send.at[n], recv_sem=gup_recv.at[n],
                device_id=(partner,), device_id_type=MESH).start()

        def pump(i):
            for start, every, low, load, finish_ in (
                    (0, 2, EARLY, c_in, c_send), (7, 1, 0, d_load, d_send), (15, 1, 0, e_load, e_store)):
                since = i - start

                @pl.when((since >= 1) & ((since - 1) % every == 0) & ((since - 1) // every < nc - low))
                def _(finish_=finish_, since=since, every=every, low=low):
                    finish_((since - 1) // every + low)

                @pl.when((since >= 0) & (since % every == 0) & (since // every < nc - low))
                def _(load=load, since=since, every=every, low=low):
                    load(since // every + low)

        def step(i, carry):
            q, n = i // 3, i % 3
            slot = i % 2

            @pl.when((i < steps) & (n == 0))
            def _():
                @pl.when(q + 1 < DX_TILES)
                def _():
                    load_du(q + 1)

                with jax.named_scope("wait_du"):
                    wait_for(du.at[0], local.at[TILE_IN + q % 2])

            @pl.when(i < 3)
            def _():
                with jax.named_scope("wait_wall"):
                    wait_for(w.at[pl.ds(0, cols)], w_sem.at[n])

            @pl.when((i >= 3 * half_tiles) & (i < steps))
            def _():
                here = own_at(q, n)
                with jax.named_scope("wait_dxr"):
                    wait_for(dxr_hbm.at[here], dx_recv.at[i - 3 * half_tiles])
                copy(dxr_hbm.at[here], got, local.at[GOT_IN]).start()
                copy(dy_hbm.at[here], res, local.at[RES_IN]).start()

            @pl.when((i >= 2) & (i < 3 * half_tiles + 2))
            def _():
                with jax.named_scope("wait_dxs"):
                    wait_for(out32.at[0], dx_send.at[i - 2])

            @pl.when((i >= 3 * half_tiles + 2) & (i < steps))
            def _():
                wait_for(out16.at[0], local.at[DX_OUT + slot])

            @pl.when(i < steps)
            def _():
                part = pl.ds(pl.multiple_of(n * cols, cols), cols)
                with jax.named_scope("dx_dot"):
                    out32[slot] = lax.dot_general(
                        du[q % 2], w[part, :], (((1,), (1,)), ((), ())), preferred_element_type=F32)

            @pl.when(i < 3 * half_tiles)
            def _():
                pltpu.make_async_remote_copy(
                    src_ref=out32.at[slot], dst_ref=dxr_hbm.at[own_at(q, n)], send_sem=dx_send.at[i], recv_sem=dx_recv.at[i],
                    device_id=(partner,), device_id_type=MESH).start()

            @pl.when((i >= 3 * half_tiles) & (i < steps))
            def _():
                wait_for(got, local.at[GOT_IN])
                wait_for(res, local.at[RES_IN])
                out16[slot] = (res[...].astype(F32) + (out32[slot] + got[...])).astype(BF16)
                copy(out16.at[slot], dx_hbm.at[own_at(q, n)], local.at[DX_OUT + slot]).start()

            pump(i)
            return carry

        lax.fori_loop(0, max(steps, nc + 16), step, 0)
        for slot in range(2):
            wait_for(out16.at[0], local.at[DX_OUT + slot])
        e_wait_out(nc - 1)
        for n in range(nc):
            wait_for(sized[1].at[0], rs_send.at[1, n])
            wait_for(sized[0].at[0], rs_send.at[2, n])

    pl.run_scoped(
        last,
        pltpu.VMEM((width, hidden), BF16), pltpu.VMEM((2, dx_tile, hidden), BF16),
        pltpu.VMEM((2, dx_tile, cols), F32), pltpu.VMEM((2, dx_tile, cols), BF16),
        pltpu.VMEM((dx_tile, cols), F32), pltpu.VMEM((dx_tile, cols), BF16),
        pltpu.VMEM((nc - EARLY, 3, 2, rows, fc), BF16), pltpu.VMEM((nc - EARLY, 3, 2, units, cols), BF16),
        pltpu.VMEM((3, 3, rows, fc), BF16), pltpu.VMEM((3, 3, units, cols), BF16),
        pltpu.VMEM((nc, 3, rows, fc), BF16), pltpu.VMEM((nc, 3, units, cols), BF16),
        pltpu.VMEM((4, 3, rows, fc), BF16), pltpu.VMEM((4, 3, units, cols), BF16),
        pltpu.VMEM((3 * rows, fc), BF16), pltpu.VMEM((units, width), BF16))

    def drain(n, carry):
        for s in range(3):
            for i in range(2):
                wait_for(one_array[s].at[n], ag_send.at[i, s, n])
        wait_for(sized[2].at[n], rs_send.at[0, n])
        wait_for(gup_hbm.at[0, 0], gup_recv.at[n])
        return carry

    with jax.named_scope("drain"):
        lax.fori_loop(0, nc, drain, 0)
    wait_for(xr_hbm, pair_send.at[1])
    wait_for(dyr_hbm, pair_send.at[2])


def finish(nc, units, gup, gdown, dx, gup_out, gdown_out, dx_out, v_in, v_out, v_down, v_dx, sem_in, sem_out):
    pieces = v_dx.shape[0]
    rows = v_dx.shape[1]
    copy(gup, v_in, sem_in.at[pieces]).start()
    copy(gdown, v_down, sem_in.at[pieces + 1]).start()
    for i in range(pieces):
        copy(dx.at[pl.ds(i * rows, rows)], v_dx.at[i], sem_in.at[i]).start()
    copy(gup, v_in, sem_in.at[pieces]).wait()
    per = 128 // math.gcd(128, units)
    for first in range(0, CHIPS * CORES * nc, per):
        parts = []
        for u in range(first, first + per):
            d, n = u // nc, u % nc
            r, c = d // CORES, d % CORES
            parts.append(v_in[c, n, :, r * units:(r + 1) * units])
        v_out[:, first * units:(first + per) * units] = jnp.concatenate(parts, axis=1)
    copy(v_out, gup_out, sem_out.at[pieces]).start()
    copy(gdown, v_down, sem_in.at[pieces + 1]).wait()
    copy(v_down, gdown_out, sem_out.at[pieces + 1]).start()
    for i in range(pieces):
        copy(dx.at[pl.ds(i * rows, rows)], v_dx.at[i], sem_in.at[i]).wait()
        copy(v_dx.at[i], dx_out.at[pl.ds(i * rows, rows)], sem_out.at[i]).start()
    copy(v_out, gup_out, sem_out.at[pieces]).wait()
    copy(v_down, gdown_out, sem_out.at[pieces + 1]).wait()
    for i in range(pieces):
        copy(v_dx.at[i], dx_out.at[pl.ds(i * rows, rows)], sem_out.at[i]).wait()


def chunks_of(units):
    return 9 if units % 144 == 0 else 1


def solution(mesh):
    def device_fn(x_loc, dy_loc, up_loc, down_loc):
        width = x_loc.shape[-1]
        x = x_loc.reshape(-1, width)
        dy = dy_loc.reshape(-1, width)
        tokens = x.shape[0]
        down = down_loc[0]
        half, units_all = up_loc.shape[1], down.shape[0]
        nc = chunks_of(units_all)
        units = units_all // nc
        fc = CHIPS * units
        rows, cols = 2 * half // 3, width // 3
        up = up_loc[0]

        def hbm(*shape, dtype=BF16):
            return jax.ShapeDtypeStruct(shape, dtype)

        one, two = (rows, fc), (units, cols)
        outs = [
            hbm(CORES, nc, half, fc), hbm(units_all, width), hbm(tokens, width),
            hbm(tokens, width), hbm(tokens, width),
            *[hbm(nc, 3, blocks, *s) for blocks in (8, 8, 4, 2) for s in (one, two)],
            hbm(nc, 3, *one), hbm(nc, 3, *two), hbm(nc, 3, 2, *one), hbm(nc, 3, 2, *two),
            hbm(nc, 2 * tokens, fc), hbm(tokens, width, dtype=F32),
        ]
        dma = pltpu.SemaphoreType.DMA
        half_steps = 3 * DX_TILES // 2
        got = pl.pallas_call(
            functools.partial(kernel, nc),
            out_shape=outs,
            in_specs=[pl.BlockSpec(memory_space=pl.ANY)] * 4,
            out_specs=[pl.BlockSpec(memory_space=pl.ANY)] * len(outs),
            scratch_shapes=[
                dma((2, 3, nc)), dma((2, 3, nc)), dma((3, nc)), dma((3, nc)), dma((3,)), dma((4,)),
                dma((half_steps,)), dma((half_steps,)), dma((nc,)), dma((nc,)), dma((3,)), dma((13,)),
            ],
            compiler_params=pltpu.CompilerParams(
                collective_id=0, has_side_effects=True, vmem_limit_bytes=67_000_000),
        )(x, dy, up, down)
        pieces = 8
        g_up, g_down, dx = pl.pallas_call(
            functools.partial(finish, nc, units),
            out_shape=[hbm(half, up.shape[1]), hbm(units_all, width), hbm(tokens, width)],
            in_specs=[pl.BlockSpec(memory_space=pl.ANY)] * 3,
            out_specs=[pl.BlockSpec(memory_space=pl.ANY)] * 3,
            scratch_shapes=[
                pltpu.VMEM((CORES, nc, half, fc), BF16), pltpu.VMEM((half, up.shape[1]), BF16),
                pltpu.VMEM((units_all, width), BF16), pltpu.VMEM((pieces, tokens // pieces, width), BF16),
                dma((pieces + 2,)), dma((pieces + 2,)),
            ],
            compiler_params=pltpu.CompilerParams(vmem_limit_bytes=67_000_000),
        )(*got[:3])
        return g_up[None], g_down[None], dx.reshape(x_loc.shape)

    return jax.shard_map(
        device_fn, mesh=mesh, in_specs=(P("data"), P("data"), P(None, "data"), P(None, "data")),
        out_specs=(P(None, "data"), P(None, "data"), P("data")), check_vma=False)
```

```python
import functools
import math

import jax
import jax.numpy as jnp
from jax import lax
from jax.experimental import pallas as pl
from jax.experimental.pallas import tpu as pltpu
from jax.sharding import PartitionSpec as P

MESH = pl.DeviceIdType.MESH
F32, BF16 = jnp.float32, jnp.bfloat16
CHIPS, COLOURS, CORES = 8, 3, 2
DX_TILES = 8
UP_TILES = 8
PARTS = 2
UP_IN, X_IN, DY_IN, W1_IN, W2_IN, G1_OUT, G2_OUT, DU_OUT, SUM_IN, SUM_OUT, OWN_0, OWN_1, OWN_2 = range(13)
TILE_IN, GOT_IN, RES_IN, DX_OUT = range(0, 8, 2)
C_IN, D_IN, E_IN, GUP_OUT, GDOWN_OUT = range(8, 13)
EARLY = 4


def copy(src, dst, sem):
    return pltpu.make_async_copy(src, dst, sem)


def wait_for(ref, sem):
    pltpu.make_async_copy(ref, ref, sem).wait()


def gelu_both(u):
    scale = math.sqrt(2.0 / math.pi)
    square = u * u
    th = jnp.tanh(u * (scale + (0.044715 * scale) * square))
    half = 0.5 * th
    cdf = 0.5 + half
    slope = cdf + (u * (0.5 - th * half)) * (scale + (0.134145 * scale) * square)
    return u * cdf, slope


def kernel(nc, x_hbm, dy_hbm, up_hbm, down_hbm,
           gup_hbm, gdown_hbm, dx_hbm,
           xr_hbm, dyr_hbm, a1, a2, p1, p2, ra1, ra2, rb1, rb2, rc1, rc2, cb1, cb2, du_hbm, dxr_hbm,
           ag_send, ag_recv, rs_send, rs_recv, pair_send, pair_recv, dx_send, dx_recv, gup_send, gup_recv, w_sem, local):
    me = lax.axis_index("data")
    core = me % 2
    bits = [(me // 2) % 2, (me // 4) % 2, (me // 8) % 2]
    partner = me + 1 - 2 * core
    near = [me + (2 << d) * (1 - 2 * bits[d]) for d in range(3)]

    tokens, width = x_hbm.shape
    both = 2 * tokens
    rows = a1.shape[3]
    fc = a1.shape[4]
    units = a2.shape[3]
    cols = a2.shape[4]
    half = up_hbm.shape[0]
    third = half // 3

    def chip(colour, m, order):
        total = 0
        for i in range(3):
            d = (colour + i) % 3
            flipped = (m >> order[i]) & 1
            total = total + (1 << d) * ((1 - bits[d]) if flipped else bits[d])
        return total

    GATHER, REDUCE = (0, 1, 2), (2, 1, 0)

    def up_rows(colour, m, order):
        return pl.ds(pl.multiple_of(chip(colour, m, order) * (3 * rows) + colour * rows, 16), rows)

    def down_rows(colour, m, order):
        return pl.ds(pl.multiple_of(chip(colour, m, order) * units, 16), units)

    def down_cols(colour):
        return pl.ds(colour * cols, cols)

    def ag_start(n, s, arrays=(0, 1)):
        have = 1 << s
        for k in range(COLOURS):
            for i in arrays:
                buf = (a1, a2)[i]
                pltpu.make_async_remote_copy(
                    src_ref=buf.at[n, k, pl.ds(0, have)], dst_ref=buf.at[n, k, pl.ds(have, have)],
                    send_sem=ag_send.at[i, s, n], recv_sem=ag_recv.at[i, s, n],
                    device_id=(near[(k + s) % 3],), device_id_type=MESH).start()

    one_array = (rc1, rb1, ra1)
    sized = (rb1, ra1, p1)

    def ag_wait(n, s, arrays=(0, 1)):
        for i in arrays:
            wait_for(one_array[s].at[n], ag_recv.at[i, s, n])

    def rs_start(n, s, k, src1, src2):
        dst1, dst2 = ((ra1, ra2), (rb1, rb2), (rc1, rc2))[s]
        for src, dst in ((src1, dst1), (src2, dst2)):
            pltpu.make_async_remote_copy(
                src_ref=src, dst_ref=dst.at[n, k], send_sem=rs_send.at[s, n], recv_sem=rs_recv.at[s, n],
                device_id=(near[(k + s) % 3],), device_id_type=MESH).start()

    def rs_wait(n, s):
        wait_for(sized[2 - s].at[n], rs_recv.at[s, n])

    barrier = pltpu.get_barrier_semaphore()
    for other in (partner, *near):
        pl.semaphore_signal(barrier, inc=1, device_id=(other,), device_id_type=MESH)

    def to_partner(src, dst, i):
        pltpu.make_async_remote_copy(
            src_ref=src, dst_ref=dst, send_sem=pair_send.at[i], recv_sem=pair_recv.at[i],
            device_id=(partner,), device_id_type=MESH).start()

    mine = pl.ds(pl.multiple_of(core * tokens, 16), tokens)
    theirs = pl.ds(pl.multiple_of((1 - core) * tokens, 16), tokens)

    def c_load(n, c1, c2, sem):
        with jax.named_scope("wait_rs0"):
            rs_wait(n, 0)
        for i, (b1, b2) in enumerate(((p1, p2), (ra1, ra2))):
            for k in range(COLOURS):
                pair = pl.ds(2 * (3 * i + k), 2)
                copy(b1.at[n, k, pl.ds(2, 2)], c1.at[pair], sem).start()
                copy(b2.at[n, k, pl.ds(2, 2)], c2.at[pair], sem).start()

    def c_sum(c1, c2, to1, to2, sem):
        wait_for(p1.at[0], sem)
        for k in range(COLOURS):
            for j in range(2):
                to1[k, j] = c1[2 * k + j] + c1[2 * k + j + 6]
                to2[k, j] = c2[2 * k + j] + c2[2 * k + j + 6]

    def main(x, dy, w1, w2, ud, at, s1, s2, c1, c2, co1, co2):
        own_down = x.at[pl.ds(0, nc * units)]
        blocks = up_hbm.shape[1] // width
        for b in range(blocks):
            copy(up_hbm.at[:, pl.ds(b * width, width)], x.at[pl.ds(nc * units + b * half, half)], local.at[UP_IN]).start()
        copy(down_hbm, own_down, local.at[X_IN]).start()
        wait_for(up_hbm, local.at[UP_IN])

        def unit(chip_, core_, n):
            first = ((chip_ * CORES + core_) * nc + n) * units
            b, c = first // width, first % width
            return x[nc * units + b * half:nc * units + (b + 1) * half, c:c + units]

        whole = pl.ds(pl.multiple_of(core * third, 16), 2 * third)
        rest = pl.ds(pl.multiple_of((1 - core) * 2 * third, 16), third)
        to_rest = pl.ds(pl.multiple_of(core * third, 16), third)

        def permute(n):
            for c in range(CORES):
                first = (n * CORES + c) * half
                ud[first:first + half, :] = jnp.concatenate([unit(r, c, n) for r in range(CHIPS)], axis=1)

        def own_up(n):
            def part(c, which):
                return ud.at[pl.ds(pl.multiple_of((n * CORES + c) * half + which.start, 16), which.size)]

            sem = min(n, 1)
            for which, dst in ((whole, a1.at[n, 2 * core, 0]), (rest, a1.at[n, 1, 0, to_rest])):
                pltpu.make_async_remote_copy(
                    src_ref=part(1 - core, which), dst_ref=dst, send_sem=pair_send.at[0], recv_sem=pair_recv.at[3 * sem],
                    device_id=(partner,), device_id_type=MESH).start()
                copy(part(core, which), dst, local.at[OWN_0 + sem]).start()

        def down_own(n):
            for k in range(COLOURS):
                copy(x.at[pl.ds(n * units, units), down_cols(k)], a2.at[n, k, 0], local.at[OWN_2 if n else X_IN]).start()

        permute(0)
        with jax.named_scope("entry"):
            pl.semaphore_wait(barrier, 4)
        own_up(0)
        for k in range(COLOURS):
            pltpu.make_async_remote_copy(
                src_ref=down_hbm.at[pl.ds(0, units), down_cols(k)], dst_ref=a2.at[0, k, 1],
                send_sem=ag_send.at[1, 0, 0], recv_sem=ag_recv.at[1, 0, 0],
                device_id=(near[k],), device_id_type=MESH).start()
        wait_for(down_hbm, local.at[X_IN])
        down_own(0)
        for n in range(1, nc):
            permute(n)
        for n in range(1, nc):
            down_own(n)
            own_up(n)
        to_partner(x_hbm, xr_hbm, 1)
        to_partner(dy_hbm, dyr_hbm, 2)
        with jax.named_scope("own_wait"):
            wait_for(down_hbm.at[pl.ds(0, units)], local.at[X_IN])
            wait_for(du_hbm.at[0, pl.ds(0, half)], local.at[OWN_0])
            wait_for(du_hbm.at[0, pl.ds(0, half)], pair_recv.at[0])
        ag_start(0, 0, (0,))
        wait_for(down_hbm.at[pl.ds(0, (nc - 1) * units)], local.at[OWN_2])
        copy(x_hbm, x.at[mine], local.at[X_IN]).start()
        copy(dy_hbm, dy.at[mine], local.at[DY_IN]).start()
        for s in range(2):
            for i in range(2):
                with jax.named_scope(f"ag0{s}{i}"):
                    ag_wait(0, s, (i,))
                ag_start(0, s + 1, (i,))
        wait_for(du_hbm.at[0, pl.ds(0, (nc - 1) * half)], local.at[OWN_1])
        wait_for(du_hbm.at[0, pl.ds(0, (nc - 1) * half)], pair_recv.at[3])
        ag_start(1, 0)
        with jax.named_scope("xr"):
            wait_for(xr_hbm, pair_recv.at[1])
        copy(xr_hbm, x.at[theirs], local.at[X_IN]).start()

        def load_up(n):
            for k in range(COLOURS):
                for m in range(CHIPS):
                    copy(a1.at[n, k, m], w1.at[up_rows(k, m, GATHER)], local.at[W1_IN]).start()

        def load_down(n):
            for k in range(COLOURS):
                for m in range(CHIPS):
                    copy(a2.at[n, k, m], w2.at[down_rows(k, m, GATHER), down_cols(k)], local.at[W2_IN]).start()

        with jax.named_scope("ag020"):
            ag_wait(0, 2, (0,))
        load_up(0)
        with jax.named_scope("tokens"):
            wait_for(x, local.at[X_IN])
            wait_for(du_hbm.at[0, pl.ds(0, nc * half)], pair_send.at[0])

        def send_first(src, dst, n):
            for k in range(COLOURS):
                pltpu.make_async_remote_copy(
                    src_ref=src.at[n, k, pl.ds(4, 4)], dst_ref=dst.at[n, k], send_sem=rs_send.at[0, n],
                    recv_sem=rs_recv.at[0, n], device_id=(near[k],), device_id_type=MESH).start()

        def send_both(n):
            wait_for(p2.at[0], local.at[G2_OUT])
            send_first(p2, ra2, n)
            wait_for(p1.at[0], local.at[G1_OUT])
            send_first(p1, ra1, n)

        def c_in(n):
            c_load(n, c1, c2, local.at[SUM_IN])

        def c_add(n):
            c_sum(c1, c2, co1, co2, local.at[SUM_IN])
            copy(co1, cb1.at[n], local.at[SUM_OUT]).start()
            copy(co2, cb2.at[n], local.at[SUM_OUT]).start()

        def c_go(n):
            wait_for(sized[1].at[0], local.at[SUM_OUT])
            for k in range(COLOURS):
                rs_start(n, 1, k, cb1.at[n, k], cb2.at[n, k])

        up_tile = both // UP_TILES

        def chunk(n, carry):
            size = up_tile // PARTS
            strip = min(128, size)

            def use(first, u, da):
                for c in range(0, fc, 128):
                    lanes = slice(c, c + 128)
                    for r in range(0, size, strip):
                        at_r = pl.ds(pl.multiple_of(first + r, strip), strip)
                        a, slope = gelu_both(u(r, at_r, lanes).astype(F32))
                        ud[at_r, lanes] = (da[r:r + strip, lanes] * slope).astype(BF16)
                        at[lanes, at_r] = a.astype(BF16).T

            def da_of(at_t):
                return lax.dot_general(dy[at_t, :], w2[...], (((1,), (1,)), ((), ())), preferred_element_type=F32)

            with jax.named_scope("wait_w1"):
                wait_for(w1, local.at[W1_IN])

            @pl.when(n == 0)
            def _():
                def u_step(t, carry):
                    at_t = pl.ds(pl.multiple_of(t * 2 * up_tile, up_tile), 2 * up_tile)
                    ud[at_t, :] = jnp.dot(x[at_t, :], w1[...], preferred_element_type=F32).astype(BF16)
                    return carry

                with jax.named_scope("u0"):
                    lax.fori_loop(0, UP_TILES // 2, u_step, 0)
                with jax.named_scope("wait_100"):
                    ag_wait(1, 0, (0,))
                ag_start(1, 1, (0,))
                with jax.named_scope("first_w2"):
                    wait_for(dyr_hbm, pair_recv.at[2])
                    copy(dyr_hbm, dy.at[theirs], local.at[DY_IN]).start()
                    ag_wait(0, 2, (1,))
                    load_down(0)
                    wait_for(dy, local.at[DY_IN])
                    wait_for(w2, local.at[W2_IN])

                def da_step(t, carry):
                    for part in range(PARTS):
                        first = t * up_tile + part * size
                        da = da_of(pl.ds(pl.multiple_of(first, size), size))
                        use(first, lambda r, at_r, lanes: ud[at_r, lanes], da)

                    for when, s, i in ((0, 0, 1), (3, 1, 0), (6, 1, 1)):
                        @pl.when(t == when)
                        def _(s=s, i=i):
                            with jax.named_scope(f"wait_1{s}{i}"):
                                ag_wait(1, s, (i,))
                            ag_start(1, s + 1, (i,))

                    return carry

                with jax.named_scope("da0"):
                    lax.fori_loop(0, UP_TILES, da_step, 0)
                ag_start(2, 0)
                ag_start(3, 0)

            def up_step(t, carry):
                for part in range(PARTS):
                    first = t * up_tile + part * size
                    at_t = pl.ds(pl.multiple_of(first, size), size)
                    u = jnp.dot(x[at_t, :], w1[...], preferred_element_type=F32).astype(BF16)
                    da = da_of(at_t)
                    use(first, lambda r, at_r, lanes, u=u: u[r:r + strip, lanes], da)

                @pl.when(t == 4)
                def _():
                    @pl.when(n + 1 < nc)
                    def _():
                        with jax.named_scope("wait_ag1"):
                            ag_wait(n + 1, 1)
                        ag_start(n + 1, 2)

                    @pl.when(n + 2 < nc)
                    def _():
                        with jax.named_scope("wait_ag0"):
                            ag_wait(n + 2, 0)
                        ag_start(n + 2, 1)

                    @pl.when(n + 3 < nc)
                    def _():
                        ag_start(n + 3, 0)

                    send_both(n - 1)

                @pl.when((t == 6) & (n == nc - 1))
                def _():
                    c_go(0)
                    c_add(1)
                    c_in(2)

                return carry

            @pl.when(n > 0)
            def _():
                with jax.named_scope("wait_w2"):
                    wait_for(w2, local.at[W2_IN])
                with jax.named_scope("up"):
                    lax.fori_loop(0, UP_TILES, up_step, 0)

            copy(ud, du_hbm.at[n], local.at[DU_OUT]).start()

            @pl.when(n == nc - 1)
            def _():
                c_go(1)
                c_add(2)
                c_in(3)

            def down_grad(k, carry):
                part = pl.ds(pl.multiple_of(k * cols, cols), cols)
                s2[:, part] = jnp.dot(at[...], dy[:, part], preferred_element_type=F32).astype(BF16)
                return carry

            with jax.named_scope("down_grad"):
                lax.fori_loop(0, 3, down_grad, 0)
            for k in range(COLOURS):
                for m in range(CHIPS):
                    copy(s2.at[down_rows(k, m, REDUCE), down_cols(k)], p2.at[n, k, m], local.at[G2_OUT]).start()

            @pl.when(n == nc - 2)
            def _():
                c_in(0)

            @pl.when(n == nc - 1)
            def _():
                c_go(2)
                c_add(3)

            def up_grad(k, carry):
                part = pl.ds(pl.multiple_of(k * cols, cols), cols)

                @pl.when((k == 2) & (n + 1 < nc))
                def _():
                    with jax.named_scope("wait_ag2"):
                        ag_wait(n + 1, 2)
                    load_up(n + 1)
                    load_down(n + 1)

                s1[part, :] = lax.dot_general(
                    x[:, part], ud[...], (((0,), (0,)), ((), ())), preferred_element_type=F32).astype(BF16)
                return carry

            with jax.named_scope("up_grad"):
                lax.fori_loop(0, 3, up_grad, 0)
            for k in range(COLOURS):
                for m in range(CHIPS):
                    copy(s1.at[up_rows(k, m, REDUCE)], p1.at[n, k, m], local.at[G1_OUT]).start()

            @pl.when(n == 0)
            def _():
                with jax.named_scope("wait_20"):
                    ag_wait(2, 0)
                ag_start(2, 1)

            @pl.when(n == nc - 2)
            def _():
                c_add(0)
                c_in(1)

            @pl.when(n == nc - 1)
            def _():
                c_go(3)

            wait_for(ud, local.at[DU_OUT])
            return carry

        lax.fori_loop(0, nc, chunk, 0)
        send_both(nc - 1)

    pl.run_scoped(
        main,
        pltpu.VMEM((both, width), BF16), pltpu.VMEM((both, width), BF16),
        pltpu.VMEM((width, fc), BF16), pltpu.VMEM((fc, width), BF16),
        pltpu.VMEM((both, fc), BF16), pltpu.VMEM((fc, both), BF16),
        pltpu.VMEM((width, fc), BF16), pltpu.VMEM((fc, width), BF16),
        pltpu.VMEM((12, rows, fc), BF16), pltpu.VMEM((12, units, cols), BF16),
        pltpu.VMEM((3, 2, rows, fc), BF16), pltpu.VMEM((3, 2, units, cols), BF16))

    dx_tile = both // DX_TILES
    half_tiles = DX_TILES // 2
    steps = 3 * DX_TILES
    own_from = 3 * half_tiles
    hidden = nc * fc

    def last(w, du, wide, out16, res,
             co1, co2, do1, do2, e1, e2, eo1, eo2):
        def load_w(n, third_):
            for p in range(8):
                r, k = divmod(8 * third_ + p, 3)
                m = 0
                for i in range(3):
                    d = (k + i) % 3
                    m = m + (1 << i) * ((1 - bits[d]) if (r >> d) & 1 else bits[d])
                copy(a1.at[n, k, m], w.at[pl.ds((8 * third_ + p) * rows, rows), pl.ds(pl.multiple_of(n * fc, fc), fc)],
                     w_sem.at[third_]).start()

        def tokens_at(q):
            later = q // half_tiles
            owner = (1 - later) * (1 - core) + later * core
            return pl.multiple_of(owner * tokens + (q % half_tiles) * dx_tile, dx_tile)

        def load_du(q):
            slot = q % 2
            for n in range(nc):
                copy(du_hbm.at[n, pl.ds(tokens_at(q), dx_tile)], du.at[slot, :, pl.ds(n * fc, fc)], local.at[TILE_IN + slot]).start()

        for third_ in range(3):
            lax.fori_loop(0, nc, lambda n, carry, third_=third_: (load_w(n, third_), carry)[1], 0)
            if third_ == 0:
                load_du(0)

        def own_at(q, n):
            return (pl.ds(pl.multiple_of((q % half_tiles) * dx_tile, dx_tile), dx_tile), pl.ds(pl.multiple_of(n * cols, cols), cols))

        def c_in(n):
            c_load(n, e1, e2, local.at[C_IN])

        def c_send(n):
            to1, to2 = co1.at[n - EARLY], co2.at[n - EARLY]
            c_sum(e1, e2, to1, to2, local.at[C_IN])
            for k in range(COLOURS):
                rs_start(n, 1, k, to1.at[k], to2.at[k])

        def sum_of(e, k, terms):
            total = e[k].astype(F32)
            for i in range(1, terms):
                total = total + e[3 * i + k].astype(F32)
            return total.astype(BF16)

        def d_load(n):
            with jax.named_scope("wait_rs1"):
                rs_wait(n, 1)
            for i, (b1, b2) in enumerate(((p1, p2), (ra1, ra2), (rb1, rb2))):
                for k in range(COLOURS):
                    copy(b1.at[n, k, 1], e1.at[3 * i + k], local.at[D_IN]).start()
                    copy(b2.at[n, k, 1], e2.at[3 * i + k], local.at[D_IN]).start()

        def d_send(n):
            wait_for(e1.at[pl.ds(0, 9)], local.at[D_IN])
            wait_for(e2.at[pl.ds(0, 9)], local.at[D_IN])

            for k in range(COLOURS):
                do1[n, k] = sum_of(e1, k, 3)
                do2[n, k] = sum_of(e2, k, 3)
                rs_start(n, 2, k, do1.at[n, k], do2.at[n, k])

        def e_load(n):
            with jax.named_scope("wait_rs2"):
                rs_wait(n, 2)
            for i, (b1, b2) in enumerate(((p1, p2), (ra1, ra2), (rb1, rb2))):
                for k in range(COLOURS):
                    copy(b1.at[n, k, 0], e1.at[3 * i + k], local.at[E_IN]).start()
                    copy(b2.at[n, k, 0], e2.at[3 * i + k], local.at[E_IN]).start()
            copy(rc1.at[n], e1.at[pl.ds(9, 3)], local.at[E_IN]).start()
            copy(rc2.at[n], e2.at[pl.ds(9, 3)], local.at[E_IN]).start()

        keep = pl.ds(pl.multiple_of(core * half, 16), half)
        give = pl.ds(pl.multiple_of((1 - core) * half, 16), half)

        def e_wait_out(n):
            wait_for(gup_hbm.at[0, 0], local.at[GUP_OUT])
            wait_for(gdown_hbm.at[pl.ds(0, units)], local.at[GDOWN_OUT])
            wait_for(gup_hbm.at[0, 0], gup_send.at[n])

        def e_store(n):
            wait_for(e1, local.at[E_IN])
            wait_for(e2, local.at[E_IN])

            @pl.when(n > 0)
            def _():
                e_wait_out(n - 1)

            for k in range(COLOURS):
                eo1[k * rows:(k + 1) * rows, :] = sum_of(e1, k, 4)
                eo2[:, k * cols:(k + 1) * cols] = sum_of(e2, k, 4)
            copy(eo1.at[keep], gup_hbm.at[core, n], local.at[GUP_OUT]).start()
            copy(eo2, gdown_hbm.at[pl.ds(pl.multiple_of(n * units, 16), units)], local.at[GDOWN_OUT]).start()
            pltpu.make_async_remote_copy(
                src_ref=eo1.at[give], dst_ref=gup_hbm.at[core, n], send_sem=gup_send.at[n], recv_sem=gup_recv.at[n],
                device_id=(partner,), device_id_type=MESH).start()

        def pump(i):
            for start, low, load, finish_ in ((0, EARLY, c_in, c_send), (6, 0, d_load, d_send), (15, 0, e_load, e_store)):
                n = i - start + low

                @pl.when((n > low) & (n <= nc))
                def _(finish_=finish_, n=n):
                    finish_(n - 1)

                @pl.when((n >= low) & (n < nc))
                def _(load=load, n=n):
                    load(n)

        def step(i, carry):
            q, n = i // 3, i % 3
            slot = i % 2

            @pl.when((i < steps) & (n == 0))
            def _():
                @pl.when(q + 1 < DX_TILES)
                def _():
                    load_du(q + 1)

                with jax.named_scope("wait_du"):
                    wait_for(du.at[0], local.at[TILE_IN + q % 2])

            @pl.when(i < 3)
            def _():
                with jax.named_scope("wait_wall"):
                    wait_for(w.at[pl.ds(0, cols)], w_sem.at[n])

            @pl.when((i >= own_from - 1) & (i < steps - 1))
            def _():
                here = own_at((i + 1) // 3, (i + 1) % 3)
                with jax.named_scope("wait_dxr"):
                    wait_for(dxr_hbm.at[here], dx_recv.at[i + 1 - own_from])

                @pl.when(i < own_from + 2)
                def _():
                    wait_for(wide.at[0], dx_send.at[i - 2])

                copy(dxr_hbm.at[here], wide.at[(i + 1) % 3], local.at[GOT_IN + 1 - slot]).start()
                copy(dy_hbm.at[here], res.at[1 - slot], local.at[RES_IN + 1 - slot]).start()

            @pl.when((i >= 3) & (i < own_from))
            def _():
                with jax.named_scope("wait_dxs"):
                    wait_for(wide.at[0], dx_send.at[i - 3])

            @pl.when((i >= own_from + 2) & (i < steps))
            def _():
                wait_for(out16.at[0], local.at[DX_OUT + slot])

            def dot():
                part = pl.ds(pl.multiple_of(n * cols, cols), cols)
                return lax.dot_general(du[q % 2], w[part, :], (((1,), (1,)), ((), ())), preferred_element_type=F32)

            @pl.when(i < own_from)
            def _():
                with jax.named_scope("dx_dot"):
                    wide[i % 3] = dot()
                pltpu.make_async_remote_copy(
                    src_ref=wide.at[i % 3], dst_ref=dxr_hbm.at[own_at(q, n)], send_sem=dx_send.at[i], recv_sem=dx_recv.at[i],
                    device_id=(partner,), device_id_type=MESH).start()

            @pl.when((i >= own_from) & (i < steps))
            def _():
                with jax.named_scope("wait_got"):
                    wait_for(wide.at[0], local.at[GOT_IN + slot])
                    wait_for(res.at[0], local.at[RES_IN + slot])
                with jax.named_scope("dx_dot2"):
                    out16[slot] = (res[slot].astype(F32) + (dot() + wide[i % 3])).astype(BF16)
                copy(out16.at[slot], dx_hbm.at[own_at(q, n)], local.at[DX_OUT + slot]).start()

            pump(i)
            return carry

        lax.fori_loop(0, max(steps, nc + 16), step, 0)
        for slot in range(2):
            wait_for(out16.at[0], local.at[DX_OUT + slot])
        e_wait_out(nc - 1)
        for n in range(nc):
            wait_for(sized[1].at[0], rs_send.at[1, n])
            wait_for(sized[0].at[0], rs_send.at[2, n])

    pl.run_scoped(
        last,
        pltpu.VMEM((width, hidden), BF16), pltpu.VMEM((2, dx_tile, hidden), BF16),
        pltpu.VMEM((3, dx_tile, cols), F32), pltpu.VMEM((2, dx_tile, cols), BF16), pltpu.VMEM((2, dx_tile, cols), BF16),
        pltpu.VMEM((nc - EARLY, 3, 2, rows, fc), BF16), pltpu.VMEM((nc - EARLY, 3, 2, units, cols), BF16),
        pltpu.VMEM((nc, 3, rows, fc), BF16), pltpu.VMEM((nc, 3, units, cols), BF16),
        pltpu.VMEM((12, rows, fc), BF16), pltpu.VMEM((12, units, cols), BF16),
        pltpu.VMEM((3 * rows, fc), BF16), pltpu.VMEM((units, width), BF16))

    def drain(n, carry):
        for s in range(3):
            for i in range(2):
                wait_for(one_array[s].at[n], ag_send.at[i, s, n])
        wait_for(sized[2].at[n], rs_send.at[0, n])
        wait_for(gup_hbm.at[0, 0], gup_recv.at[n])
        return carry

    with jax.named_scope("drain"):
        lax.fori_loop(0, nc, drain, 0)
    wait_for(xr_hbm, pair_send.at[1])
    wait_for(dyr_hbm, pair_send.at[2])


def finish(nc, units, gup, gdown, dx, gup_out, gdown_out, dx_out, v_in, v_out, v_down, v_dx, sem_in, sem_out):
    pieces = v_dx.shape[0]
    rows = v_dx.shape[1]
    copy(gup, v_in, sem_in.at[pieces]).start()
    copy(gdown, v_down, sem_in.at[pieces + 1]).start()
    for i in range(pieces):
        copy(dx.at[pl.ds(i * rows, rows)], v_dx.at[i], sem_in.at[i]).start()
    copy(gup, v_in, sem_in.at[pieces]).wait()
    per = 128 // math.gcd(128, units)
    for first in range(0, CHIPS * CORES * nc, per):
        parts = []
        for u in range(first, first + per):
            d, n = u // nc, u % nc
            r, c = d // CORES, d % CORES
            parts.append(v_in[c, n, :, r * units:(r + 1) * units])
        v_out[:, first * units:(first + per) * units] = jnp.concatenate(parts, axis=1)
    copy(v_out, gup_out, sem_out.at[pieces]).start()
    copy(gdown, v_down, sem_in.at[pieces + 1]).wait()
    copy(v_down, gdown_out, sem_out.at[pieces + 1]).start()
    for i in range(pieces):
        copy(dx.at[pl.ds(i * rows, rows)], v_dx.at[i], sem_in.at[i]).wait()
        copy(v_dx.at[i], dx_out.at[pl.ds(i * rows, rows)], sem_out.at[i]).start()
    copy(v_out, gup_out, sem_out.at[pieces]).wait()
    copy(v_down, gdown_out, sem_out.at[pieces + 1]).wait()
    for i in range(pieces):
        copy(v_dx.at[i], dx_out.at[pl.ds(i * rows, rows)], sem_out.at[i]).wait()


def chunks_of(units):
    return 9 if units % 144 == 0 else 1


def solution(mesh):
    def device_fn(x_loc, dy_loc, up_loc, down_loc):
        width = x_loc.shape[-1]
        x = x_loc.reshape(-1, width)
        dy = dy_loc.reshape(-1, width)
        tokens = x.shape[0]
        down = down_loc[0]
        half, units_all = up_loc.shape[1], down.shape[0]
        nc = chunks_of(units_all)
        units = units_all // nc
        fc = CHIPS * units
        rows, cols = 2 * half // 3, width // 3
        up = up_loc[0]

        def hbm(*shape, dtype=BF16):
            return jax.ShapeDtypeStruct(shape, dtype)

        one, two = (rows, fc), (units, cols)
        outs = [
            hbm(CORES, nc, half, fc), hbm(units_all, width), hbm(tokens, width),
            hbm(tokens, width), hbm(tokens, width),
            *[hbm(nc, 3, blocks, *s) for blocks in (8, 8, 4, 2) for s in (one, two)],
            hbm(nc, 3, *one), hbm(nc, 3, *two), hbm(nc, 3, 2, *one), hbm(nc, 3, 2, *two),
            hbm(nc, 2 * tokens, fc), hbm(tokens, width, dtype=F32),
        ]
        dma = pltpu.SemaphoreType.DMA
        half_steps = 3 * DX_TILES // 2
        got = pl.pallas_call(
            functools.partial(kernel, nc),
            out_shape=outs,
            in_specs=[pl.BlockSpec(memory_space=pl.ANY)] * 4,
            out_specs=[pl.BlockSpec(memory_space=pl.ANY)] * len(outs),
            scratch_shapes=[
                dma((2, 3, nc)), dma((2, 3, nc)), dma((3, nc)), dma((3, nc)), dma((3,)), dma((4,)),
                dma((half_steps,)), dma((half_steps,)), dma((nc,)), dma((nc,)), dma((3,)), dma((13,)),
            ],
            compiler_params=pltpu.CompilerParams(
                collective_id=0, has_side_effects=True, vmem_limit_bytes=67_000_000),
        )(x, dy, up, down)
        pieces = 8
        g_up, g_down, dx = pl.pallas_call(
            functools.partial(finish, nc, units),
            out_shape=[hbm(half, up.shape[1]), hbm(units_all, width), hbm(tokens, width)],
            in_specs=[pl.BlockSpec(memory_space=pl.ANY)] * 3,
            out_specs=[pl.BlockSpec(memory_space=pl.ANY)] * 3,
            scratch_shapes=[
                pltpu.VMEM((CORES, nc, half, fc), BF16), pltpu.VMEM((half, up.shape[1]), BF16),
                pltpu.VMEM((units_all, width), BF16), pltpu.VMEM((pieces, tokens // pieces, width), BF16),
                dma((pieces + 2,)), dma((pieces + 2,)),
            ],
            compiler_params=pltpu.CompilerParams(vmem_limit_bytes=67_000_000),
        )(*got[:3])
        return g_up[None], g_down[None], dx.reshape(x_loc.shape)

    return jax.shard_map(
        device_fn, mesh=mesh, in_specs=(P("data"), P("data"), P(None, "data"), P(None, "data")),
        out_specs=(P(None, "data"), P(None, "data"), P("data")), check_vma=False)
```

```python
import functools
import math

import jax
import jax.numpy as jnp
from jax import lax
from jax.experimental import pallas as pl
from jax.experimental.pallas import tpu as pltpu
from jax.sharding import PartitionSpec as P

MESH = pl.DeviceIdType.MESH
F32, BF16 = jnp.float32, jnp.bfloat16
CHIPS, COLOURS, CORES = 8, 3, 2
DX_TILES = 8
UP_TILES = 8
PARTS = 2
UP_IN, X_IN, DY_IN, W1_IN, W2_IN, G1_OUT, G2_OUT, DU_OUT, SUM_IN, SUM_OUT, OWN_0, OWN_1, OWN_2 = range(13)
TILE_IN, GOT_IN, RES_IN, DX_OUT = range(0, 8, 2)
C_IN, D_IN, E_IN, GUP_OUT, GDOWN_OUT = range(8, 13)
EARLY = 4


def copy(src, dst, sem):
    return pltpu.make_async_copy(src, dst, sem)


def wait_for(ref, sem):
    pltpu.make_async_copy(ref, ref, sem).wait()


def gelu_both(u):
    scale = math.sqrt(2.0 / math.pi)
    square = u * u
    th = jnp.tanh(u * (scale + (0.044715 * scale) * square))
    half = 0.5 * th
    cdf = 0.5 + half
    slope = cdf + (u * (0.5 - th * half)) * (scale + (0.134145 * scale) * square)
    return u * cdf, slope


def kernel(nc, x_hbm, dy_hbm, up_hbm, down_hbm,
           gup_hbm, gdown_hbm, dx_hbm,
           xr_hbm, dyr_hbm, a1, a2, p1, p2, ra1, ra2, rb1, rb2, rc1, rc2, cb1, cb2, du_hbm, dxr_hbm,
           ag_send, ag_recv, rs_send, rs_recv, pair_send, pair_recv, dx_send, dx_recv, gup_send, gup_recv, w_sem, local):
    me = lax.axis_index("data")
    core = me % 2
    bits = [(me // 2) % 2, (me // 4) % 2, (me // 8) % 2]
    partner = me + 1 - 2 * core
    near = [me + (2 << d) * (1 - 2 * bits[d]) for d in range(3)]

    tokens, width = x_hbm.shape
    both = 2 * tokens
    rows = a1.shape[3]
    fc = a1.shape[4]
    units = a2.shape[3]
    cols = a2.shape[4]
    half = up_hbm.shape[0]
    third = half // 3

    def chip(colour, m, order):
        total = 0
        for i in range(3):
            d = (colour + i) % 3
            flipped = (m >> order[i]) & 1
            total = total + (1 << d) * ((1 - bits[d]) if flipped else bits[d])
        return total

    GATHER, REDUCE = (0, 1, 2), (2, 1, 0)

    def up_rows(colour, m, order):
        return pl.ds(pl.multiple_of(chip(colour, m, order) * (3 * rows) + colour * rows, 16), rows)

    def down_rows(colour, m, order):
        return pl.ds(pl.multiple_of(chip(colour, m, order) * units, 16), units)

    def down_cols(colour):
        return pl.ds(colour * cols, cols)

    def ag_start(n, s, arrays=(0, 1)):
        have = 1 << s
        for k in range(COLOURS):
            for i in arrays:
                buf = (a1, a2)[i]
                pltpu.make_async_remote_copy(
                    src_ref=buf.at[n, k, pl.ds(0, have)], dst_ref=buf.at[n, k, pl.ds(have, have)],
                    send_sem=ag_send.at[i, s, n], recv_sem=ag_recv.at[i, s, n],
                    device_id=(near[(k + s) % 3],), device_id_type=MESH).start()

    one_array = (rc1, rb1, ra1)
    sized = (rb1, ra1, p1)

    def ag_wait(n, s, arrays=(0, 1)):
        for i in arrays:
            wait_for(one_array[s].at[n], ag_recv.at[i, s, n])

    def rs_start(n, s, k, src1, src2):
        dst1, dst2 = ((ra1, ra2), (rb1, rb2), (rc1, rc2))[s]
        for src, dst in ((src1, dst1), (src2, dst2)):
            pltpu.make_async_remote_copy(
                src_ref=src, dst_ref=dst.at[n, k], send_sem=rs_send.at[s, n], recv_sem=rs_recv.at[s, n],
                device_id=(near[(k + s) % 3],), device_id_type=MESH).start()

    def rs_wait(n, s):
        wait_for(sized[2 - s].at[n], rs_recv.at[s, n])

    barrier = pltpu.get_barrier_semaphore()
    for other in (partner, *near):
        pl.semaphore_signal(barrier, inc=1, device_id=(other,), device_id_type=MESH)

    def to_partner(src, dst, i):
        pltpu.make_async_remote_copy(
            src_ref=src, dst_ref=dst, send_sem=pair_send.at[i], recv_sem=pair_recv.at[i],
            device_id=(partner,), device_id_type=MESH).start()

    mine = pl.ds(pl.multiple_of(core * tokens, 16), tokens)
    theirs = pl.ds(pl.multiple_of((1 - core) * tokens, 16), tokens)

    def c_load(n, c1, c2, sem):
        with jax.named_scope("wait_rs0"):
            rs_wait(n, 0)
        for i, (b1, b2) in enumerate(((p1, p2), (ra1, ra2))):
            for k in range(COLOURS):
                pair = pl.ds(2 * (3 * i + k), 2)
                copy(b1.at[n, k, pl.ds(2, 2)], c1.at[pair], sem).start()
                copy(b2.at[n, k, pl.ds(2, 2)], c2.at[pair], sem).start()

    def c_sum(c1, c2, to1, to2, sem):
        wait_for(p1.at[0], sem)
        for k in range(COLOURS):
            for j in range(2):
                to1[k, j] = c1[2 * k + j] + c1[2 * k + j + 6]
                to2[k, j] = c2[2 * k + j] + c2[2 * k + j + 6]

    def main(x, dy, w1, w2, ud, at, s1, s2, c1, c2, co1, co2):
        own_down = x.at[pl.ds(0, nc * units)]
        blocks = up_hbm.shape[1] // width
        for b in range(blocks):
            copy(up_hbm.at[:, pl.ds(b * width, width)], x.at[pl.ds(nc * units + b * half, half)], local.at[UP_IN]).start()
        copy(down_hbm, own_down, local.at[X_IN]).start()
        wait_for(up_hbm, local.at[UP_IN])

        def unit(chip_, core_, n):
            first = ((chip_ * CORES + core_) * nc + n) * units
            b, c = first // width, first % width
            return x[nc * units + b * half:nc * units + (b + 1) * half, c:c + units]

        whole = pl.ds(pl.multiple_of(core * third, 16), 2 * third)
        rest = pl.ds(pl.multiple_of((1 - core) * 2 * third, 16), third)
        to_rest = pl.ds(pl.multiple_of(core * third, 16), third)

        def permute(n):
            for c in range(CORES):
                first = (n * CORES + c) * half
                ud[first:first + half, :] = jnp.concatenate([unit(r, c, n) for r in range(CHIPS)], axis=1)

        def own_up(n):
            def part(c, which):
                return ud.at[pl.ds(pl.multiple_of((n * CORES + c) * half + which.start, 16), which.size)]

            sem = min(n, 1)
            for which, dst in ((whole, a1.at[n, 2 * core, 0]), (rest, a1.at[n, 1, 0, to_rest])):
                pltpu.make_async_remote_copy(
                    src_ref=part(1 - core, which), dst_ref=dst, send_sem=pair_send.at[0], recv_sem=pair_recv.at[3 * sem],
                    device_id=(partner,), device_id_type=MESH).start()
                copy(part(core, which), dst, local.at[OWN_0 + sem]).start()

        def down_own(n):
            for k in range(COLOURS):
                copy(x.at[pl.ds(n * units, units), down_cols(k)], a2.at[n, k, 0], local.at[OWN_2 if n else X_IN]).start()

        permute(0)
        with jax.named_scope("entry"):
            pl.semaphore_wait(barrier, 4)
        own_up(0)
        for k in range(COLOURS):
            pltpu.make_async_remote_copy(
                src_ref=down_hbm.at[pl.ds(0, units), down_cols(k)], dst_ref=a2.at[0, k, 1],
                send_sem=ag_send.at[1, 0, 0], recv_sem=ag_recv.at[1, 0, 0],
                device_id=(near[k],), device_id_type=MESH).start()
        wait_for(down_hbm, local.at[X_IN])
        for n in range(nc):
            down_own(n)
        for n in range(1, 4):
            permute(n)
        with jax.named_scope("own_wait"):
            wait_for(du_hbm.at[0, pl.ds(0, half)], local.at[OWN_0])
            wait_for(du_hbm.at[0, pl.ds(0, half)], pair_recv.at[0])
        ag_start(0, 0, (0,))
        for n in range(4, nc):
            permute(n)
        for n in range(1, nc):
            own_up(n)
        to_partner(x_hbm, xr_hbm, 1)
        to_partner(dy_hbm, dyr_hbm, 2)
        wait_for(down_hbm.at[pl.ds(0, units)], local.at[X_IN])
        wait_for(down_hbm.at[pl.ds(0, (nc - 1) * units)], local.at[OWN_2])
        ag_start(1, 0, (1,))
        copy(x_hbm, x.at[mine], local.at[X_IN]).start()
        copy(dy_hbm, dy.at[mine], local.at[DY_IN]).start()
        for s in range(2):
            for i in range(2):
                with jax.named_scope(f"ag0{s}{i}"):
                    ag_wait(0, s, (i,))
                ag_start(0, s + 1, (i,))
        wait_for(du_hbm.at[0, pl.ds(0, (nc - 1) * half)], local.at[OWN_1])
        wait_for(du_hbm.at[0, pl.ds(0, (nc - 1) * half)], pair_recv.at[3])
        ag_start(1, 0, (0,))
        ag_start(2, 0)
        with jax.named_scope("xr"):
            wait_for(xr_hbm, pair_recv.at[1])
        copy(xr_hbm, x.at[theirs], local.at[X_IN]).start()

        def load_up(n):
            for k in range(COLOURS):
                for m in range(CHIPS):
                    copy(a1.at[n, k, m], w1.at[up_rows(k, m, GATHER)], local.at[W1_IN]).start()

        def load_down(n):
            for k in range(COLOURS):
                for m in range(CHIPS):
                    copy(a2.at[n, k, m], w2.at[down_rows(k, m, GATHER), down_cols(k)], local.at[W2_IN]).start()

        with jax.named_scope("ag020"):
            ag_wait(0, 2, (0,))
        load_up(0)
        with jax.named_scope("tokens"):
            wait_for(x, local.at[X_IN])
            wait_for(du_hbm.at[0, pl.ds(0, nc * half)], pair_send.at[0])

        def send_first(src, dst, n):
            for k in range(COLOURS):
                pltpu.make_async_remote_copy(
                    src_ref=src.at[n, k, pl.ds(4, 4)], dst_ref=dst.at[n, k], send_sem=rs_send.at[0, n],
                    recv_sem=rs_recv.at[0, n], device_id=(near[k],), device_id_type=MESH).start()

        def send_both(n):
            wait_for(p2.at[0], local.at[G2_OUT])
            send_first(p2, ra2, n)
            wait_for(p1.at[0], local.at[G1_OUT])
            send_first(p1, ra1, n)

        def c_in(n):
            c_load(n, c1, c2, local.at[SUM_IN])

        def c_add(n):
            c_sum(c1, c2, co1, co2, local.at[SUM_IN])
            copy(co1, cb1.at[n], local.at[SUM_OUT]).start()
            copy(co2, cb2.at[n], local.at[SUM_OUT]).start()

        def c_go(n):
            wait_for(sized[1].at[0], local.at[SUM_OUT])
            for k in range(COLOURS):
                rs_start(n, 1, k, cb1.at[n, k], cb2.at[n, k])

        up_tile = both // UP_TILES

        def chunk(n, carry):
            size = up_tile // PARTS
            strip = min(128, size)

            def use(first, u, da):
                for c in range(0, fc, 128):
                    lanes = slice(c, c + 128)
                    for r in range(0, size, strip):
                        at_r = pl.ds(pl.multiple_of(first + r, strip), strip)
                        a, slope = gelu_both(u(r, at_r, lanes).astype(F32))
                        ud[at_r, lanes] = (da[r:r + strip, lanes] * slope).astype(BF16)
                        at[lanes, at_r] = a.astype(BF16).T

            def da_of(at_t):
                return lax.dot_general(dy[at_t, :], w2[...], (((1,), (1,)), ((), ())), preferred_element_type=F32)

            with jax.named_scope("wait_w1"):
                wait_for(w1, local.at[W1_IN])

            @pl.when(n == 0)
            def _():
                def u_step(t, carry):
                    at_t = pl.ds(pl.multiple_of(t * 2 * up_tile, up_tile), 2 * up_tile)
                    ud[at_t, :] = jnp.dot(x[at_t, :], w1[...], preferred_element_type=F32).astype(BF16)

                    @pl.when(t == 1)
                    def _():
                        with jax.named_scope("dyr"):
                            wait_for(dyr_hbm, pair_recv.at[2])
                        copy(dyr_hbm, dy.at[theirs], local.at[DY_IN]).start()

                    @pl.when(t == 2)
                    def _():
                        with jax.named_scope("ag021"):
                            ag_wait(0, 2, (1,))
                        load_down(0)

                    return carry

                with jax.named_scope("u0"):
                    lax.fori_loop(0, UP_TILES // 2, u_step, 0)
                with jax.named_scope("wait_100"):
                    ag_wait(1, 0, (0,))
                ag_start(1, 1, (0,))
                with jax.named_scope("first_w2"):
                    wait_for(dy, local.at[DY_IN])
                    wait_for(w2, local.at[W2_IN])

                def da_step(t, carry):
                    for part in range(PARTS):
                        first = t * up_tile + part * size
                        da = da_of(pl.ds(pl.multiple_of(first, size), size))
                        use(first, lambda r, at_r, lanes: ud[at_r, lanes], da)

                    for when, s, i in ((0, 0, 1), (3, 1, 0), (6, 1, 1)):
                        @pl.when(t == when)
                        def _(s=s, i=i):
                            with jax.named_scope(f"wait_1{s}{i}"):
                                ag_wait(1, s, (i,))
                            ag_start(1, s + 1, (i,))

                    return carry

                with jax.named_scope("da0"):
                    lax.fori_loop(0, UP_TILES, da_step, 0)
                with jax.named_scope("wait_20"):
                    ag_wait(2, 0)
                ag_start(2, 1)
                ag_start(3, 0)

            def up_step(t, carry):
                for part in range(PARTS):
                    first = t * up_tile + part * size
                    at_t = pl.ds(pl.multiple_of(first, size), size)
                    u = jnp.dot(x[at_t, :], w1[...], preferred_element_type=F32).astype(BF16)
                    da = da_of(at_t)
                    use(first, lambda r, at_r, lanes, u=u: u[r:r + strip, lanes], da)

                @pl.when((t == 2) & (n == 1))
                def _():
                    with jax.named_scope("wait_30"):
                        ag_wait(3, 0)
                    ag_start(3, 1)
                    ag_start(4, 0)

                @pl.when(t == 2)
                def _():
                    send_both(n - 1)

                @pl.when((t == 6) & (n == nc - 1))
                def _():
                    c_go(0)
                    c_add(1)
                    c_in(2)

                return carry

            @pl.when(n > 0)
            def _():
                with jax.named_scope("wait_w2"):
                    wait_for(w2, local.at[W2_IN])
                with jax.named_scope("up"):
                    lax.fori_loop(0, UP_TILES, up_step, 0)

            copy(ud, du_hbm.at[n], local.at[DU_OUT]).start()

            @pl.when(n == nc - 1)
            def _():
                c_go(1)
                c_add(2)
                c_in(3)

            def down_grad(k, carry):
                part = pl.ds(pl.multiple_of(k * cols, cols), cols)
                s2[:, part] = jnp.dot(at[...], dy[:, part], preferred_element_type=F32).astype(BF16)
                return carry

            with jax.named_scope("down_grad"):
                lax.fori_loop(0, 3, down_grad, 0)
            for k in range(COLOURS):
                for m in range(CHIPS):
                    copy(s2.at[down_rows(k, m, REDUCE), down_cols(k)], p2.at[n, k, m], local.at[G2_OUT]).start()

            @pl.when((n > 0) & (n + 2 < nc))
            def _():
                with jax.named_scope("wait_ag1"):
                    ag_wait(n + 2, 1)
                ag_start(n + 2, 2)

            @pl.when((n > 0) & (n + 3 < nc))
            def _():
                with jax.named_scope("wait_ag0"):
                    ag_wait(n + 3, 0)
                ag_start(n + 3, 1)

            @pl.when((n > 0) & (n + 4 < nc))
            def _():
                ag_start(n + 4, 0)

            @pl.when(n == nc - 2)
            def _():
                c_in(0)

            @pl.when(n == nc - 1)
            def _():
                c_go(2)
                c_add(3)

            def up_grad(k, carry):
                part = pl.ds(pl.multiple_of(k * cols, cols), cols)

                @pl.when((k == 2) & (n + 1 < nc))
                def _():
                    with jax.named_scope("wait_ag2"):
                        ag_wait(n + 1, 2)
                    load_up(n + 1)
                    load_down(n + 1)

                s1[part, :] = lax.dot_general(
                    x[:, part], ud[...], (((0,), (0,)), ((), ())), preferred_element_type=F32).astype(BF16)
                return carry

            with jax.named_scope("up_grad"):
                lax.fori_loop(0, 3, up_grad, 0)
            for k in range(COLOURS):
                for m in range(CHIPS):
                    copy(s1.at[up_rows(k, m, REDUCE)], p1.at[n, k, m], local.at[G1_OUT]).start()

            @pl.when(n == 0)
            def _():
                with jax.named_scope("wait_21"):
                    ag_wait(2, 1)
                ag_start(2, 2)

            @pl.when(n == nc - 2)
            def _():
                c_add(0)
                c_in(1)

            @pl.when(n == nc - 1)
            def _():
                c_go(3)

            wait_for(ud, local.at[DU_OUT])
            return carry

        lax.fori_loop(0, nc, chunk, 0)
        send_both(nc - 1)

    pl.run_scoped(
        main,
        pltpu.VMEM((both, width), BF16), pltpu.VMEM((both, width), BF16),
        pltpu.VMEM((width, fc), BF16), pltpu.VMEM((fc, width), BF16),
        pltpu.VMEM((both, fc), BF16), pltpu.VMEM((fc, both), BF16),
        pltpu.VMEM((width, fc), BF16), pltpu.VMEM((fc, width), BF16),
        pltpu.VMEM((12, rows, fc), BF16), pltpu.VMEM((12, units, cols), BF16),
        pltpu.VMEM((3, 2, rows, fc), BF16), pltpu.VMEM((3, 2, units, cols), BF16))

    dx_tile = both // DX_TILES
    half_tiles = DX_TILES // 2
    steps = 3 * DX_TILES
    own_from = 3 * half_tiles
    hidden = nc * fc

    def last(w, du, wide, out16, res,
             co1, co2, do1, do2, e1, e2, eo1, eo2):
        def load_w(n, third_):
            for p in range(8):
                r, k = divmod(8 * third_ + p, 3)
                m = 0
                for i in range(3):
                    d = (k + i) % 3
                    m = m + (1 << i) * ((1 - bits[d]) if (r >> d) & 1 else bits[d])
                copy(a1.at[n, k, m], w.at[pl.ds((8 * third_ + p) * rows, rows), pl.ds(pl.multiple_of(n * fc, fc), fc)],
                     w_sem.at[third_]).start()

        def tokens_at(q):
            later = q // half_tiles
            owner = (1 - later) * (1 - core) + later * core
            return pl.multiple_of(owner * tokens + (q % half_tiles) * dx_tile, dx_tile)

        def load_du(q):
            slot = q % 2
            for n in range(nc):
                copy(du_hbm.at[n, pl.ds(tokens_at(q), dx_tile)], du.at[slot, :, pl.ds(n * fc, fc)], local.at[TILE_IN + slot]).start()

        for third_ in range(3):
            lax.fori_loop(0, nc, lambda n, carry, third_=third_: (load_w(n, third_), carry)[1], 0)
            if third_ == 0:
                load_du(0)

        def own_at(q, n):
            return (pl.ds(pl.multiple_of((q % half_tiles) * dx_tile, dx_tile), dx_tile), pl.ds(pl.multiple_of(n * cols, cols), cols))

        def c_in(n):
            c_load(n, e1, e2, local.at[C_IN])

        def c_send(n):
            to1, to2 = co1.at[n - EARLY], co2.at[n - EARLY]
            c_sum(e1, e2, to1, to2, local.at[C_IN])
            for k in range(COLOURS):
                rs_start(n, 1, k, to1.at[k], to2.at[k])

        def sum_of(e, k, terms):
            total = e[k].astype(F32)
            for i in range(1, terms):
                total = total + e[3 * i + k].astype(F32)
            return total.astype(BF16)

        def d_load(n):
            with jax.named_scope("wait_rs1"):
                rs_wait(n, 1)
            for i, (b1, b2) in enumerate(((p1, p2), (ra1, ra2), (rb1, rb2))):
                for k in range(COLOURS):
                    copy(b1.at[n, k, 1], e1.at[3 * i + k], local.at[D_IN]).start()
                    copy(b2.at[n, k, 1], e2.at[3 * i + k], local.at[D_IN]).start()

        def d_send(n):
            wait_for(e1.at[pl.ds(0, 9)], local.at[D_IN])
            wait_for(e2.at[pl.ds(0, 9)], local.at[D_IN])

            for k in range(COLOURS):
                do1[n, k] = sum_of(e1, k, 3)
                do2[n, k] = sum_of(e2, k, 3)
                rs_start(n, 2, k, do1.at[n, k], do2.at[n, k])

        def e_load(n):
            with jax.named_scope("wait_rs2"):
                rs_wait(n, 2)
            for i, (b1, b2) in enumerate(((p1, p2), (ra1, ra2), (rb1, rb2))):
                for k in range(COLOURS):
                    copy(b1.at[n, k, 0], e1.at[3 * i + k], local.at[E_IN]).start()
                    copy(b2.at[n, k, 0], e2.at[3 * i + k], local.at[E_IN]).start()
            copy(rc1.at[n], e1.at[pl.ds(9, 3)], local.at[E_IN]).start()
            copy(rc2.at[n], e2.at[pl.ds(9, 3)], local.at[E_IN]).start()

        keep = pl.ds(pl.multiple_of(core * half, 16), half)
        give = pl.ds(pl.multiple_of((1 - core) * half, 16), half)

        def e_wait_out(n):
            wait_for(gup_hbm.at[0, 0], local.at[GUP_OUT])
            wait_for(gdown_hbm.at[pl.ds(0, units)], local.at[GDOWN_OUT])
            wait_for(gup_hbm.at[0, 0], gup_send.at[n])

        def e_store(n):
            wait_for(e1, local.at[E_IN])
            wait_for(e2, local.at[E_IN])

            @pl.when(n > 0)
            def _():
                e_wait_out(n - 1)

            for k in range(COLOURS):
                eo1[k * rows:(k + 1) * rows, :] = sum_of(e1, k, 4)
                eo2[:, k * cols:(k + 1) * cols] = sum_of(e2, k, 4)
            copy(eo1.at[keep], gup_hbm.at[core, n], local.at[GUP_OUT]).start()
            copy(eo2, gdown_hbm.at[pl.ds(pl.multiple_of(n * units, 16), units)], local.at[GDOWN_OUT]).start()
            pltpu.make_async_remote_copy(
                src_ref=eo1.at[give], dst_ref=gup_hbm.at[core, n], send_sem=gup_send.at[n], recv_sem=gup_recv.at[n],
                device_id=(partner,), device_id_type=MESH).start()

        def pump(i):
            for start, low, high, load, finish_ in (
                    (0, EARLY, nc - 1, c_in, c_send), (8, nc - 1, nc, c_in, c_send), (10, 0, nc, d_load, d_send), (19, 0, nc, e_load, e_store)):
                n = i - start + low

                @pl.when((n > low) & (n <= high))
                def _(finish_=finish_, n=n):
                    finish_(n - 1)

                @pl.when((n >= low) & (n < high))
                def _(load=load, n=n):
                    load(n)

        def step(i, carry):
            q, n = i // 3, i % 3
            slot = i % 2

            @pl.when((i < steps) & (n == 0))
            def _():
                @pl.when(q + 1 < DX_TILES)
                def _():
                    load_du(q + 1)

                with jax.named_scope("wait_du"):
                    wait_for(du.at[0], local.at[TILE_IN + q % 2])

            @pl.when(i < 3)
            def _():
                with jax.named_scope("wait_wall"):
                    wait_for(w.at[pl.ds(0, cols)], w_sem.at[n])

            @pl.when((i >= own_from - 1) & (i < steps - 1))
            def _():
                here = own_at((i + 1) // 3, (i + 1) % 3)
                with jax.named_scope("wait_dxr"):
                    wait_for(dxr_hbm.at[here], dx_recv.at[i + 1 - own_from])

                @pl.when(i < own_from + 2)
                def _():
                    wait_for(wide.at[0], dx_send.at[i - 2])

                copy(dxr_hbm.at[here], wide.at[(i + 1) % 3], local.at[GOT_IN + 1 - slot]).start()
                copy(dy_hbm.at[here], res.at[1 - slot], local.at[RES_IN + 1 - slot]).start()

            @pl.when((i >= 3) & (i < own_from))
            def _():
                with jax.named_scope("wait_dxs"):
                    wait_for(wide.at[0], dx_send.at[i - 3])

            @pl.when((i >= own_from + 2) & (i < steps))
            def _():
                wait_for(out16.at[0], local.at[DX_OUT + slot])

            def dot():
                part = pl.ds(pl.multiple_of(n * cols, cols), cols)
                return lax.dot_general(du[q % 2], w[part, :], (((1,), (1,)), ((), ())), preferred_element_type=F32)

            @pl.when(i < own_from)
            def _():
                with jax.named_scope("dx_dot"):
                    wide[i % 3] = dot()
                pltpu.make_async_remote_copy(
                    src_ref=wide.at[i % 3], dst_ref=dxr_hbm.at[own_at(q, n)], send_sem=dx_send.at[i], recv_sem=dx_recv.at[i],
                    device_id=(partner,), device_id_type=MESH).start()

            @pl.when((i >= own_from) & (i < steps))
            def _():
                with jax.named_scope("wait_got"):
                    wait_for(wide.at[0], local.at[GOT_IN + slot])
                    wait_for(res.at[0], local.at[RES_IN + slot])
                with jax.named_scope("dx_dot2"):
                    out16[slot] = (res[slot].astype(F32) + (dot() + wide[i % 3])).astype(BF16)
                copy(out16.at[slot], dx_hbm.at[own_at(q, n)], local.at[DX_OUT + slot]).start()

            pump(i)
            return carry

        lax.fori_loop(0, max(steps, nc + 20), step, 0)
        for slot in range(2):
            wait_for(out16.at[0], local.at[DX_OUT + slot])
        e_wait_out(nc - 1)
        for n in range(nc):
            wait_for(sized[1].at[0], rs_send.at[1, n])
            wait_for(sized[0].at[0], rs_send.at[2, n])

    pl.run_scoped(
        last,
        pltpu.VMEM((width, hidden), BF16), pltpu.VMEM((2, dx_tile, hidden), BF16),
        pltpu.VMEM((3, dx_tile, cols), F32), pltpu.VMEM((2, dx_tile, cols), BF16), pltpu.VMEM((2, dx_tile, cols), BF16),
        pltpu.VMEM((nc - EARLY, 3, 2, rows, fc), BF16), pltpu.VMEM((nc - EARLY, 3, 2, units, cols), BF16),
        pltpu.VMEM((nc, 3, rows, fc), BF16), pltpu.VMEM((nc, 3, units, cols), BF16),
        pltpu.VMEM((12, rows, fc), BF16), pltpu.VMEM((12, units, cols), BF16),
        pltpu.VMEM((3 * rows, fc), BF16), pltpu.VMEM((units, width), BF16))

    def drain(n, carry):
        for s in range(3):
            for i in range(2):
                wait_for(one_array[s].at[n], ag_send.at[i, s, n])
        wait_for(sized[2].at[n], rs_send.at[0, n])
        wait_for(gup_hbm.at[0, 0], gup_recv.at[n])
        return carry

    with jax.named_scope("drain"):
        lax.fori_loop(0, nc, drain, 0)
    wait_for(xr_hbm, pair_send.at[1])
    wait_for(dyr_hbm, pair_send.at[2])


def finish(nc, units, gup, gdown, dx, gup_out, gdown_out, dx_out, v_in, v_out, v_down, v_dx, sem_in, sem_out):
    pieces = v_dx.shape[0]
    rows = v_dx.shape[1]
    copy(gup, v_in, sem_in.at[pieces]).start()
    copy(gdown, v_down, sem_in.at[pieces + 1]).start()
    for i in range(pieces):
        copy(dx.at[pl.ds(i * rows, rows)], v_dx.at[i], sem_in.at[i]).start()
    copy(gup, v_in, sem_in.at[pieces]).wait()
    per = 128 // math.gcd(128, units)
    for first in range(0, CHIPS * CORES * nc, per):
        parts = []
        for u in range(first, first + per):
            d, n = u // nc, u % nc
            r, c = d // CORES, d % CORES
            parts.append(v_in[c, n, :, r * units:(r + 1) * units])
        v_out[:, first * units:(first + per) * units] = jnp.concatenate(parts, axis=1)
    copy(v_out, gup_out, sem_out.at[pieces]).start()
    copy(gdown, v_down, sem_in.at[pieces + 1]).wait()
    copy(v_down, gdown_out, sem_out.at[pieces + 1]).start()
    for i in range(pieces):
        copy(dx.at[pl.ds(i * rows, rows)], v_dx.at[i], sem_in.at[i]).wait()
        copy(v_dx.at[i], dx_out.at[pl.ds(i * rows, rows)], sem_out.at[i]).start()
    copy(v_out, gup_out, sem_out.at[pieces]).wait()
    copy(v_down, gdown_out, sem_out.at[pieces + 1]).wait()
    for i in range(pieces):
        copy(v_dx.at[i], dx_out.at[pl.ds(i * rows, rows)], sem_out.at[i]).wait()


def chunks_of(units):
    return 9 if units % 144 == 0 else 1


def solution(mesh):
    def device_fn(x_loc, dy_loc, up_loc, down_loc):
        width = x_loc.shape[-1]
        x = x_loc.reshape(-1, width)
        dy = dy_loc.reshape(-1, width)
        tokens = x.shape[0]
        down = down_loc[0]
        half, units_all = up_loc.shape[1], down.shape[0]
        nc = chunks_of(units_all)
        units = units_all // nc
        fc = CHIPS * units
        rows, cols = 2 * half // 3, width // 3
        up = up_loc[0]

        def hbm(*shape, dtype=BF16):
            return jax.ShapeDtypeStruct(shape, dtype)

        one, two = (rows, fc), (units, cols)
        outs = [
            hbm(CORES, nc, half, fc), hbm(units_all, width), hbm(tokens, width),
            hbm(tokens, width), hbm(tokens, width),
            *[hbm(nc, 3, blocks, *s) for blocks in (8, 8, 4, 2) for s in (one, two)],
            hbm(nc, 3, *one), hbm(nc, 3, *two), hbm(nc, 3, 2, *one), hbm(nc, 3, 2, *two),
            hbm(nc, 2 * tokens, fc), hbm(tokens, width, dtype=F32),
        ]
        dma = pltpu.SemaphoreType.DMA
        half_steps = 3 * DX_TILES // 2
        got = pl.pallas_call(
            functools.partial(kernel, nc),
            out_shape=outs,
            in_specs=[pl.BlockSpec(memory_space=pl.ANY)] * 4,
            out_specs=[pl.BlockSpec(memory_space=pl.ANY)] * len(outs),
            scratch_shapes=[
                dma((2, 3, nc)), dma((2, 3, nc)), dma((3, nc)), dma((3, nc)), dma((3,)), dma((4,)),
                dma((half_steps,)), dma((half_steps,)), dma((nc,)), dma((nc,)), dma((3,)), dma((13,)),
            ],
            compiler_params=pltpu.CompilerParams(
                collective_id=0, has_side_effects=True, vmem_limit_bytes=67_000_000),
        )(x, dy, up, down)
        pieces = 8
        g_up, g_down, dx = pl.pallas_call(
            functools.partial(finish, nc, units),
            out_shape=[hbm(half, up.shape[1]), hbm(units_all, width), hbm(tokens, width)],
            in_specs=[pl.BlockSpec(memory_space=pl.ANY)] * 3,
            out_specs=[pl.BlockSpec(memory_space=pl.ANY)] * 3,
            scratch_shapes=[
                pltpu.VMEM((CORES, nc, half, fc), BF16), pltpu.VMEM((half, up.shape[1]), BF16),
                pltpu.VMEM((units_all, width), BF16), pltpu.VMEM((pieces, tokens // pieces, width), BF16),
                dma((pieces + 2,)), dma((pieces + 2,)),
            ],
            compiler_params=pltpu.CompilerParams(vmem_limit_bytes=67_000_000),
        )(*got[:3])
        return g_up[None], g_down[None], dx.reshape(x_loc.shape)

    return jax.shard_map(
        device_fn, mesh=mesh, in_specs=(P("data"), P("data"), P(None, "data"), P(None, "data")),
        out_specs=(P(None, "data"), P(None, "data"), P("data")), check_vma=False)
```

```python
import functools
import math

import jax
import jax.numpy as jnp
from jax import lax
from jax.experimental import pallas as pl
from jax.experimental.pallas import tpu as pltpu
from jax.sharding import PartitionSpec as P

MESH = pl.DeviceIdType.MESH
F32, BF16 = jnp.float32, jnp.bfloat16
CHIPS, COLOURS, CORES = 8, 3, 2
CHUNKS = 9
VMEM_BYTES = 67_000_000
DX_TILES = 8
UP_TILES = 8
PARTS = 2
UP_IN, X_IN, DY_IN, W1_IN, W2_IN, G1_OUT, G2_OUT, DU_OUT, SUM_IN, SUM_OUT, OWN_0, OWN_1, OWN_2 = range(13)
TILE_IN, GOT_IN, RES_IN, DX_OUT = range(0, 8, 2)
C_IN, D_IN, E_IN, GUP_OUT, GDOWN_OUT = range(8, 13)
EARLY = 4


def copy(src, dst, sem):
    return pltpu.make_async_copy(src, dst, sem)


def wait_for(ref, sem):
    pltpu.make_async_copy(ref, ref, sem).wait()


def gelu_both(u):
    scale = math.sqrt(2.0 / math.pi)
    square = u * u
    th = jnp.tanh(u * (scale + (0.044715 * scale) * square))
    half = 0.5 * th
    cdf = 0.5 + half
    slope = cdf + (u * (0.5 - th * half)) * (scale + (0.134145 * scale) * square)
    return u * cdf, slope


def kernel(nc, x_hbm, dy_hbm, up_hbm, down_hbm,
           gup_hbm, gdown_hbm, dx_hbm,
           xr_hbm, dyr_hbm, a1, a2, p1, p2, ra1, ra2, rb1, rb2, rc1, rc2, cb1, cb2, du_hbm, dxr_hbm,
           ag_send, ag_recv, rs_send, rs_recv, pair_send, pair_recv, dx_send, dx_recv, gup_send, gup_recv, w_sem, local):
    me = lax.axis_index("data")
    core = me % 2
    bits = [(me // 2) % 2, (me // 4) % 2, (me // 8) % 2]
    partner = me + 1 - 2 * core
    near = [me + (2 << d) * (1 - 2 * bits[d]) for d in range(3)]

    tokens, width = x_hbm.shape
    both = 2 * tokens
    *_, rows, fc = a1.shape
    *_, units, cols = a2.shape
    half = up_hbm.shape[0]
    third = half // 3

    def chip(colour, m, order):
        total = 0
        for i in range(3):
            d = (colour + i) % 3
            flipped = (m >> order[i]) & 1
            total = total + (1 << d) * ((1 - bits[d]) if flipped else bits[d])
        return total

    GATHER, REDUCE = (0, 1, 2), (2, 1, 0)

    def up_rows(colour, m, order):
        return pl.ds(pl.multiple_of(chip(colour, m, order) * (3 * rows) + colour * rows, 16), rows)

    def down_rows(colour, m, order):
        return pl.ds(pl.multiple_of(chip(colour, m, order) * units, 16), units)

    def down_cols(colour):
        return pl.ds(colour * cols, cols)

    def ag_start(n, s, arrays=(0, 1)):
        have = 1 << s
        for k in range(COLOURS):
            for i in arrays:
                buf = (a1, a2)[i]
                pltpu.make_async_remote_copy(
                    src_ref=buf.at[n, k, pl.ds(0, have)], dst_ref=buf.at[n, k, pl.ds(have, have)],
                    send_sem=ag_send.at[i, s, n], recv_sem=ag_recv.at[i, s, n],
                    device_id=(near[(k + s) % 3],), device_id_type=MESH).start()

    one_array = (rc1, rb1, ra1)
    sized = (rb1, ra1, p1)

    def ag_wait(n, s, arrays=(0, 1)):
        for i in arrays:
            wait_for(one_array[s].at[n], ag_recv.at[i, s, n])

    def rs_start(n, s, k, src1, src2):
        dst1, dst2 = ((ra1, ra2), (rb1, rb2), (rc1, rc2))[s]
        for src, dst in ((src1, dst1), (src2, dst2)):
            pltpu.make_async_remote_copy(
                src_ref=src, dst_ref=dst.at[n, k], send_sem=rs_send.at[s, n], recv_sem=rs_recv.at[s, n],
                device_id=(near[(k + s) % 3],), device_id_type=MESH).start()

    def rs_wait(n, s):
        wait_for(sized[2 - s].at[n], rs_recv.at[s, n])

    barrier = pltpu.get_barrier_semaphore()
    for other in (partner, *near):
        pl.semaphore_signal(barrier, inc=1, device_id=(other,), device_id_type=MESH)

    def to_partner(src, dst, i):
        pltpu.make_async_remote_copy(
            src_ref=src, dst_ref=dst, send_sem=pair_send.at[i], recv_sem=pair_recv.at[i],
            device_id=(partner,), device_id_type=MESH).start()

    mine = pl.ds(pl.multiple_of(core * tokens, 16), tokens)
    theirs = pl.ds(pl.multiple_of((1 - core) * tokens, 16), tokens)

    def c_load(n, c1, c2, sem):
        with jax.named_scope("wait_rs0"):
            rs_wait(n, 0)
        for i, (b1, b2) in enumerate(((p1, p2), (ra1, ra2))):
            for k in range(COLOURS):
                pair = pl.ds(2 * (3 * i + k), 2)
                copy(b1.at[n, k, pl.ds(2, 2)], c1.at[pair], sem).start()
                copy(b2.at[n, k, pl.ds(2, 2)], c2.at[pair], sem).start()

    def c_sum(c1, c2, to1, to2, sem):
        wait_for(p1.at[0], sem)
        for k in range(COLOURS):
            for j in range(2):
                to1[k, j] = c1[2 * k + j] + c1[2 * k + j + 6]
                to2[k, j] = c2[2 * k + j] + c2[2 * k + j + 6]

    def main(x, dy, w1, w2, ud, at, s1, s2, c1, c2, co1, co2):
        own_down = x.at[pl.ds(0, nc * units)]
        blocks = up_hbm.shape[1] // width
        for b in range(blocks):
            copy(up_hbm.at[:, pl.ds(b * width, width)], x.at[pl.ds(nc * units + b * half, half)], local.at[UP_IN]).start()
        copy(down_hbm, own_down, local.at[X_IN]).start()
        wait_for(up_hbm, local.at[UP_IN])

        def unit(chip_, core_, n):
            first = ((chip_ * CORES + core_) * nc + n) * units
            b, c = first // width, first % width
            return x[nc * units + b * half:nc * units + (b + 1) * half, c:c + units]

        whole = pl.ds(pl.multiple_of(core * third, 16), 2 * third)
        rest = pl.ds(pl.multiple_of((1 - core) * 2 * third, 16), third)
        to_rest = pl.ds(pl.multiple_of(core * third, 16), third)

        def permute(n):
            for c in range(CORES):
                first = (n * CORES + c) * half
                ud[first:first + half, :] = jnp.concatenate([unit(r, c, n) for r in range(CHIPS)], axis=1)

        def own_up(n):
            def part(c, which):
                return ud.at[pl.ds(pl.multiple_of((n * CORES + c) * half + which.start, 16), which.size)]

            sem = min(n, 1)
            for which, dst in ((whole, a1.at[n, 2 * core, 0]), (rest, a1.at[n, 1, 0, to_rest])):
                pltpu.make_async_remote_copy(
                    src_ref=part(1 - core, which), dst_ref=dst, send_sem=pair_send.at[0], recv_sem=pair_recv.at[3 * sem],
                    device_id=(partner,), device_id_type=MESH).start()
                copy(part(core, which), dst, local.at[OWN_0 + sem]).start()

        def down_own(n):
            for k in range(COLOURS):
                copy(x.at[pl.ds(n * units, units), down_cols(k)], a2.at[n, k, 0], local.at[OWN_2 if n else X_IN]).start()

        permute(0)
        with jax.named_scope("entry"):
            pl.semaphore_wait(barrier, 4)
        own_up(0)
        for k in range(COLOURS):
            pltpu.make_async_remote_copy(
                src_ref=down_hbm.at[pl.ds(0, units), down_cols(k)], dst_ref=a2.at[0, k, 1],
                send_sem=ag_send.at[1, 0, 0], recv_sem=ag_recv.at[1, 0, 0],
                device_id=(near[k],), device_id_type=MESH).start()
        wait_for(down_hbm, local.at[X_IN])
        for n in range(nc):
            down_own(n)
        for n in range(1, 4):
            permute(n)
        with jax.named_scope("own_wait"):
            wait_for(du_hbm.at[0, pl.ds(0, half)], local.at[OWN_0])
            wait_for(du_hbm.at[0, pl.ds(0, half)], pair_recv.at[0])
        ag_start(0, 0, (0,))
        for n in range(4, nc):
            permute(n)
        for n in range(1, nc):
            own_up(n)
        to_partner(x_hbm, xr_hbm, 1)
        to_partner(dy_hbm, dyr_hbm, 2)
        wait_for(down_hbm.at[pl.ds(0, units)], local.at[X_IN])
        wait_for(down_hbm.at[pl.ds(0, (nc - 1) * units)], local.at[OWN_2])
        ag_start(1, 0, (1,))
        copy(x_hbm, x.at[mine], local.at[X_IN]).start()
        copy(dy_hbm, dy.at[mine], local.at[DY_IN]).start()
        for s in range(2):
            for i in range(2):
                with jax.named_scope(f"ag0{s}{i}"):
                    ag_wait(0, s, (i,))
                ag_start(0, s + 1, (i,))
        wait_for(du_hbm.at[0, pl.ds(0, (nc - 1) * half)], local.at[OWN_1])
        wait_for(du_hbm.at[0, pl.ds(0, (nc - 1) * half)], pair_recv.at[3])
        ag_start(1, 0, (0,))
        ag_start(2, 0)
        with jax.named_scope("xr"):
            wait_for(xr_hbm, pair_recv.at[1])
        copy(xr_hbm, x.at[theirs], local.at[X_IN]).start()

        def load_up(n):
            for k in range(COLOURS):
                for m in range(CHIPS):
                    copy(a1.at[n, k, m], w1.at[up_rows(k, m, GATHER)], local.at[W1_IN]).start()

        def load_down(n):
            for k in range(COLOURS):
                for m in range(CHIPS):
                    copy(a2.at[n, k, m], w2.at[down_rows(k, m, GATHER), down_cols(k)], local.at[W2_IN]).start()

        with jax.named_scope("ag020"):
            ag_wait(0, 2, (0,))
        load_up(0)
        with jax.named_scope("tokens"):
            wait_for(x, local.at[X_IN])
            wait_for(du_hbm.at[0, pl.ds(0, nc * half)], pair_send.at[0])

        def send_first(src, dst, n):
            for k in range(COLOURS):
                pltpu.make_async_remote_copy(
                    src_ref=src.at[n, k, pl.ds(4, 4)], dst_ref=dst.at[n, k], send_sem=rs_send.at[0, n],
                    recv_sem=rs_recv.at[0, n], device_id=(near[k],), device_id_type=MESH).start()

        def send_down(n):
            wait_for(p1.at[0], local.at[G1_OUT])
            wait_for(p2.at[0], local.at[G2_OUT])
            send_first(p2, ra2, n)

        def c_in(n):
            c_load(n, c1, c2, local.at[SUM_IN])

        def c_add(n):
            c_sum(c1, c2, co1, co2, local.at[SUM_IN])
            copy(co1, cb1.at[n], local.at[SUM_OUT]).start()
            copy(co2, cb2.at[n], local.at[SUM_OUT]).start()

        def c_go(n):
            wait_for(sized[1].at[0], local.at[SUM_OUT])
            for k in range(COLOURS):
                rs_start(n, 1, k, cb1.at[n, k], cb2.at[n, k])

        def early(slot):
            if slot > 1:
                c_go(slot - 2)
            if 0 < slot <= EARLY:
                c_add(slot - 1)
            if slot < EARLY:
                c_in(slot)

        up_tile = both // UP_TILES

        def chunk(n, carry):
            size = up_tile // PARTS
            strip = min(128, size)

            def use(first, u, da):
                for c in range(0, fc, 128):
                    lanes = slice(c, c + 128)
                    for r in range(0, size, strip):
                        at_r = pl.ds(pl.multiple_of(first + r, strip), strip)
                        a, slope = gelu_both(u(r, at_r, lanes).astype(F32))
                        ud[at_r, lanes] = (da[r:r + strip, lanes] * slope).astype(BF16)
                        at[lanes, at_r] = a.astype(BF16).T

            def da_of(at_t):
                return lax.dot_general(dy[at_t, :], w2[...], (((1,), (1,)), ((), ())), preferred_element_type=F32)

            with jax.named_scope("wait_w1"):
                wait_for(w1, local.at[W1_IN])

            @pl.when(n == 0)
            def _():
                def u_step(t, carry):
                    at_t = pl.ds(pl.multiple_of(t * 2 * up_tile, up_tile), 2 * up_tile)
                    ud[at_t, :] = jnp.dot(x[at_t, :], w1[...], preferred_element_type=F32).astype(BF16)

                    @pl.when(t == 1)
                    def _():
                        with jax.named_scope("dyr"):
                            wait_for(dyr_hbm, pair_recv.at[2])
                        copy(dyr_hbm, dy.at[theirs], local.at[DY_IN]).start()

                    @pl.when(t == 2)
                    def _():
                        with jax.named_scope("ag021"):
                            ag_wait(0, 2, (1,))
                        load_down(0)

                    return carry

                with jax.named_scope("u0"):
                    lax.fori_loop(0, UP_TILES // 2, u_step, 0)
                with jax.named_scope("wait_100"):
                    ag_wait(1, 0, (0,))
                ag_start(1, 1, (0,))
                with jax.named_scope("first_w2"):
                    wait_for(dy, local.at[DY_IN])
                    wait_for(w2, local.at[W2_IN])

                def da_step(t, carry):
                    for part in range(PARTS):
                        first = t * up_tile + part * size
                        da = da_of(pl.ds(pl.multiple_of(first, size), size))
                        use(first, lambda r, at_r, lanes: ud[at_r, lanes], da)

                    for when, s, i in ((0, 0, 1), (3, 1, 0), (6, 1, 1)):
                        @pl.when(t == when)
                        def _(s=s, i=i):
                            with jax.named_scope(f"wait_1{s}{i}"):
                                ag_wait(1, s, (i,))
                            ag_start(1, s + 1, (i,))

                    return carry

                with jax.named_scope("da0"):
                    lax.fori_loop(0, UP_TILES, da_step, 0)
                with jax.named_scope("wait_20"):
                    ag_wait(2, 0)
                ag_start(2, 1)
                ag_start(3, 0)

            def up_step(t, carry):
                for part in range(PARTS):
                    first = t * up_tile + part * size
                    at_t = pl.ds(pl.multiple_of(first, size), size)
                    u = jnp.dot(x[at_t, :], w1[...], preferred_element_type=F32).astype(BF16)
                    da = da_of(at_t)
                    use(first, lambda r, at_r, lanes, u=u: u[r:r + strip, lanes], da)

                @pl.when((t == 2) & (n == 1))
                def _():
                    with jax.named_scope("wait_30"):
                        ag_wait(3, 0)
                    ag_start(3, 1)
                    ag_start(4, 0)

                @pl.when(t == 2)
                def _():
                    send_down(n - 1)

                    @pl.when(n > nc - 4)
                    def _():
                        send_first(p1, ra1, n - 1)

                    @pl.when((n > 2) & (n < nc - 1))
                    def _():
                        send_first(p1, ra1, n - 3)

                @pl.when((t == 6) & (n == nc - 2))
                def _():
                    early(0)

                @pl.when((t == 6) & (n == nc - 1))
                def _():
                    early(3)

                return carry

            @pl.when(n > 0)
            def _():
                with jax.named_scope("wait_w2"):
                    wait_for(w2, local.at[W2_IN])
                with jax.named_scope("up"):
                    lax.fori_loop(0, UP_TILES, up_step, 0)

            copy(ud, du_hbm.at[n], local.at[DU_OUT]).start()

            @pl.when(n == nc - 1)
            def _():
                early(4)

            def down_grad(k, carry):
                part = pl.ds(pl.multiple_of(k * cols, cols), cols)
                s2[:, part] = jnp.dot(at[...], dy[:, part], preferred_element_type=F32).astype(BF16)
                return carry

            with jax.named_scope("down_grad"):
                lax.fori_loop(0, 3, down_grad, 0)
            for k in range(COLOURS):
                for m in range(CHIPS):
                    copy(s2.at[down_rows(k, m, REDUCE), down_cols(k)], p2.at[n, k, m], local.at[G2_OUT]).start()

            @pl.when((n > 0) & (n + 2 < nc))
            def _():
                with jax.named_scope("wait_ag1"):
                    ag_wait(n + 2, 1)
                ag_start(n + 2, 2)

            @pl.when((n > 0) & (n + 3 < nc))
            def _():
                with jax.named_scope("wait_ag0"):
                    ag_wait(n + 3, 0)
                ag_start(n + 3, 1)

            @pl.when((n > 0) & (n + 4 < nc))
            def _():
                ag_start(n + 4, 0)

            @pl.when(n == nc - 2)
            def _():
                early(1)

            @pl.when(n == nc - 1)
            def _():
                early(5)

            def up_grad(k, carry):
                part = pl.ds(pl.multiple_of(k * cols, cols), cols)

                @pl.when((k == 2) & (n + 1 < nc))
                def _():
                    with jax.named_scope("wait_ag2"):
                        ag_wait(n + 1, 2)
                    load_up(n + 1)
                    load_down(n + 1)

                s1[part, :] = lax.dot_general(
                    x[:, part], ud[...], (((0,), (0,)), ((), ())), preferred_element_type=F32).astype(BF16)
                return carry

            with jax.named_scope("up_grad"):
                lax.fori_loop(0, 3, up_grad, 0)
            for k in range(COLOURS):
                for m in range(CHIPS):
                    copy(s1.at[up_rows(k, m, REDUCE)], p1.at[n, k, m], local.at[G1_OUT]).start()

            @pl.when(n == 0)
            def _():
                with jax.named_scope("wait_21"):
                    ag_wait(2, 1)
                ag_start(2, 2)

            @pl.when(n == nc - 2)
            def _():
                early(2)

            wait_for(ud, local.at[DU_OUT])
            return carry

        lax.fori_loop(0, nc, chunk, 0)
        send_down(nc - 1)
        send_first(p1, ra1, nc - 1)

    pl.run_scoped(
        main,
        pltpu.VMEM((both, width), BF16), pltpu.VMEM((both, width), BF16),
        pltpu.VMEM((width, fc), BF16), pltpu.VMEM((fc, width), BF16),
        pltpu.VMEM((both, fc), BF16), pltpu.VMEM((fc, both), BF16),
        pltpu.VMEM((width, fc), BF16), pltpu.VMEM((fc, width), BF16),
        pltpu.VMEM((12, rows, fc), BF16), pltpu.VMEM((12, units, cols), BF16),
        pltpu.VMEM((3, 2, rows, fc), BF16), pltpu.VMEM((3, 2, units, cols), BF16))

    dx_tile = both // DX_TILES
    half_tiles = DX_TILES // 2
    steps = 3 * DX_TILES
    own_from = 3 * half_tiles
    hidden = nc * fc

    def last(w, du, wide, out16, res,
             co1, co2, do1, do2, e1, e2, eo1, eo2):
        def load_w(n, third_):
            for p in range(CHIPS):
                piece = CHIPS * third_ + p
                r, k = divmod(piece, COLOURS)
                m = 0
                for i in range(3):
                    d = (k + i) % 3
                    m = m + (1 << i) * ((1 - bits[d]) if (r >> d) & 1 else bits[d])
                copy(a1.at[n, k, m], w.at[pl.ds(piece * rows, rows), pl.ds(pl.multiple_of(n * fc, fc), fc)],
                     w_sem.at[third_]).start()

        def tokens_at(q):
            later = q // half_tiles
            owner = (1 - later) * (1 - core) + later * core
            return pl.multiple_of(owner * tokens + (q % half_tiles) * dx_tile, dx_tile)

        def load_du(q):
            slot = q % 2
            for n in range(nc):
                copy(du_hbm.at[n, pl.ds(tokens_at(q), dx_tile)], du.at[slot, :, pl.ds(n * fc, fc)], local.at[TILE_IN + slot]).start()

        for third_ in range(COLOURS):
            lax.fori_loop(0, nc, lambda n, carry, third_=third_: (load_w(n, third_), carry)[1], 0)
            if third_ == 0:
                load_du(0)

        def own_at(q, n):
            return (pl.ds(pl.multiple_of((q % half_tiles) * dx_tile, dx_tile), dx_tile), pl.ds(pl.multiple_of(n * cols, cols), cols))

        def c_in(n):
            c_load(n, e1, e2, local.at[C_IN])

        def c_send(n):
            to1, to2 = co1.at[n - EARLY], co2.at[n - EARLY]
            c_sum(e1, e2, to1, to2, local.at[C_IN])
            for k in range(COLOURS):
                rs_start(n, 1, k, to1.at[k], to2.at[k])

        def sum_of(e, k, terms):
            total = e[k].astype(F32)
            for i in range(1, terms):
                total = total + e[3 * i + k].astype(F32)
            return total.astype(BF16)

        def d_load(n):
            with jax.named_scope("wait_rs1"):
                rs_wait(n, 1)
            for i, (b1, b2) in enumerate(((p1, p2), (ra1, ra2), (rb1, rb2))):
                for k in range(COLOURS):
                    copy(b1.at[n, k, 1], e1.at[3 * i + k], local.at[D_IN]).start()
                    copy(b2.at[n, k, 1], e2.at[3 * i + k], local.at[D_IN]).start()

        def d_send(n):
            wait_for(e1.at[pl.ds(0, 9)], local.at[D_IN])
            wait_for(e2.at[pl.ds(0, 9)], local.at[D_IN])

            for k in range(COLOURS):
                do1[n, k] = sum_of(e1, k, 3)
                do2[n, k] = sum_of(e2, k, 3)
                rs_start(n, 2, k, do1.at[n, k], do2.at[n, k])

        def e_load(n):
            with jax.named_scope("wait_rs2"):
                rs_wait(n, 2)
            for i, (b1, b2) in enumerate(((p1, p2), (ra1, ra2), (rb1, rb2))):
                for k in range(COLOURS):
                    copy(b1.at[n, k, 0], e1.at[3 * i + k], local.at[E_IN]).start()
                    copy(b2.at[n, k, 0], e2.at[3 * i + k], local.at[E_IN]).start()
            copy(rc1.at[n], e1.at[pl.ds(9, 3)], local.at[E_IN]).start()
            copy(rc2.at[n], e2.at[pl.ds(9, 3)], local.at[E_IN]).start()

        keep = pl.ds(pl.multiple_of(core * half, 16), half)
        give = pl.ds(pl.multiple_of((1 - core) * half, 16), half)

        def e_wait_out(n):
            wait_for(gup_hbm.at[0, 0], local.at[GUP_OUT])
            wait_for(gdown_hbm.at[pl.ds(0, units)], local.at[GDOWN_OUT])
            wait_for(gup_hbm.at[0, 0], gup_send.at[n])

        def e_store(n):
            wait_for(e1, local.at[E_IN])
            wait_for(e2, local.at[E_IN])

            @pl.when(n > 0)
            def _():
                e_wait_out(n - 1)

            for k in range(COLOURS):
                eo1[k * rows:(k + 1) * rows, :] = sum_of(e1, k, 4)
                eo2[:, k * cols:(k + 1) * cols] = sum_of(e2, k, 4)
            copy(eo1.at[keep], gup_hbm.at[core, n], local.at[GUP_OUT]).start()
            copy(eo2, gdown_hbm.at[pl.ds(pl.multiple_of(n * units, 16), units)], local.at[GDOWN_OUT]).start()
            pltpu.make_async_remote_copy(
                src_ref=eo1.at[give], dst_ref=gup_hbm.at[core, n], send_sem=gup_send.at[n], recv_sem=gup_recv.at[n],
                device_id=(partner,), device_id_type=MESH).start()

        def pump(i):
            for start, low, high, load, finish_ in (
                    (0, EARLY, nc - 1, c_in, c_send), (7, nc - 1, nc, c_in, c_send), (8, 0, nc, d_load, d_send), (17, 0, nc, e_load, e_store)):
                n = i - start + low

                @pl.when((n > low) & (n <= high))
                def _(finish_=finish_, n=n):
                    finish_(n - 1)

                @pl.when((n >= low) & (n < high))
                def _(load=load, n=n):
                    load(n)

        def step(i, carry):
            q, n = i // 3, i % 3
            slot = i % 2

            @pl.when((i < steps) & (n == 0))
            def _():
                @pl.when(q + 1 < DX_TILES)
                def _():
                    load_du(q + 1)

                with jax.named_scope("wait_du"):
                    wait_for(du.at[0], local.at[TILE_IN + q % 2])

            @pl.when(i < 3)
            def _():
                with jax.named_scope("wait_wall"):
                    wait_for(w.at[pl.ds(0, cols)], w_sem.at[n])

            @pl.when((i >= own_from - 1) & (i < steps - 1))
            def _():
                here = own_at((i + 1) // 3, (i + 1) % 3)
                with jax.named_scope("wait_dxr"):
                    wait_for(dxr_hbm.at[here], dx_recv.at[i + 1 - own_from])

                @pl.when(i < own_from + 2)
                def _():
                    wait_for(wide.at[0], dx_send.at[i - 2])

                copy(dxr_hbm.at[here], wide.at[(i + 1) % 3], local.at[GOT_IN + 1 - slot]).start()
                copy(dy_hbm.at[here], res.at[1 - slot], local.at[RES_IN + 1 - slot]).start()

            @pl.when((i >= 3) & (i < own_from))
            def _():
                with jax.named_scope("wait_dxs"):
                    wait_for(wide.at[0], dx_send.at[i - 3])

            @pl.when((i >= own_from + 2) & (i < steps))
            def _():
                wait_for(out16.at[0], local.at[DX_OUT + slot])

            def dot():
                part = pl.ds(pl.multiple_of(n * cols, cols), cols)
                return lax.dot_general(du[q % 2], w[part, :], (((1,), (1,)), ((), ())), preferred_element_type=F32)

            @pl.when(i < own_from)
            def _():
                with jax.named_scope("dx_dot"):
                    wide[i % 3] = dot()
                pltpu.make_async_remote_copy(
                    src_ref=wide.at[i % 3], dst_ref=dxr_hbm.at[own_at(q, n)], send_sem=dx_send.at[i], recv_sem=dx_recv.at[i],
                    device_id=(partner,), device_id_type=MESH).start()

            @pl.when((i >= own_from) & (i < steps))
            def _():
                with jax.named_scope("wait_got"):
                    wait_for(wide.at[0], local.at[GOT_IN + slot])
                    wait_for(res.at[0], local.at[RES_IN + slot])
                with jax.named_scope("dx_dot2"):
                    out16[slot] = (res[slot].astype(F32) + (dot() + wide[i % 3])).astype(BF16)
                copy(out16.at[slot], dx_hbm.at[own_at(q, n)], local.at[DX_OUT + slot]).start()

            pump(i)
            return carry

        lax.fori_loop(0, max(steps, nc + 18), step, 0)
        for slot in range(2):
            wait_for(out16.at[0], local.at[DX_OUT + slot])
        e_wait_out(nc - 1)
        for n in range(nc):
            wait_for(sized[1].at[0], rs_send.at[1, n])
            wait_for(sized[0].at[0], rs_send.at[2, n])

    pl.run_scoped(
        last,
        pltpu.VMEM((width, hidden), BF16), pltpu.VMEM((2, dx_tile, hidden), BF16),
        pltpu.VMEM((3, dx_tile, cols), F32), pltpu.VMEM((2, dx_tile, cols), BF16), pltpu.VMEM((2, dx_tile, cols), BF16),
        pltpu.VMEM((nc - EARLY, 3, 2, rows, fc), BF16), pltpu.VMEM((nc - EARLY, 3, 2, units, cols), BF16),
        pltpu.VMEM((nc, 3, rows, fc), BF16), pltpu.VMEM((nc, 3, units, cols), BF16),
        pltpu.VMEM((12, rows, fc), BF16), pltpu.VMEM((12, units, cols), BF16),
        pltpu.VMEM((3 * rows, fc), BF16), pltpu.VMEM((units, width), BF16))

    def drain(n, carry):
        for s in range(3):
            for i in range(2):
                wait_for(one_array[s].at[n], ag_send.at[i, s, n])
        wait_for(sized[2].at[n], rs_send.at[0, n])
        wait_for(gup_hbm.at[0, 0], gup_recv.at[n])
        return carry

    with jax.named_scope("drain"):
        lax.fori_loop(0, nc, drain, 0)
    wait_for(xr_hbm, pair_send.at[1])
    wait_for(dyr_hbm, pair_send.at[2])


def finish(nc, units, gup, gdown, dx, gup_out, gdown_out, dx_out, v_in, v_out, v_down, v_dx, sem_in, sem_out):
    pieces = v_dx.shape[0]
    rows = v_dx.shape[1]
    copy(gup, v_in, sem_in.at[pieces]).start()
    copy(gdown, v_down, sem_in.at[pieces + 1]).start()
    for i in range(pieces):
        copy(dx.at[pl.ds(i * rows, rows)], v_dx.at[i], sem_in.at[i]).start()
    copy(gup, v_in, sem_in.at[pieces]).wait()
    per = 128 // math.gcd(128, units)
    for first in range(0, CHIPS * CORES * nc, per):
        parts = []
        for u in range(first, first + per):
            d, n = u // nc, u % nc
            r, c = d // CORES, d % CORES
            parts.append(v_in[c, n, :, r * units:(r + 1) * units])
        v_out[:, first * units:(first + per) * units] = jnp.concatenate(parts, axis=1)
    copy(v_out, gup_out, sem_out.at[pieces]).start()
    copy(gdown, v_down, sem_in.at[pieces + 1]).wait()
    copy(v_down, gdown_out, sem_out.at[pieces + 1]).start()
    for i in range(pieces):
        copy(dx.at[pl.ds(i * rows, rows)], v_dx.at[i], sem_in.at[i]).wait()
        copy(v_dx.at[i], dx_out.at[pl.ds(i * rows, rows)], sem_out.at[i]).start()
    copy(v_out, gup_out, sem_out.at[pieces]).wait()
    copy(v_down, gdown_out, sem_out.at[pieces + 1]).wait()
    for i in range(pieces):
        copy(v_dx.at[i], dx_out.at[pl.ds(i * rows, rows)], sem_out.at[i]).wait()


def solution(mesh):
    def device_fn(x_loc, dy_loc, up_loc, down_loc):
        width = x_loc.shape[-1]
        x = x_loc.reshape(-1, width)
        dy = dy_loc.reshape(-1, width)
        tokens = x.shape[0]
        down = down_loc[0]
        half, units_all = up_loc.shape[1], down.shape[0]
        nc = CHUNKS
        units = units_all // nc
        fc = CHIPS * units
        rows, cols = 2 * half // 3, width // 3
        up = up_loc[0]

        def hbm(*shape, dtype=BF16):
            return jax.ShapeDtypeStruct(shape, dtype)

        one, two = (rows, fc), (units, cols)
        outs = [
            hbm(CORES, nc, half, fc), hbm(units_all, width), hbm(tokens, width),
            hbm(tokens, width), hbm(tokens, width),
            *[hbm(nc, 3, blocks, *s) for blocks in (8, 8, 4, 2) for s in (one, two)],
            hbm(nc, 3, *one), hbm(nc, 3, *two), hbm(nc, 3, 2, *one), hbm(nc, 3, 2, *two),
            hbm(nc, 2 * tokens, fc), hbm(tokens, width, dtype=F32),
        ]
        dma = pltpu.SemaphoreType.DMA
        half_steps = 3 * DX_TILES // 2
        got = pl.pallas_call(
            functools.partial(kernel, nc),
            out_shape=outs,
            in_specs=[pl.BlockSpec(memory_space=pl.ANY)] * 4,
            out_specs=[pl.BlockSpec(memory_space=pl.ANY)] * len(outs),
            scratch_shapes=[
                dma((2, 3, nc)), dma((2, 3, nc)), dma((3, nc)), dma((3, nc)), dma((3,)), dma((4,)),
                dma((half_steps,)), dma((half_steps,)), dma((nc,)), dma((nc,)), dma((3,)), dma((13,)),
            ],
            compiler_params=pltpu.CompilerParams(
                collective_id=0, has_side_effects=True, vmem_limit_bytes=VMEM_BYTES),
        )(x, dy, up, down)
        pieces = 8
        g_up, g_down, dx = pl.pallas_call(
            functools.partial(finish, nc, units),
            out_shape=[hbm(half, up.shape[1]), hbm(units_all, width), hbm(tokens, width)],
            in_specs=[pl.BlockSpec(memory_space=pl.ANY)] * 3,
            out_specs=[pl.BlockSpec(memory_space=pl.ANY)] * 3,
            scratch_shapes=[
                pltpu.VMEM((CORES, nc, half, fc), BF16), pltpu.VMEM((half, up.shape[1]), BF16),
                pltpu.VMEM((units_all, width), BF16), pltpu.VMEM((pieces, tokens // pieces, width), BF16),
                dma((pieces + 2,)), dma((pieces + 2,)),
            ],
            compiler_params=pltpu.CompilerParams(vmem_limit_bytes=VMEM_BYTES),
        )(*got[:3])
        return g_up[None], g_down[None], dx.reshape(x_loc.shape)

    return jax.shard_map(
        device_fn, mesh=mesh, in_specs=(P("data"), P("data"), P(None, "data"), P(None, "data")),
        out_specs=(P(None, "data"), P(None, "data"), P("data")), check_vma=False)
```

```python
import functools
import math

import jax
import jax.numpy as jnp
from jax import lax
from jax.experimental import pallas as pl
from jax.experimental.pallas import tpu as pltpu
from jax.sharding import PartitionSpec as P

MESH = pl.DeviceIdType.MESH
F32, BF16 = jnp.float32, jnp.bfloat16
CHIPS, COLOURS, CORES = 8, 3, 2
CHUNKS = 9
VMEM_BYTES = 67_000_000
DX_TILES = 8
UP_TILES = 8
PARTS = 2
UP_IN, X_IN, DY_IN, W1_IN, W2_IN, G1_OUT, G2_OUT, DU_OUT, SUM_IN, SUM_OUT, OWN_0, OWN_1, OWN_2 = range(13)
TILE_IN, GOT_IN, RES_IN, DX_OUT = range(0, 8, 2)
C_IN, D_IN, E_IN, GUP_OUT, GDOWN_OUT = range(8, 13)
EARLY = 4


def copy(src, dst, sem):
    return pltpu.make_async_copy(src, dst, sem)


def wait_for(ref, sem):
    pltpu.make_async_copy(ref, ref, sem).wait()


def gelu_both(u):
    scale = math.sqrt(2.0 / math.pi)
    square = u * u
    th = jnp.tanh(u * (scale + (0.044715 * scale) * square))
    half = 0.5 * th
    cdf = 0.5 + half
    slope = cdf + (u * (0.5 - th * half)) * (scale + (0.134145 * scale) * square)
    return u * cdf, slope


def kernel(nc, x_hbm, dy_hbm, up_hbm, down_hbm,
           gup_hbm, gdown_hbm, dx_hbm,
           xr_hbm, dyr_hbm, a1, a2, p1, p2, ra1, ra2, rb1, rb2, rc1, rc2, cb1, cb2, du_hbm, dxr_hbm,
           ag_send, ag_recv, rs_send, rs_recv, pair_send, pair_recv, dx_send, dx_recv, gup_send, gup_recv, w_sem, local):
    me = lax.axis_index("data")
    core = me % 2
    bits = [(me // 2) % 2, (me // 4) % 2, (me // 8) % 2]
    partner = me + 1 - 2 * core
    near = [me + (2 << d) * (1 - 2 * bits[d]) for d in range(3)]

    tokens, width = x_hbm.shape
    both = 2 * tokens
    *_, rows, fc = a1.shape
    *_, units, cols = a2.shape
    half = up_hbm.shape[0]
    third = half // 3

    def chip(colour, m, order):
        total = 0
        for i in range(3):
            d = (colour + i) % 3
            flipped = (m >> order[i]) & 1
            total = total + (1 << d) * ((1 - bits[d]) if flipped else bits[d])
        return total

    GATHER, REDUCE = (0, 1, 2), (2, 1, 0)

    def up_rows(colour, m, order):
        return pl.ds(pl.multiple_of(chip(colour, m, order) * (3 * rows) + colour * rows, 16), rows)

    def down_rows(colour, m, order):
        return pl.ds(pl.multiple_of(chip(colour, m, order) * units, 16), units)

    def down_cols(colour):
        return pl.ds(colour * cols, cols)

    def ag_start(n, s, arrays=(0, 1)):
        have = 1 << s
        for k in range(COLOURS):
            for i in arrays:
                buf = (a1, a2)[i]
                pltpu.make_async_remote_copy(
                    src_ref=buf.at[n, k, pl.ds(0, have)], dst_ref=buf.at[n, k, pl.ds(have, have)],
                    send_sem=ag_send.at[i, s, n], recv_sem=ag_recv.at[i, s, n],
                    device_id=(near[(k + s) % 3],), device_id_type=MESH).start()

    one_array = (rc1, rb1, ra1)
    sized = (rb1, ra1, p1)

    def ag_wait(n, s, arrays=(0, 1)):
        for i in arrays:
            wait_for(one_array[s].at[n], ag_recv.at[i, s, n])

    def rs_start(n, s, k, src1, src2):
        dst1, dst2 = ((ra1, ra2), (rb1, rb2), (rc1, rc2))[s]
        for src, dst in ((src1, dst1), (src2, dst2)):
            pltpu.make_async_remote_copy(
                src_ref=src, dst_ref=dst.at[n, k], send_sem=rs_send.at[s, n], recv_sem=rs_recv.at[s, n],
                device_id=(near[(k + s) % 3],), device_id_type=MESH).start()

    def rs_wait(n, s):
        wait_for(sized[2 - s].at[n], rs_recv.at[s, n])

    barrier = pltpu.get_barrier_semaphore()
    for other in (partner, *near):
        pl.semaphore_signal(barrier, inc=1, device_id=(other,), device_id_type=MESH)

    def to_partner(src, dst, i):
        pltpu.make_async_remote_copy(
            src_ref=src, dst_ref=dst, send_sem=pair_send.at[i], recv_sem=pair_recv.at[i],
            device_id=(partner,), device_id_type=MESH).start()

    mine = pl.ds(pl.multiple_of(core * tokens, 16), tokens)
    theirs = pl.ds(pl.multiple_of((1 - core) * tokens, 16), tokens)

    def c_load(n, c1, c2, sem):
        with jax.named_scope("wait_rs0"):
            rs_wait(n, 0)
        for i, (b1, b2) in enumerate(((p1, p2), (ra1, ra2))):
            for k in range(COLOURS):
                pair = pl.ds(2 * (3 * i + k), 2)
                copy(b1.at[n, k, pl.ds(2, 2)], c1.at[pair], sem).start()
                copy(b2.at[n, k, pl.ds(2, 2)], c2.at[pair], sem).start()

    def c_sum(c1, c2, to1, to2, sem):
        wait_for(p1.at[0], sem)
        for k in range(COLOURS):
            for j in range(2):
                to1[k, j] = c1[2 * k + j] + c1[2 * k + j + 6]
                to2[k, j] = c2[2 * k + j] + c2[2 * k + j + 6]

    def main(x, dy, w1, w2, ud, at, s1, s2, c1, c2, co1, co2):
        own_down = x.at[pl.ds(0, nc * units)]
        blocks = up_hbm.shape[1] // width
        for b in range(blocks):
            copy(up_hbm.at[:, pl.ds(b * width, width)], x.at[pl.ds(nc * units + b * half, half)], local.at[UP_IN]).start()
        copy(down_hbm, own_down, local.at[X_IN]).start()
        with jax.named_scope("entry"):
            pl.semaphore_wait(barrier, 4)
        for n in range(2):
            for k in range(COLOURS):
                pltpu.make_async_remote_copy(
                    src_ref=down_hbm.at[pl.ds(n * units, units), down_cols(k)], dst_ref=a2.at[n, k, 1],
                    send_sem=ag_send.at[1, 0, n], recv_sem=ag_recv.at[1, 0, n],
                    device_id=(near[k],), device_id_type=MESH).start()
        wait_for(up_hbm, local.at[UP_IN])

        def unit(chip_, core_, n):
            first = ((chip_ * CORES + core_) * nc + n) * units
            b, c = first // width, first % width
            return x[nc * units + b * half:nc * units + (b + 1) * half, c:c + units]

        whole = pl.ds(pl.multiple_of(core * third, 16), 2 * third)
        rest = pl.ds(pl.multiple_of((1 - core) * 2 * third, 16), third)
        to_rest = pl.ds(pl.multiple_of(core * third, 16), third)

        def permute(n):
            for c in range(CORES):
                first = (n * CORES + c) * half
                ud[first:first + half, :] = jnp.concatenate([unit(r, c, n) for r in range(CHIPS)], axis=1)

        def own_up(n):
            def part(c, which):
                return ud.at[pl.ds(pl.multiple_of((n * CORES + c) * half + which.start, 16), which.size)]

            sem = min(n, 1)
            for which, dst in ((whole, a1.at[n, 2 * core, 0]), (rest, a1.at[n, 1, 0, to_rest])):
                pltpu.make_async_remote_copy(
                    src_ref=part(1 - core, which), dst_ref=dst, send_sem=pair_send.at[0], recv_sem=pair_recv.at[3 * sem],
                    device_id=(partner,), device_id_type=MESH).start()
                copy(part(core, which), dst, local.at[OWN_0 + sem]).start()

        def down_own(n):
            for k in range(COLOURS):
                copy(x.at[pl.ds(n * units, units), down_cols(k)], a2.at[n, k, 0], local.at[OWN_2 if n else X_IN]).start()

        permute(0)
        own_up(0)
        wait_for(down_hbm, local.at[X_IN])
        for n in range(nc):
            down_own(n)
        for n in range(1, 4):
            permute(n)
        with jax.named_scope("own_wait"):
            wait_for(du_hbm.at[0, pl.ds(0, half)], local.at[OWN_0])
            wait_for(du_hbm.at[0, pl.ds(0, half)], pair_recv.at[0])
        ag_start(0, 0, (0,))
        for n in range(4, nc):
            permute(n)
        for n in range(1, nc):
            own_up(n)
        to_partner(x_hbm, xr_hbm, 1)
        to_partner(dy_hbm, dyr_hbm, 2)
        wait_for(down_hbm.at[pl.ds(0, units)], local.at[X_IN])
        wait_for(down_hbm.at[pl.ds(0, (nc - 1) * units)], local.at[OWN_2])
        copy(x_hbm, x.at[mine], local.at[X_IN]).start()
        copy(dy_hbm, dy.at[mine], local.at[DY_IN]).start()
        for s in range(2):
            for i in range(2):
                with jax.named_scope(f"ag0{s}{i}"):
                    ag_wait(0, s, (i,))
                ag_start(0, s + 1, (i,))
        wait_for(du_hbm.at[0, pl.ds(0, (nc - 1) * half)], local.at[OWN_1])
        wait_for(du_hbm.at[0, pl.ds(0, (nc - 1) * half)], pair_recv.at[3])
        ag_start(1, 0, (0,))
        ag_start(2, 0)
        with jax.named_scope("xr"):
            wait_for(xr_hbm, pair_recv.at[1])
        copy(xr_hbm, x.at[theirs], local.at[X_IN]).start()

        def load_up(n):
            for k in range(COLOURS):
                for m in range(CHIPS):
                    copy(a1.at[n, k, m], w1.at[up_rows(k, m, GATHER)], local.at[W1_IN]).start()

        def load_down(n):
            for k in range(COLOURS):
                for m in range(CHIPS):
                    copy(a2.at[n, k, m], w2.at[down_rows(k, m, GATHER), down_cols(k)], local.at[W2_IN]).start()

        with jax.named_scope("ag020"):
            ag_wait(0, 2, (0,))
        load_up(0)
        with jax.named_scope("tokens"):
            wait_for(x, local.at[X_IN])
            wait_for(du_hbm.at[0, pl.ds(0, nc * half)], pair_send.at[0])

        def send_first(src, dst, n):
            for k in range(COLOURS):
                pltpu.make_async_remote_copy(
                    src_ref=src.at[n, k, pl.ds(4, 4)], dst_ref=dst.at[n, k], send_sem=rs_send.at[0, n],
                    recv_sem=rs_recv.at[0, n], device_id=(near[k],), device_id_type=MESH).start()

        def send_down(n):
            wait_for(p1.at[0], local.at[G1_OUT])
            wait_for(p2.at[0], local.at[G2_OUT])
            send_first(p2, ra2, n)

        def c_in(n):
            c_load(n, c1, c2, local.at[SUM_IN])

        def c_add(n):
            c_sum(c1, c2, co1, co2, local.at[SUM_IN])
            copy(co1, cb1.at[n], local.at[SUM_OUT]).start()
            copy(co2, cb2.at[n], local.at[SUM_OUT]).start()

        def c_go(n):
            wait_for(sized[1].at[0], local.at[SUM_OUT])
            for k in range(COLOURS):
                rs_start(n, 1, k, cb1.at[n, k], cb2.at[n, k])

        def early(slot):
            if slot > 1:
                c_go(slot - 2)
            if 0 < slot <= EARLY:
                c_add(slot - 1)
            if slot < EARLY:
                c_in(slot)

        up_tile = both // UP_TILES

        def chunk(n, carry):
            size = up_tile // PARTS
            strip = min(128, size)

            def use(first, u, da):
                for c in range(0, fc, 128):
                    lanes = slice(c, c + 128)
                    for r in range(0, size, strip):
                        at_r = pl.ds(pl.multiple_of(first + r, strip), strip)
                        a, slope = gelu_both(u(r, at_r, lanes).astype(F32))
                        ud[at_r, lanes] = (da[r:r + strip, lanes] * slope).astype(BF16)
                        at[lanes, at_r] = a.astype(BF16).T

            def da_of(at_t):
                return lax.dot_general(dy[at_t, :], w2[...], (((1,), (1,)), ((), ())), preferred_element_type=F32)

            with jax.named_scope("wait_w1"):
                wait_for(w1, local.at[W1_IN])

            @pl.when(n == 0)
            def _():
                def u_step(t, carry):
                    at_t = pl.ds(pl.multiple_of(t * 2 * up_tile, up_tile), 2 * up_tile)
                    ud[at_t, :] = jnp.dot(x[at_t, :], w1[...], preferred_element_type=F32).astype(BF16)

                    @pl.when(t == 1)
                    def _():
                        with jax.named_scope("dyr"):
                            wait_for(dyr_hbm, pair_recv.at[2])
                        copy(dyr_hbm, dy.at[theirs], local.at[DY_IN]).start()

                    @pl.when(t == 2)
                    def _():
                        with jax.named_scope("ag021"):
                            ag_wait(0, 2, (1,))
                        load_down(0)

                    return carry

                with jax.named_scope("u0"):
                    lax.fori_loop(0, UP_TILES // 2, u_step, 0)
                with jax.named_scope("wait_100"):
                    ag_wait(1, 0, (0,))
                ag_start(1, 1, (0,))
                with jax.named_scope("first_w2"):
                    wait_for(dy, local.at[DY_IN])
                    wait_for(w2, local.at[W2_IN])

                def da_step(t, carry):
                    for part in range(PARTS):
                        first = t * up_tile + part * size
                        da = da_of(pl.ds(pl.multiple_of(first, size), size))
                        use(first, lambda r, at_r, lanes: ud[at_r, lanes], da)

                    for when, s, i in ((0, 0, 1), (3, 1, 0), (6, 1, 1)):
                        @pl.when(t == when)
                        def _(s=s, i=i):
                            with jax.named_scope(f"wait_1{s}{i}"):
                                ag_wait(1, s, (i,))
                            ag_start(1, s + 1, (i,))

                    return carry

                with jax.named_scope("da0"):
                    lax.fori_loop(0, UP_TILES, da_step, 0)
                with jax.named_scope("wait_20"):
                    ag_wait(2, 0)
                ag_start(2, 1)
                ag_start(3, 0)

            def up_step(t, carry):
                for part in range(PARTS):
                    first = t * up_tile + part * size
                    at_t = pl.ds(pl.multiple_of(first, size), size)
                    u = jnp.dot(x[at_t, :], w1[...], preferred_element_type=F32).astype(BF16)
                    da = da_of(at_t)
                    use(first, lambda r, at_r, lanes, u=u: u[r:r + strip, lanes], da)

                @pl.when((t == 2) & (n == 1))
                def _():
                    with jax.named_scope("wait_30"):
                        ag_wait(3, 0)
                    ag_start(3, 1)
                    ag_start(4, 0)

                @pl.when(t == 2)
                def _():
                    send_down(n - 1)

                    @pl.when(n > nc - 4)
                    def _():
                        send_first(p1, ra1, n - 1)

                    @pl.when((n > 2) & (n < nc - 1))
                    def _():
                        send_first(p1, ra1, n - 3)

                @pl.when((t == 6) & (n == nc - 2))
                def _():
                    early(0)

                @pl.when((t == 6) & (n == nc - 1))
                def _():
                    early(3)

                return carry

            @pl.when(n > 0)
            def _():
                with jax.named_scope("wait_w2"):
                    wait_for(w2, local.at[W2_IN])
                with jax.named_scope("up"):
                    lax.fori_loop(0, UP_TILES, up_step, 0)

            copy(ud, du_hbm.at[n], local.at[DU_OUT]).start()

            @pl.when(n == nc - 1)
            def _():
                early(4)

            def down_grad(k, carry):
                part = pl.ds(pl.multiple_of(k * cols, cols), cols)
                s2[:, part] = jnp.dot(at[...], dy[:, part], preferred_element_type=F32).astype(BF16)
                return carry

            with jax.named_scope("down_grad"):
                lax.fori_loop(0, 3, down_grad, 0)
            for k in range(COLOURS):
                for m in range(CHIPS):
                    copy(s2.at[down_rows(k, m, REDUCE), down_cols(k)], p2.at[n, k, m], local.at[G2_OUT]).start()

            @pl.when((n > 0) & (n + 2 < nc))
            def _():
                with jax.named_scope("wait_ag1"):
                    ag_wait(n + 2, 1)
                ag_start(n + 2, 2)

            @pl.when((n > 0) & (n + 3 < nc))
            def _():
                with jax.named_scope("wait_ag0"):
                    ag_wait(n + 3, 0)
                ag_start(n + 3, 1)

            @pl.when((n > 0) & (n + 4 < nc))
            def _():
                ag_start(n + 4, 0)

            @pl.when(n == nc - 2)
            def _():
                early(1)

            @pl.when(n == nc - 1)
            def _():
                early(5)

            def up_grad(k, carry):
                part = pl.ds(pl.multiple_of(k * cols, cols), cols)

                @pl.when((k == 2) & (n + 1 < nc))
                def _():
                    with jax.named_scope("wait_ag2"):
                        ag_wait(n + 1, 2)
                    load_up(n + 1)
                    load_down(n + 1)

                s1[part, :] = lax.dot_general(
                    x[:, part], ud[...], (((0,), (0,)), ((), ())), preferred_element_type=F32).astype(BF16)
                return carry

            with jax.named_scope("up_grad"):
                lax.fori_loop(0, 3, up_grad, 0)
            for k in range(COLOURS):
                for m in range(CHIPS):
                    copy(s1.at[up_rows(k, m, REDUCE)], p1.at[n, k, m], local.at[G1_OUT]).start()

            @pl.when(n == 0)
            def _():
                with jax.named_scope("wait_21"):
                    ag_wait(2, 1)
                ag_start(2, 2)

            @pl.when(n == nc - 2)
            def _():
                early(2)

            wait_for(ud, local.at[DU_OUT])
            return carry

        lax.fori_loop(0, nc, chunk, 0)
        send_down(nc - 1)
        send_first(p1, ra1, nc - 1)

    pl.run_scoped(
        main,
        pltpu.VMEM((both, width), BF16), pltpu.VMEM((both, width), BF16),
        pltpu.VMEM((width, fc), BF16), pltpu.VMEM((fc, width), BF16),
        pltpu.VMEM((both, fc), BF16), pltpu.VMEM((fc, both), BF16),
        pltpu.VMEM((width, fc), BF16), pltpu.VMEM((fc, width), BF16),
        pltpu.VMEM((12, rows, fc), BF16), pltpu.VMEM((12, units, cols), BF16),
        pltpu.VMEM((3, 2, rows, fc), BF16), pltpu.VMEM((3, 2, units, cols), BF16))

    dx_tile = both // DX_TILES
    half_tiles = DX_TILES // 2
    steps = 3 * DX_TILES
    own_from = 3 * half_tiles
    hidden = nc * fc

    def last(w, du, wide, out16, res,
             co1, co2, do1, do2, e1, e2, eo1, eo2):
        def load_w(n, third_):
            for p in range(CHIPS):
                piece = CHIPS * third_ + p
                r, k = divmod(piece, COLOURS)
                m = 0
                for i in range(3):
                    d = (k + i) % 3
                    m = m + (1 << i) * ((1 - bits[d]) if (r >> d) & 1 else bits[d])
                copy(a1.at[n, k, m], w.at[pl.ds(piece * rows, rows), pl.ds(pl.multiple_of(n * fc, fc), fc)],
                     w_sem.at[third_]).start()

        def tokens_at(q):
            later = q // half_tiles
            owner = (1 - later) * (1 - core) + later * core
            return pl.multiple_of(owner * tokens + (q % half_tiles) * dx_tile, dx_tile)

        def load_du(q):
            slot = q % 2
            for n in range(nc):
                copy(du_hbm.at[n, pl.ds(tokens_at(q), dx_tile)], du.at[slot, :, pl.ds(n * fc, fc)], local.at[TILE_IN + slot]).start()

        for third_ in range(COLOURS):
            lax.fori_loop(0, nc, lambda n, carry, third_=third_: (load_w(n, third_), carry)[1], 0)
            if third_ == 0:
                load_du(0)

        def own_at(q, n):
            return (pl.ds(pl.multiple_of((q % half_tiles) * dx_tile, dx_tile), dx_tile), pl.ds(pl.multiple_of(n * cols, cols), cols))

        def c_in(n):
            c_load(n, e1, e2, local.at[C_IN])

        def c_send(n):
            to1, to2 = co1.at[n - EARLY], co2.at[n - EARLY]
            c_sum(e1, e2, to1, to2, local.at[C_IN])
            for k in range(COLOURS):
                rs_start(n, 1, k, to1.at[k], to2.at[k])

        def sum_of(e, k, terms):
            total = e[k].astype(F32)
            for i in range(1, terms):
                total = total + e[3 * i + k].astype(F32)
            return total.astype(BF16)

        def d_load(n):
            with jax.named_scope("wait_rs1"):
                rs_wait(n, 1)
            for i, (b1, b2) in enumerate(((p1, p2), (ra1, ra2), (rb1, rb2))):
                for k in range(COLOURS):
                    copy(b1.at[n, k, 1], e1.at[3 * i + k], local.at[D_IN]).start()
                    copy(b2.at[n, k, 1], e2.at[3 * i + k], local.at[D_IN]).start()

        def d_send(n):
            wait_for(e1.at[pl.ds(0, 9)], local.at[D_IN])
            wait_for(e2.at[pl.ds(0, 9)], local.at[D_IN])

            for k in range(COLOURS):
                do1[n, k] = sum_of(e1, k, 3)
                do2[n, k] = sum_of(e2, k, 3)
                rs_start(n, 2, k, do1.at[n, k], do2.at[n, k])

        def e_load(n):
            with jax.named_scope("wait_rs2"):
                rs_wait(n, 2)
            for i, (b1, b2) in enumerate(((p1, p2), (ra1, ra2), (rb1, rb2))):
                for k in range(COLOURS):
                    copy(b1.at[n, k, 0], e1.at[3 * i + k], local.at[E_IN]).start()
                    copy(b2.at[n, k, 0], e2.at[3 * i + k], local.at[E_IN]).start()
            copy(rc1.at[n], e1.at[pl.ds(9, 3)], local.at[E_IN]).start()
            copy(rc2.at[n], e2.at[pl.ds(9, 3)], local.at[E_IN]).start()

        keep = pl.ds(pl.multiple_of(core * half, 16), half)
        give = pl.ds(pl.multiple_of((1 - core) * half, 16), half)

        def e_wait_out(n):
            wait_for(gup_hbm.at[0, 0], local.at[GUP_OUT])
            wait_for(gdown_hbm.at[pl.ds(0, units)], local.at[GDOWN_OUT])
            wait_for(gup_hbm.at[0, 0], gup_send.at[n])

        def e_store(n):
            wait_for(e1, local.at[E_IN])
            wait_for(e2, local.at[E_IN])

            @pl.when(n > 0)
            def _():
                e_wait_out(n - 1)

            for k in range(COLOURS):
                eo1[k * rows:(k + 1) * rows, :] = sum_of(e1, k, 4)
                eo2[:, k * cols:(k + 1) * cols] = sum_of(e2, k, 4)
            copy(eo1.at[keep], gup_hbm.at[core, n], local.at[GUP_OUT]).start()
            copy(eo2, gdown_hbm.at[pl.ds(pl.multiple_of(n * units, 16), units)], local.at[GDOWN_OUT]).start()
            pltpu.make_async_remote_copy(
                src_ref=eo1.at[give], dst_ref=gup_hbm.at[core, n], send_sem=gup_send.at[n], recv_sem=gup_recv.at[n],
                device_id=(partner,), device_id_type=MESH).start()

        def pump(i):
            for start, low, high, load, finish_ in (
                    (0, EARLY, nc - 1, c_in, c_send), (7, nc - 1, nc, c_in, c_send), (8, 0, nc, d_load, d_send), (17, 0, nc, e_load, e_store)):
                n = i - start + low

                @pl.when((n > low) & (n <= high))
                def _(finish_=finish_, n=n):
                    finish_(n - 1)

                @pl.when((n >= low) & (n < high))
                def _(load=load, n=n):
                    load(n)

        def step(i, carry):
            q, n = i // 3, i % 3
            slot = i % 2

            @pl.when((i < steps) & (n == 0))
            def _():
                @pl.when(q + 1 < DX_TILES)
                def _():
                    load_du(q + 1)

                with jax.named_scope("wait_du"):
                    wait_for(du.at[0], local.at[TILE_IN + q % 2])

            @pl.when(i < 3)
            def _():
                with jax.named_scope("wait_wall"):
                    wait_for(w.at[pl.ds(0, cols)], w_sem.at[n])

            @pl.when((i >= own_from - 1) & (i < steps - 1))
            def _():
                here = own_at((i + 1) // 3, (i + 1) % 3)
                with jax.named_scope("wait_dxr"):
                    wait_for(dxr_hbm.at[here], dx_recv.at[i + 1 - own_from])

                @pl.when(i < own_from + 2)
                def _():
                    wait_for(wide.at[0], dx_send.at[i - 2])

                copy(dxr_hbm.at[here], wide.at[(i + 1) % 3], local.at[GOT_IN + 1 - slot]).start()
                copy(dy_hbm.at[here], res.at[1 - slot], local.at[RES_IN + 1 - slot]).start()

            @pl.when((i >= 3) & (i < own_from))
            def _():
                with jax.named_scope("wait_dxs"):
                    wait_for(wide.at[0], dx_send.at[i - 3])

            @pl.when((i >= own_from + 2) & (i < steps))
            def _():
                wait_for(out16.at[0], local.at[DX_OUT + slot])

            def dot():
                part = pl.ds(pl.multiple_of(n * cols, cols), cols)
                return lax.dot_general(du[q % 2], w[part, :], (((1,), (1,)), ((), ())), preferred_element_type=F32)

            @pl.when(i < own_from)
            def _():
                with jax.named_scope("dx_dot"):
                    wide[i % 3] = dot()
                pltpu.make_async_remote_copy(
                    src_ref=wide.at[i % 3], dst_ref=dxr_hbm.at[own_at(q, n)], send_sem=dx_send.at[i], recv_sem=dx_recv.at[i],
                    device_id=(partner,), device_id_type=MESH).start()

            @pl.when((i >= own_from) & (i < steps))
            def _():
                with jax.named_scope("wait_got"):
                    wait_for(wide.at[0], local.at[GOT_IN + slot])
                    wait_for(res.at[0], local.at[RES_IN + slot])
                with jax.named_scope("dx_dot2"):
                    out16[slot] = (res[slot].astype(F32) + (dot() + wide[i % 3])).astype(BF16)
                copy(out16.at[slot], dx_hbm.at[own_at(q, n)], local.at[DX_OUT + slot]).start()

            pump(i)
            return carry

        lax.fori_loop(0, max(steps, nc + 18), step, 0)
        for slot in range(2):
            wait_for(out16.at[0], local.at[DX_OUT + slot])
        e_wait_out(nc - 1)
        for n in range(nc):
            wait_for(sized[1].at[0], rs_send.at[1, n])
            wait_for(sized[0].at[0], rs_send.at[2, n])

    pl.run_scoped(
        last,
        pltpu.VMEM((width, hidden), BF16), pltpu.VMEM((2, dx_tile, hidden), BF16),
        pltpu.VMEM((3, dx_tile, cols), F32), pltpu.VMEM((2, dx_tile, cols), BF16), pltpu.VMEM((2, dx_tile, cols), BF16),
        pltpu.VMEM((nc - EARLY, 3, 2, rows, fc), BF16), pltpu.VMEM((nc - EARLY, 3, 2, units, cols), BF16),
        pltpu.VMEM((nc, 3, rows, fc), BF16), pltpu.VMEM((nc, 3, units, cols), BF16),
        pltpu.VMEM((12, rows, fc), BF16), pltpu.VMEM((12, units, cols), BF16),
        pltpu.VMEM((3 * rows, fc), BF16), pltpu.VMEM((units, width), BF16))

    def drain(n, carry):
        for s in range(3):
            for i in range(2):
                wait_for(one_array[s].at[n], ag_send.at[i, s, n])
        wait_for(sized[2].at[n], rs_send.at[0, n])
        wait_for(gup_hbm.at[0, 0], gup_recv.at[n])
        return carry

    with jax.named_scope("drain"):
        lax.fori_loop(0, nc, drain, 0)
    wait_for(xr_hbm, pair_send.at[1])
    wait_for(dyr_hbm, pair_send.at[2])


def finish(nc, units, gup, gdown, dx, gup_out, gdown_out, dx_out, v_in, v_out, v_down, v_dx, sem_in, sem_out):
    pieces = v_dx.shape[0]
    rows = v_dx.shape[1]
    copy(gup, v_in, sem_in.at[pieces]).start()
    copy(gdown, v_down, sem_in.at[pieces + 1]).start()
    for i in range(pieces):
        copy(dx.at[pl.ds(i * rows, rows)], v_dx.at[i], sem_in.at[i]).start()
    copy(gup, v_in, sem_in.at[pieces]).wait()
    per = 128 // math.gcd(128, units)
    for first in range(0, CHIPS * CORES * nc, per):
        parts = []
        for u in range(first, first + per):
            d, n = u // nc, u % nc
            r, c = d // CORES, d % CORES
            parts.append(v_in[c, n, :, r * units:(r + 1) * units])
        v_out[:, first * units:(first + per) * units] = jnp.concatenate(parts, axis=1)
    copy(v_out, gup_out, sem_out.at[pieces]).start()
    copy(gdown, v_down, sem_in.at[pieces + 1]).wait()
    copy(v_down, gdown_out, sem_out.at[pieces + 1]).start()
    for i in range(pieces):
        copy(dx.at[pl.ds(i * rows, rows)], v_dx.at[i], sem_in.at[i]).wait()
        copy(v_dx.at[i], dx_out.at[pl.ds(i * rows, rows)], sem_out.at[i]).start()
    copy(v_out, gup_out, sem_out.at[pieces]).wait()
    copy(v_down, gdown_out, sem_out.at[pieces + 1]).wait()
    for i in range(pieces):
        copy(v_dx.at[i], dx_out.at[pl.ds(i * rows, rows)], sem_out.at[i]).wait()


def solution(mesh):
    def device_fn(x_loc, dy_loc, up_loc, down_loc):
        width = x_loc.shape[-1]
        x = x_loc.reshape(-1, width)
        dy = dy_loc.reshape(-1, width)
        tokens = x.shape[0]
        down = down_loc[0]
        half, units_all = up_loc.shape[1], down.shape[0]
        nc = CHUNKS
        units = units_all // nc
        fc = CHIPS * units
        rows, cols = 2 * half // 3, width // 3
        up = up_loc[0]

        def hbm(*shape, dtype=BF16):
            return jax.ShapeDtypeStruct(shape, dtype)

        one, two = (rows, fc), (units, cols)
        outs = [
            hbm(CORES, nc, half, fc), hbm(units_all, width), hbm(tokens, width),
            hbm(tokens, width), hbm(tokens, width),
            *[hbm(nc, 3, blocks, *s) for blocks in (8, 8, 4, 2) for s in (one, two)],
            hbm(nc, 3, *one), hbm(nc, 3, *two), hbm(nc, 3, 2, *one), hbm(nc, 3, 2, *two),
            hbm(nc, 2 * tokens, fc), hbm(tokens, width, dtype=F32),
        ]
        dma = pltpu.SemaphoreType.DMA
        half_steps = 3 * DX_TILES // 2
        got = pl.pallas_call(
            functools.partial(kernel, nc),
            out_shape=outs,
            in_specs=[pl.BlockSpec(memory_space=pl.ANY)] * 4,
            out_specs=[pl.BlockSpec(memory_space=pl.ANY)] * len(outs),
            scratch_shapes=[
                dma((2, 3, nc)), dma((2, 3, nc)), dma((3, nc)), dma((3, nc)), dma((3,)), dma((4,)),
                dma((half_steps,)), dma((half_steps,)), dma((nc,)), dma((nc,)), dma((3,)), dma((13,)),
            ],
            compiler_params=pltpu.CompilerParams(
                collective_id=0, has_side_effects=True, vmem_limit_bytes=VMEM_BYTES),
        )(x, dy, up, down)
        pieces = 8
        g_up, g_down, dx = pl.pallas_call(
            functools.partial(finish, nc, units),
            out_shape=[hbm(half, up.shape[1]), hbm(units_all, width), hbm(tokens, width)],
            in_specs=[pl.BlockSpec(memory_space=pl.ANY)] * 3,
            out_specs=[pl.BlockSpec(memory_space=pl.ANY)] * 3,
            scratch_shapes=[
                pltpu.VMEM((CORES, nc, half, fc), BF16), pltpu.VMEM((half, up.shape[1]), BF16),
                pltpu.VMEM((units_all, width), BF16), pltpu.VMEM((pieces, tokens // pieces, width), BF16),
                dma((pieces + 2,)), dma((pieces + 2,)),
            ],
            compiler_params=pltpu.CompilerParams(vmem_limit_bytes=VMEM_BYTES),
        )(*got[:3])
        return g_up[None], g_down[None], dx.reshape(x_loc.shape)

    return jax.shard_map(
        device_fn, mesh=mesh, in_specs=(P("data"), P("data"), P(None, "data"), P(None, "data")),
        out_specs=(P(None, "data"), P(None, "data"), P("data")), check_vma=False)
```

```python
import functools
import math

import jax
import jax.numpy as jnp
from jax import lax
from jax.experimental import pallas as pl
from jax.experimental.pallas import tpu as pltpu
from jax.sharding import PartitionSpec as P

MESH = pl.DeviceIdType.MESH
F32, BF16 = jnp.float32, jnp.bfloat16
CHIPS, COLOURS, CORES = 8, 3, 2
CHUNKS = 9
VMEM_BYTES = 67_000_000
DX_TILES = 8
UP_TILES = 8
PARTS = 2
UP_IN, X_IN, DY_IN, W1_IN, W2_IN, G1_OUT, G2_OUT, DU_OUT, SUM_IN, SUM_OUT, OWN_0, OWN_1, OWN_2 = range(13)
TILE_IN, GOT_IN, RES_IN, DX_OUT = range(0, 8, 2)
C_IN, D_IN, E_IN, GUP_OUT, GDOWN_OUT = range(8, 13)
EARLY = 4


def copy(src, dst, sem):
    return pltpu.make_async_copy(src, dst, sem)


def wait_for(ref, sem):
    pltpu.make_async_copy(ref, ref, sem).wait()


def gelu_both(u):
    scale = math.sqrt(2.0 / math.pi)
    square = u * u
    th = jnp.tanh(u * (scale + (0.044715 * scale) * square))
    half = 0.5 * th
    cdf = 0.5 + half
    slope = cdf + (u * (0.5 - th * half)) * (scale + (0.134145 * scale) * square)
    return u * cdf, slope


def kernel(nc, x_hbm, dy_hbm, up_hbm, down_hbm,
           gup_hbm, gdown_hbm, dx_hbm,
           xr_hbm, dyr_hbm, a1, a2, p1, p2, ra1, ra2, rb1, rb2, rc1, rc2, cb1, cb2, du_hbm, dxr_hbm,
           ag_send, ag_recv, rs_send, rs_recv, pair_send, pair_recv, dx_send, dx_recv, gup_send, gup_recv, w_sem, local):
    me = lax.axis_index("data")
    core = me % 2
    bits = [(me // 2) % 2, (me // 4) % 2, (me // 8) % 2]
    partner = me + 1 - 2 * core
    near = [me + (2 << d) * (1 - 2 * bits[d]) for d in range(3)]

    tokens, width = x_hbm.shape
    both = 2 * tokens
    *_, rows, fc = a1.shape
    *_, units, cols = a2.shape
    half = up_hbm.shape[0]
    third = half // 3

    def chip(colour, m, order):
        total = 0
        for i in range(3):
            d = (colour + i) % 3
            flipped = (m >> order[i]) & 1
            total = total + (1 << d) * ((1 - bits[d]) if flipped else bits[d])
        return total

    GATHER, REDUCE = (0, 1, 2), (2, 1, 0)

    def up_rows(colour, m, order):
        return pl.ds(pl.multiple_of(chip(colour, m, order) * (3 * rows) + colour * rows, 16), rows)

    def down_rows(colour, m, order):
        return pl.ds(pl.multiple_of(chip(colour, m, order) * units, 16), units)

    def down_cols(colour):
        return pl.ds(colour * cols, cols)

    def ag_start(n, s, arrays=(0, 1)):
        have = 1 << s
        for k in range(COLOURS):
            for i in arrays:
                buf = (a1, a2)[i]
                pltpu.make_async_remote_copy(
                    src_ref=buf.at[n, k, pl.ds(0, have)], dst_ref=buf.at[n, k, pl.ds(have, have)],
                    send_sem=ag_send.at[i, s, n], recv_sem=ag_recv.at[i, s, n],
                    device_id=(near[(k + s) % 3],), device_id_type=MESH).start()

    one_array = (rc1, rb1, ra1)
    sized = (rb1, ra1, p1)

    def ag_wait(n, s, arrays=(0, 1)):
        for i in arrays:
            wait_for(one_array[s].at[n], ag_recv.at[i, s, n])

    def rs_start(n, s, k, src1, src2):
        dst1, dst2 = ((ra1, ra2), (rb1, rb2), (rc1, rc2))[s]
        for src, dst in ((src1, dst1), (src2, dst2)):
            pltpu.make_async_remote_copy(
                src_ref=src, dst_ref=dst.at[n, k], send_sem=rs_send.at[s, n], recv_sem=rs_recv.at[s, n],
                device_id=(near[(k + s) % 3],), device_id_type=MESH).start()

    def rs_wait(n, s):
        wait_for(sized[2 - s].at[n], rs_recv.at[s, n])

    barrier = pltpu.get_barrier_semaphore()
    for other in (partner, *near):
        pl.semaphore_signal(barrier, inc=1, device_id=(other,), device_id_type=MESH)

    def to_partner(src, dst, i):
        pltpu.make_async_remote_copy(
            src_ref=src, dst_ref=dst, send_sem=pair_send.at[i], recv_sem=pair_recv.at[i],
            device_id=(partner,), device_id_type=MESH).start()

    mine = pl.ds(pl.multiple_of(core * tokens, 16), tokens)
    theirs = pl.ds(pl.multiple_of((1 - core) * tokens, 16), tokens)

    def c_load(n, c1, c2, sem):
        with jax.named_scope("wait_rs0"):
            rs_wait(n, 0)
        for i, (b1, b2) in enumerate(((p1, p2), (ra1, ra2))):
            for k in range(COLOURS):
                pair = pl.ds(2 * (3 * i + k), 2)
                copy(b1.at[n, k, pl.ds(2, 2)], c1.at[pair], sem).start()
                copy(b2.at[n, k, pl.ds(2, 2)], c2.at[pair], sem).start()

    def c_sum(c1, c2, to1, to2, sem):
        wait_for(p1.at[0], sem)
        for k in range(COLOURS):
            for j in range(2):
                to1[k, j] = c1[2 * k + j] + c1[2 * k + j + 6]
                to2[k, j] = c2[2 * k + j] + c2[2 * k + j + 6]

    def main(x, dy, w1, w2, ud, at, s1, s2, c1, c2, co1, co2):
        own_down = x.at[pl.ds(0, nc * units)]
        blocks = up_hbm.shape[1] // width
        for b in range(blocks):
            copy(up_hbm.at[:, pl.ds(b * width, width)], x.at[pl.ds(nc * units + b * half, half)], local.at[UP_IN]).start()
        copy(down_hbm, own_down, local.at[X_IN]).start()
        with jax.named_scope("entry"):
            pl.semaphore_wait(barrier, 4)
        for k in range(COLOURS):
            pltpu.make_async_remote_copy(
                src_ref=down_hbm.at[pl.ds(0, units), down_cols(k)], dst_ref=a2.at[0, k, 1],
                send_sem=ag_send.at[1, 0, 0], recv_sem=ag_recv.at[1, 0, 0],
                device_id=(near[k],), device_id_type=MESH).start()
        wait_for(up_hbm, local.at[UP_IN])

        def unit(chip_, core_, n):
            first = ((chip_ * CORES + core_) * nc + n) * units
            b, c = first // width, first % width
            return x[nc * units + b * half:nc * units + (b + 1) * half, c:c + units]

        whole = pl.ds(pl.multiple_of(core * third, 16), 2 * third)
        rest = pl.ds(pl.multiple_of((1 - core) * 2 * third, 16), third)
        to_rest = pl.ds(pl.multiple_of(core * third, 16), third)

        def permute(n):
            for c in range(CORES):
                first = (n * CORES + c) * half
                ud[first:first + half, :] = jnp.concatenate([unit(r, c, n) for r in range(CHIPS)], axis=1)

        def own_up(n):
            def part(c, which):
                return ud.at[pl.ds(pl.multiple_of((n * CORES + c) * half + which.start, 16), which.size)]

            sem = min(n, 1)
            for which, dst in ((whole, a1.at[n, 2 * core, 0]), (rest, a1.at[n, 1, 0, to_rest])):
                pltpu.make_async_remote_copy(
                    src_ref=part(1 - core, which), dst_ref=dst, send_sem=pair_send.at[0], recv_sem=pair_recv.at[3 * sem],
                    device_id=(partner,), device_id_type=MESH).start()
                copy(part(core, which), dst, local.at[OWN_0 + sem]).start()

        def down_own(n):
            for k in range(COLOURS):
                copy(x.at[pl.ds(n * units, units), down_cols(k)], a2.at[n, k, 0], local.at[OWN_2 if n else X_IN]).start()

        permute(0)
        own_up(0)
        wait_for(down_hbm, local.at[X_IN])
        for n in range(nc):
            down_own(n)
        for n in range(1, 4):
            permute(n)
        with jax.named_scope("own_wait"):
            wait_for(du_hbm.at[0, pl.ds(0, half)], local.at[OWN_0])
            wait_for(du_hbm.at[0, pl.ds(0, half)], pair_recv.at[0])
        ag_start(0, 0, (0,))
        for n in range(4, nc):
            permute(n)
        for n in range(1, nc):
            own_up(n)
        to_partner(x_hbm, xr_hbm, 1)
        to_partner(dy_hbm, dyr_hbm, 2)
        wait_for(down_hbm.at[pl.ds(0, units)], local.at[X_IN])
        wait_for(down_hbm.at[pl.ds(0, (nc - 1) * units)], local.at[OWN_2])
        ag_start(1, 0, (1,))
        copy(x_hbm, x.at[mine], local.at[X_IN]).start()
        copy(dy_hbm, dy.at[mine], local.at[DY_IN]).start()
        def load_up(n, blocks=range(CHIPS)):
            for k in range(COLOURS):
                for m in blocks:
                    copy(a1.at[n, k, m], w1.at[up_rows(k, m, GATHER)], local.at[W1_IN]).start()

        for s in range(2):
            for i in range(2):
                with jax.named_scope(f"ag0{s}{i}"):
                    ag_wait(0, s, (i,))
                ag_start(0, s + 1, (i,))
        wait_for(du_hbm.at[0, pl.ds(0, (nc - 1) * half)], local.at[OWN_1])
        wait_for(du_hbm.at[0, pl.ds(0, (nc - 1) * half)], pair_recv.at[3])
        ag_start(1, 0, (0,))
        ag_start(2, 0)
        with jax.named_scope("xr"):
            wait_for(xr_hbm, pair_recv.at[1])
        copy(xr_hbm, x.at[theirs], local.at[X_IN]).start()
        load_up(0, range(4))

        def load_down(n):
            for k in range(COLOURS):
                for m in range(CHIPS):
                    copy(a2.at[n, k, m], w2.at[down_rows(k, m, GATHER), down_cols(k)], local.at[W2_IN]).start()

        with jax.named_scope("ag020"):
            ag_wait(0, 2, (0,))
        load_up(0, range(4, CHIPS))
        with jax.named_scope("tokens"):
            wait_for(x, local.at[X_IN])
            wait_for(du_hbm.at[0, pl.ds(0, nc * half)], pair_send.at[0])

        def send_first(src, dst, n):
            for k in range(COLOURS):
                pltpu.make_async_remote_copy(
                    src_ref=src.at[n, k, pl.ds(4, 4)], dst_ref=dst.at[n, k], send_sem=rs_send.at[0, n],
                    recv_sem=rs_recv.at[0, n], device_id=(near[k],), device_id_type=MESH).start()

        def send_down(n):
            wait_for(p1.at[0], local.at[G1_OUT])
            wait_for(p2.at[0], local.at[G2_OUT])
            send_first(p2, ra2, n)

        def c_in(n):
            c_load(n, c1, c2, local.at[SUM_IN])

        def c_add(n):
            c_sum(c1, c2, co1, co2, local.at[SUM_IN])
            copy(co1, cb1.at[n], local.at[SUM_OUT]).start()
            copy(co2, cb2.at[n], local.at[SUM_OUT]).start()

        def c_go(n):
            wait_for(sized[1].at[0], local.at[SUM_OUT])
            for k in range(COLOURS):
                rs_start(n, 1, k, cb1.at[n, k], cb2.at[n, k])

        def early(slot):
            if slot > 1:
                c_go(slot - 2)
            if 0 < slot <= EARLY:
                c_add(slot - 1)
            if slot < EARLY:
                c_in(slot)

        up_tile = both // UP_TILES

        def chunk(n, carry):
            size = up_tile // PARTS
            strip = min(128, size)

            def use(first, u, da):
                for c in range(0, fc, 128):
                    lanes = slice(c, c + 128)
                    for r in range(0, size, strip):
                        at_r = pl.ds(pl.multiple_of(first + r, strip), strip)
                        a, slope = gelu_both(u(r, at_r, lanes).astype(F32))
                        ud[at_r, lanes] = (da[r:r + strip, lanes] * slope).astype(BF16)
                        at[lanes, at_r] = a.astype(BF16).T

            def da_of(at_t):
                return lax.dot_general(dy[at_t, :], w2[...], (((1,), (1,)), ((), ())), preferred_element_type=F32)

            with jax.named_scope("wait_w1"):
                wait_for(w1, local.at[W1_IN])

            @pl.when(n == 0)
            def _():
                def u_step(t, carry):
                    at_t = pl.ds(pl.multiple_of(t * 2 * up_tile, up_tile), 2 * up_tile)
                    ud[at_t, :] = jnp.dot(x[at_t, :], w1[...], preferred_element_type=F32).astype(BF16)

                    @pl.when(t == 1)
                    def _():
                        with jax.named_scope("dyr"):
                            wait_for(dyr_hbm, pair_recv.at[2])
                        copy(dyr_hbm, dy.at[theirs], local.at[DY_IN]).start()

                    @pl.when(t == 2)
                    def _():
                        with jax.named_scope("ag021"):
                            ag_wait(0, 2, (1,))
                        load_down(0)

                    return carry

                with jax.named_scope("u0"):
                    lax.fori_loop(0, UP_TILES // 2, u_step, 0)
                with jax.named_scope("wait_100"):
                    ag_wait(1, 0, (0,))
                ag_start(1, 1, (0,))
                with jax.named_scope("first_w2"):
                    wait_for(dy, local.at[DY_IN])
                    wait_for(w2, local.at[W2_IN])

                def da_step(t, carry):
                    for part in range(PARTS):
                        first = t * up_tile + part * size
                        da = da_of(pl.ds(pl.multiple_of(first, size), size))
                        use(first, lambda r, at_r, lanes: ud[at_r, lanes], da)

                    for when, s, i in ((0, 0, 1), (3, 1, 0), (6, 1, 1)):
                        @pl.when(t == when)
                        def _(s=s, i=i):
                            with jax.named_scope(f"wait_1{s}{i}"):
                                ag_wait(1, s, (i,))
                            ag_start(1, s + 1, (i,))

                    return carry

                with jax.named_scope("da0"):
                    lax.fori_loop(0, UP_TILES, da_step, 0)
                with jax.named_scope("wait_20"):
                    ag_wait(2, 0)
                ag_start(2, 1)
                ag_start(3, 0)

            def up_step(t, carry):
                for part in range(PARTS):
                    first = t * up_tile + part * size
                    at_t = pl.ds(pl.multiple_of(first, size), size)
                    u = jnp.dot(x[at_t, :], w1[...], preferred_element_type=F32).astype(BF16)
                    da = da_of(at_t)
                    use(first, lambda r, at_r, lanes, u=u: u[r:r + strip, lanes], da)

                @pl.when((t == 2) & (n == 1))
                def _():
                    with jax.named_scope("wait_30"):
                        ag_wait(3, 0)
                    ag_start(3, 1)
                    ag_start(4, 0)

                @pl.when(t == 2)
                def _():
                    send_down(n - 1)

                    @pl.when(n > nc - 4)
                    def _():
                        send_first(p1, ra1, n - 1)

                    @pl.when((n > 2) & (n < nc - 1))
                    def _():
                        send_first(p1, ra1, n - 3)

                @pl.when((t == 6) & (n == nc - 2))
                def _():
                    early(0)

                @pl.when((t == 6) & (n == nc - 1))
                def _():
                    early(3)

                return carry

            @pl.when(n > 0)
            def _():
                with jax.named_scope("wait_w2"):
                    wait_for(w2, local.at[W2_IN])
                with jax.named_scope("up"):
                    lax.fori_loop(0, UP_TILES, up_step, 0)

            copy(ud, du_hbm.at[n], local.at[DU_OUT]).start()

            @pl.when(n == nc - 1)
            def _():
                early(4)

            def down_grad(k, carry):
                part = pl.ds(pl.multiple_of(k * cols, cols), cols)
                s2[:, part] = jnp.dot(at[...], dy[:, part], preferred_element_type=F32).astype(BF16)
                return carry

            with jax.named_scope("down_grad"):
                lax.fori_loop(0, 3, down_grad, 0)
            for k in range(COLOURS):
                for m in range(CHIPS):
                    copy(s2.at[down_rows(k, m, REDUCE), down_cols(k)], p2.at[n, k, m], local.at[G2_OUT]).start()

            @pl.when((n > 0) & (n + 2 < nc))
            def _():
                with jax.named_scope("wait_ag1"):
                    ag_wait(n + 2, 1)
                ag_start(n + 2, 2)

            @pl.when((n > 0) & (n + 3 < nc))
            def _():
                with jax.named_scope("wait_ag0"):
                    ag_wait(n + 3, 0)
                ag_start(n + 3, 1)

            @pl.when((n > 0) & (n + 4 < nc))
            def _():
                ag_start(n + 4, 0)

            @pl.when(n == nc - 2)
            def _():
                early(1)

            @pl.when(n == nc - 1)
            def _():
                early(5)

            def up_grad(k, carry):
                part = pl.ds(pl.multiple_of(k * cols, cols), cols)

                @pl.when((k == 2) & (n + 1 < nc))
                def _():
                    with jax.named_scope("wait_ag2"):
                        ag_wait(n + 1, 2)
                    load_up(n + 1)
                    load_down(n + 1)

                s1[part, :] = lax.dot_general(
                    x[:, part], ud[...], (((0,), (0,)), ((), ())), preferred_element_type=F32).astype(BF16)
                return carry

            with jax.named_scope("up_grad"):
                lax.fori_loop(0, 3, up_grad, 0)
            for k in range(COLOURS):
                for m in range(CHIPS):
                    copy(s1.at[up_rows(k, m, REDUCE)], p1.at[n, k, m], local.at[G1_OUT]).start()

            @pl.when(n == 0)
            def _():
                with jax.named_scope("wait_21"):
                    ag_wait(2, 1)
                ag_start(2, 2)

            @pl.when(n == nc - 2)
            def _():
                early(2)

            wait_for(ud, local.at[DU_OUT])
            return carry

        lax.fori_loop(0, nc, chunk, 0)
        send_down(nc - 1)
        send_first(p1, ra1, nc - 1)

    pl.run_scoped(
        main,
        pltpu.VMEM((both, width), BF16), pltpu.VMEM((both, width), BF16),
        pltpu.VMEM((width, fc), BF16), pltpu.VMEM((fc, width), BF16),
        pltpu.VMEM((both, fc), BF16), pltpu.VMEM((fc, both), BF16),
        pltpu.VMEM((width, fc), BF16), pltpu.VMEM((fc, width), BF16),
        pltpu.VMEM((12, rows, fc), BF16), pltpu.VMEM((12, units, cols), BF16),
        pltpu.VMEM((3, 2, rows, fc), BF16), pltpu.VMEM((3, 2, units, cols), BF16))

    dx_tile = both // DX_TILES
    half_tiles = DX_TILES // 2
    steps = 3 * DX_TILES
    own_from = 3 * half_tiles
    hidden = nc * fc

    def last(w, du, wide, out16, res,
             co1, co2, do1, do2, e1, e2, eo1, eo2):
        def load_w(n, third_):
            for p in range(CHIPS):
                piece = CHIPS * third_ + p
                r, k = divmod(piece, COLOURS)
                m = 0
                for i in range(3):
                    d = (k + i) % 3
                    m = m + (1 << i) * ((1 - bits[d]) if (r >> d) & 1 else bits[d])
                copy(a1.at[n, k, m], w.at[pl.ds(piece * rows, rows), pl.ds(pl.multiple_of(n * fc, fc), fc)],
                     w_sem.at[third_]).start()

        def tokens_at(q):
            later = q // half_tiles
            owner = (1 - later) * (1 - core) + later * core
            return pl.multiple_of(owner * tokens + (q % half_tiles) * dx_tile, dx_tile)

        def load_du(q):
            slot = q % 2
            for n in range(nc):
                copy(du_hbm.at[n, pl.ds(tokens_at(q), dx_tile)], du.at[slot, :, pl.ds(n * fc, fc)], local.at[TILE_IN + slot]).start()

        for third_ in range(COLOURS):
            lax.fori_loop(0, nc, lambda n, carry, third_=third_: (load_w(n, third_), carry)[1], 0)
            if third_ == 0:
                load_du(0)

        def own_at(q, n):
            return (pl.ds(pl.multiple_of((q % half_tiles) * dx_tile, dx_tile), dx_tile), pl.ds(pl.multiple_of(n * cols, cols), cols))

        def c_in(n):
            c_load(n, e1, e2, local.at[C_IN])

        def c_send(n):
            to1, to2 = co1.at[n - EARLY], co2.at[n - EARLY]
            c_sum(e1, e2, to1, to2, local.at[C_IN])
            for k in range(COLOURS):
                rs_start(n, 1, k, to1.at[k], to2.at[k])

        def sum_of(e, k, terms):
            total = e[k].astype(F32)
            for i in range(1, terms):
                total = total + e[3 * i + k].astype(F32)
            return total.astype(BF16)

        def d_load(n):
            with jax.named_scope("wait_rs1"):
                rs_wait(n, 1)
            for i, (b1, b2) in enumerate(((p1, p2), (ra1, ra2), (rb1, rb2))):
                for k in range(COLOURS):
                    copy(b1.at[n, k, 1], e1.at[3 * i + k], local.at[D_IN]).start()
                    copy(b2.at[n, k, 1], e2.at[3 * i + k], local.at[D_IN]).start()

        def d_send(n):
            wait_for(e1.at[pl.ds(0, 9)], local.at[D_IN])
            wait_for(e2.at[pl.ds(0, 9)], local.at[D_IN])

            for k in range(COLOURS):
                do1[n, k] = sum_of(e1, k, 3)
                do2[n, k] = sum_of(e2, k, 3)
                rs_start(n, 2, k, do1.at[n, k], do2.at[n, k])

        def e_load(n):
            with jax.named_scope("wait_rs2"):
                rs_wait(n, 2)
            for i, (b1, b2) in enumerate(((p1, p2), (ra1, ra2), (rb1, rb2))):
                for k in range(COLOURS):
                    copy(b1.at[n, k, 0], e1.at[3 * i + k], local.at[E_IN]).start()
                    copy(b2.at[n, k, 0], e2.at[3 * i + k], local.at[E_IN]).start()
            copy(rc1.at[n], e1.at[pl.ds(9, 3)], local.at[E_IN]).start()
            copy(rc2.at[n], e2.at[pl.ds(9, 3)], local.at[E_IN]).start()

        keep = pl.ds(pl.multiple_of(core * half, 16), half)
        give = pl.ds(pl.multiple_of((1 - core) * half, 16), half)

        def e_wait_out(n):
            wait_for(gup_hbm.at[0, 0], local.at[GUP_OUT])
            wait_for(gdown_hbm.at[pl.ds(0, units)], local.at[GDOWN_OUT])
            wait_for(gup_hbm.at[0, 0], gup_send.at[n])

        def e_store(n):
            wait_for(e1, local.at[E_IN])
            wait_for(e2, local.at[E_IN])

            @pl.when(n > 0)
            def _():
                e_wait_out(n - 1)

            for k in range(COLOURS):
                eo1[k * rows:(k + 1) * rows, :] = sum_of(e1, k, 4)
                eo2[:, k * cols:(k + 1) * cols] = sum_of(e2, k, 4)
            copy(eo1.at[keep], gup_hbm.at[core, n], local.at[GUP_OUT]).start()
            copy(eo2, gdown_hbm.at[pl.ds(pl.multiple_of(n * units, 16), units)], local.at[GDOWN_OUT]).start()
            pltpu.make_async_remote_copy(
                src_ref=eo1.at[give], dst_ref=gup_hbm.at[core, n], send_sem=gup_send.at[n], recv_sem=gup_recv.at[n],
                device_id=(partner,), device_id_type=MESH).start()

        def pump(i):
            for start, low, high, load, finish_ in (
                    (0, EARLY, nc - 1, c_in, c_send), (6, nc - 1, nc, c_in, c_send), (7, 0, nc, d_load, d_send), (16, 0, nc, e_load, e_store)):
                n = i - start + low

                @pl.when((n > low) & (n <= high))
                def _(finish_=finish_, n=n):
                    finish_(n - 1)

                @pl.when((n >= low) & (n < high))
                def _(load=load, n=n):
                    load(n)

        def step(i, carry):
            q, n = i // 3, i % 3
            slot = i % 2

            @pl.when((i < steps) & (n == 0))
            def _():
                @pl.when(q + 1 < DX_TILES)
                def _():
                    load_du(q + 1)

                with jax.named_scope("wait_du"):
                    wait_for(du.at[0], local.at[TILE_IN + q % 2])

            @pl.when(i < 3)
            def _():
                with jax.named_scope("wait_wall"):
                    wait_for(w.at[pl.ds(0, cols)], w_sem.at[n])

            @pl.when((i >= own_from - 1) & (i < steps - 1))
            def _():
                here = own_at((i + 1) // 3, (i + 1) % 3)
                with jax.named_scope("wait_dxr"):
                    wait_for(dxr_hbm.at[here], dx_recv.at[i + 1 - own_from])

                @pl.when(i < own_from + 2)
                def _():
                    wait_for(wide.at[0], dx_send.at[i - 2])

                copy(dxr_hbm.at[here], wide.at[(i + 1) % 3], local.at[GOT_IN + 1 - slot]).start()
                copy(dy_hbm.at[here], res.at[1 - slot], local.at[RES_IN + 1 - slot]).start()

            @pl.when((i >= 3) & (i < own_from))
            def _():
                with jax.named_scope("wait_dxs"):
                    wait_for(wide.at[0], dx_send.at[i - 3])

            @pl.when((i >= own_from + 2) & (i < steps))
            def _():
                wait_for(out16.at[0], local.at[DX_OUT + slot])

            def dot():
                part = pl.ds(pl.multiple_of(n * cols, cols), cols)
                return lax.dot_general(du[q % 2], w[part, :], (((1,), (1,)), ((), ())), preferred_element_type=F32)

            @pl.when(i < own_from)
            def _():
                with jax.named_scope("dx_dot"):
                    wide[i % 3] = dot()
                pltpu.make_async_remote_copy(
                    src_ref=wide.at[i % 3], dst_ref=dxr_hbm.at[own_at(q, n)], send_sem=dx_send.at[i], recv_sem=dx_recv.at[i],
                    device_id=(partner,), device_id_type=MESH).start()

            @pl.when((i >= own_from) & (i < steps))
            def _():
                with jax.named_scope("wait_got"):
                    wait_for(wide.at[0], local.at[GOT_IN + slot])
                    wait_for(res.at[0], local.at[RES_IN + slot])
                with jax.named_scope("dx_dot2"):
                    out16[slot] = (res[slot].astype(F32) + (dot() + wide[i % 3])).astype(BF16)
                copy(out16.at[slot], dx_hbm.at[own_at(q, n)], local.at[DX_OUT + slot]).start()

            pump(i)
            return carry

        lax.fori_loop(0, max(steps, nc + 17), step, 0)
        for slot in range(2):
            wait_for(out16.at[0], local.at[DX_OUT + slot])
        e_wait_out(nc - 1)
        for n in range(nc):
            wait_for(sized[1].at[0], rs_send.at[1, n])
            wait_for(sized[0].at[0], rs_send.at[2, n])

    pl.run_scoped(
        last,
        pltpu.VMEM((width, hidden), BF16), pltpu.VMEM((2, dx_tile, hidden), BF16),
        pltpu.VMEM((3, dx_tile, cols), F32), pltpu.VMEM((2, dx_tile, cols), BF16), pltpu.VMEM((2, dx_tile, cols), BF16),
        pltpu.VMEM((nc - EARLY, 3, 2, rows, fc), BF16), pltpu.VMEM((nc - EARLY, 3, 2, units, cols), BF16),
        pltpu.VMEM((nc, 3, rows, fc), BF16), pltpu.VMEM((nc, 3, units, cols), BF16),
        pltpu.VMEM((12, rows, fc), BF16), pltpu.VMEM((12, units, cols), BF16),
        pltpu.VMEM((3 * rows, fc), BF16), pltpu.VMEM((units, width), BF16))

    def drain(n, carry):
        for s in range(3):
            for i in range(2):
                wait_for(one_array[s].at[n], ag_send.at[i, s, n])
        wait_for(sized[2].at[n], rs_send.at[0, n])
        wait_for(gup_hbm.at[0, 0], gup_recv.at[n])
        return carry

    with jax.named_scope("drain"):
        lax.fori_loop(0, nc, drain, 0)
    wait_for(xr_hbm, pair_send.at[1])
    wait_for(dyr_hbm, pair_send.at[2])


def finish(nc, units, gup, gdown, dx, gup_out, gdown_out, dx_out, v_in, v_out, v_down, v_dx, sem_in, sem_out):
    pieces = v_dx.shape[0]
    rows = v_dx.shape[1]
    copy(gup, v_in, sem_in.at[pieces]).start()
    copy(gdown, v_down, sem_in.at[pieces + 1]).start()
    for i in range(pieces):
        copy(dx.at[pl.ds(i * rows, rows)], v_dx.at[i], sem_in.at[i]).start()
    copy(gup, v_in, sem_in.at[pieces]).wait()
    per = 128 // math.gcd(128, units)
    for first in range(0, CHIPS * CORES * nc, per):
        parts = []
        for u in range(first, first + per):
            d, n = u // nc, u % nc
            r, c = d // CORES, d % CORES
            parts.append(v_in[c, n, :, r * units:(r + 1) * units])
        v_out[:, first * units:(first + per) * units] = jnp.concatenate(parts, axis=1)
    copy(v_out, gup_out, sem_out.at[pieces]).start()
    copy(gdown, v_down, sem_in.at[pieces + 1]).wait()
    copy(v_down, gdown_out, sem_out.at[pieces + 1]).start()
    for i in range(pieces):
        copy(dx.at[pl.ds(i * rows, rows)], v_dx.at[i], sem_in.at[i]).wait()
        copy(v_dx.at[i], dx_out.at[pl.ds(i * rows, rows)], sem_out.at[i]).start()
    copy(v_out, gup_out, sem_out.at[pieces]).wait()
    copy(v_down, gdown_out, sem_out.at[pieces + 1]).wait()
    for i in range(pieces):
        copy(v_dx.at[i], dx_out.at[pl.ds(i * rows, rows)], sem_out.at[i]).wait()


def solution(mesh):
    def device_fn(x_loc, dy_loc, up_loc, down_loc):
        width = x_loc.shape[-1]
        x = x_loc.reshape(-1, width)
        dy = dy_loc.reshape(-1, width)
        tokens = x.shape[0]
        down = down_loc[0]
        half, units_all = up_loc.shape[1], down.shape[0]
        nc = CHUNKS
        units = units_all // nc
        fc = CHIPS * units
        rows, cols = 2 * half // 3, width // 3
        up = up_loc[0]

        def hbm(*shape, dtype=BF16):
            return jax.ShapeDtypeStruct(shape, dtype)

        one, two = (rows, fc), (units, cols)
        outs = [
            hbm(CORES, nc, half, fc), hbm(units_all, width), hbm(tokens, width),
            hbm(tokens, width), hbm(tokens, width),
            *[hbm(nc, 3, blocks, *s) for blocks in (8, 8, 4, 2) for s in (one, two)],
            hbm(nc, 3, *one), hbm(nc, 3, *two), hbm(nc, 3, 2, *one), hbm(nc, 3, 2, *two),
            hbm(nc, 2 * tokens, fc), hbm(tokens, width, dtype=F32),
        ]
        dma = pltpu.SemaphoreType.DMA
        half_steps = 3 * DX_TILES // 2
        got = pl.pallas_call(
            functools.partial(kernel, nc),
            out_shape=outs,
            in_specs=[pl.BlockSpec(memory_space=pl.ANY)] * 4,
            out_specs=[pl.BlockSpec(memory_space=pl.ANY)] * len(outs),
            scratch_shapes=[
                dma((2, 3, nc)), dma((2, 3, nc)), dma((3, nc)), dma((3, nc)), dma((3,)), dma((4,)),
                dma((half_steps,)), dma((half_steps,)), dma((nc,)), dma((nc,)), dma((3,)), dma((13,)),
            ],
            compiler_params=pltpu.CompilerParams(
                collective_id=0, has_side_effects=True, vmem_limit_bytes=VMEM_BYTES),
        )(x, dy, up, down)
        pieces = 8
        g_up, g_down, dx = pl.pallas_call(
            functools.partial(finish, nc, units),
            out_shape=[hbm(half, up.shape[1]), hbm(units_all, width), hbm(tokens, width)],
            in_specs=[pl.BlockSpec(memory_space=pl.ANY)] * 3,
            out_specs=[pl.BlockSpec(memory_space=pl.ANY)] * 3,
            scratch_shapes=[
                pltpu.VMEM((CORES, nc, half, fc), BF16), pltpu.VMEM((half, up.shape[1]), BF16),
                pltpu.VMEM((units_all, width), BF16), pltpu.VMEM((pieces, tokens // pieces, width), BF16),
                dma((pieces + 2,)), dma((pieces + 2,)),
            ],
            compiler_params=pltpu.CompilerParams(vmem_limit_bytes=VMEM_BYTES),
        )(*got[:3])
        return g_up[None], g_down[None], dx.reshape(x_loc.shape)

    return jax.shard_map(
        device_fn, mesh=mesh, in_specs=(P("data"), P("data"), P(None, "data"), P(None, "data")),
        out_specs=(P(None, "data"), P(None, "data"), P("data")), check_vma=False)
```

```python
import functools
import math

import jax
import jax.numpy as jnp
from jax import lax
from jax.experimental import pallas as pl
from jax.experimental.pallas import tpu as pltpu
from jax.sharding import PartitionSpec as P

MESH = pl.DeviceIdType.MESH
F32, BF16 = jnp.float32, jnp.bfloat16
CHIPS, COLOURS, CORES = 8, 3, 2
CHUNKS = 9
VMEM_BYTES = 67_000_000
DX_TILES = 8
UP_TILES = 8
PARTS = 2
UP_IN, X_IN, DY_IN, W1_IN, W2_IN, G1_OUT, G2_OUT, DU_OUT, SUM_IN, SUM_OUT, OWN_0, OWN_1, OWN_2 = range(13)
TILE_IN, GOT_IN, RES_IN, DX_OUT = range(0, 8, 2)
C_IN, D_IN, E_IN, GUP_OUT, GDOWN_OUT = range(8, 13)
EARLY = 4


def copy(src, dst, sem):
    return pltpu.make_async_copy(src, dst, sem)


def wait_for(ref, sem):
    pltpu.make_async_copy(ref, ref, sem).wait()


def gelu_both(u):
    scale = math.sqrt(2.0 / math.pi)
    square = u * u
    th = jnp.tanh(u * (scale + (0.044715 * scale) * square))
    half = 0.5 * th
    cdf = 0.5 + half
    slope = cdf + (u * (0.5 - th * half)) * (scale + (0.134145 * scale) * square)
    return u * cdf, slope


def kernel(nc, x_hbm, dy_hbm, up_hbm, down_hbm,
           gup_hbm, gdown_hbm, dx_hbm,
           xr_hbm, dyr_hbm, a1, a2, p1, p2, ra1, ra2, rb1, rb2, rc1, rc2, cb1, cb2, du_hbm, dxr_hbm,
           ag_send, ag_recv, rs_send, rs_recv, pair_send, pair_recv, dx_send, dx_recv, gup_send, gup_recv, w_sem, local):
    me = lax.axis_index("data")
    core = me % 2
    bits = [(me // 2) % 2, (me // 4) % 2, (me // 8) % 2]
    partner = me + 1 - 2 * core
    near = [me + (2 << d) * (1 - 2 * bits[d]) for d in range(3)]

    tokens, width = x_hbm.shape
    both = 2 * tokens
    *_, rows, fc = a1.shape
    *_, units, cols = a2.shape
    half = up_hbm.shape[0]
    third = half // 3

    def chip(colour, m, order):
        total = 0
        for i in range(3):
            d = (colour + i) % 3
            flipped = (m >> order[i]) & 1
            total = total + (1 << d) * ((1 - bits[d]) if flipped else bits[d])
        return total

    GATHER, REDUCE = (0, 1, 2), (2, 1, 0)

    def up_rows(colour, m, order):
        return pl.ds(pl.multiple_of(chip(colour, m, order) * (3 * rows) + colour * rows, 16), rows)

    def down_rows(colour, m, order):
        return pl.ds(pl.multiple_of(chip(colour, m, order) * units, 16), units)

    def down_cols(colour):
        return pl.ds(colour * cols, cols)

    def ag_start(n, s, arrays=(0, 1)):
        have = 1 << s
        for k in range(COLOURS):
            for i in arrays:
                buf = (a1, a2)[i]
                pltpu.make_async_remote_copy(
                    src_ref=buf.at[n, k, pl.ds(0, have)], dst_ref=buf.at[n, k, pl.ds(have, have)],
                    send_sem=ag_send.at[i, s, n], recv_sem=ag_recv.at[i, s, n],
                    device_id=(near[(k + s) % 3],), device_id_type=MESH).start()

    one_array = (rc1, rb1, ra1)
    sized = (rb1, ra1, p1)

    def ag_wait(n, s, arrays=(0, 1)):
        for i in arrays:
            wait_for(one_array[s].at[n], ag_recv.at[i, s, n])

    def rs_start(n, s, k, src1, src2):
        dst1, dst2 = ((ra1, ra2), (rb1, rb2), (rc1, rc2))[s]
        for src, dst in ((src1, dst1), (src2, dst2)):
            pltpu.make_async_remote_copy(
                src_ref=src, dst_ref=dst.at[n, k], send_sem=rs_send.at[s, n], recv_sem=rs_recv.at[s, n],
                device_id=(near[(k + s) % 3],), device_id_type=MESH).start()

    def rs_wait(n, s):
        wait_for(sized[2 - s].at[n], rs_recv.at[s, n])

    barrier = pltpu.get_barrier_semaphore()
    for other in (partner, *near):
        pl.semaphore_signal(barrier, inc=1, device_id=(other,), device_id_type=MESH)

    def to_partner(src, dst, i):
        pltpu.make_async_remote_copy(
            src_ref=src, dst_ref=dst, send_sem=pair_send.at[i], recv_sem=pair_recv.at[i],
            device_id=(partner,), device_id_type=MESH).start()

    mine = pl.ds(pl.multiple_of(core * tokens, 16), tokens)
    theirs = pl.ds(pl.multiple_of((1 - core) * tokens, 16), tokens)

    def c_load(n, c1, c2, sem):
        with jax.named_scope("wait_rs0"):
            rs_wait(n, 0)
        for i, (b1, b2) in enumerate(((p1, p2), (ra1, ra2))):
            for k in range(COLOURS):
                pair = pl.ds(2 * (3 * i + k), 2)
                copy(b1.at[n, k, pl.ds(2, 2)], c1.at[pair], sem).start()
                copy(b2.at[n, k, pl.ds(2, 2)], c2.at[pair], sem).start()

    def c_sum(c1, c2, to1, to2, sem):
        wait_for(p1.at[0], sem)
        for k in range(COLOURS):
            for j in range(2):
                to1[k, j] = c1[2 * k + j] + c1[2 * k + j + 6]
                to2[k, j] = c2[2 * k + j] + c2[2 * k + j + 6]

    def main(x, dy, w1, w2, ud, at, s1, s2, c1, c2, co1, co2):
        own_down = x.at[pl.ds(0, nc * units)]
        blocks = up_hbm.shape[1] // width
        for b in range(blocks):
            copy(up_hbm.at[:, pl.ds(b * width, width)], x.at[pl.ds(nc * units + b * half, half)], local.at[UP_IN]).start()
        copy(down_hbm, own_down, local.at[X_IN]).start()
        with jax.named_scope("entry"):
            pl.semaphore_wait(barrier, 4)
        for k in range(COLOURS):
            pltpu.make_async_remote_copy(
                src_ref=down_hbm.at[pl.ds(0, units), down_cols(k)], dst_ref=a2.at[0, k, 1],
                send_sem=ag_send.at[1, 0, 0], recv_sem=ag_recv.at[1, 0, 0],
                device_id=(near[k],), device_id_type=MESH).start()
        wait_for(up_hbm, local.at[UP_IN])

        def unit(chip_, core_, n):
            first = ((chip_ * CORES + core_) * nc + n) * units
            b, c = first // width, first % width
            return x[nc * units + b * half:nc * units + (b + 1) * half, c:c + units]

        whole = pl.ds(pl.multiple_of(core * third, 16), 2 * third)
        rest = pl.ds(pl.multiple_of((1 - core) * 2 * third, 16), third)
        to_rest = pl.ds(pl.multiple_of(core * third, 16), third)

        def permute(n):
            for c in range(CORES):
                first = (n * CORES + c) * half
                ud[first:first + half, :] = jnp.concatenate([unit(r, c, n) for r in range(CHIPS)], axis=1)

        def own_up(n):
            def part(c, which):
                return ud.at[pl.ds(pl.multiple_of((n * CORES + c) * half + which.start, 16), which.size)]

            sem = min(n, 1)
            for which, dst in ((whole, a1.at[n, 2 * core, 0]), (rest, a1.at[n, 1, 0, to_rest])):
                pltpu.make_async_remote_copy(
                    src_ref=part(1 - core, which), dst_ref=dst, send_sem=pair_send.at[0], recv_sem=pair_recv.at[3 * sem],
                    device_id=(partner,), device_id_type=MESH).start()
                copy(part(core, which), dst, local.at[OWN_0 + sem]).start()

        def down_own(n):
            for k in range(COLOURS):
                copy(x.at[pl.ds(n * units, units), down_cols(k)], a2.at[n, k, 0], local.at[OWN_2 if n else X_IN]).start()

        permute(0)
        own_up(0)
        wait_for(down_hbm, local.at[X_IN])
        for n in range(nc):
            down_own(n)
        for n in range(1, 4):
            permute(n)
        with jax.named_scope("own_wait"):
            wait_for(du_hbm.at[0, pl.ds(0, half)], local.at[OWN_0])
            wait_for(du_hbm.at[0, pl.ds(0, half)], pair_recv.at[0])
        ag_start(0, 0, (0,))
        for n in range(4, nc):
            permute(n)
        for n in range(1, nc):
            own_up(n)
        to_partner(x_hbm, xr_hbm, 1)
        to_partner(dy_hbm, dyr_hbm, 2)
        wait_for(down_hbm.at[pl.ds(0, units)], local.at[X_IN])
        wait_for(down_hbm.at[pl.ds(0, (nc - 1) * units)], local.at[OWN_2])
        ag_start(1, 0, (1,))
        copy(x_hbm, x.at[mine], local.at[X_IN]).start()
        copy(dy_hbm, dy.at[mine], local.at[DY_IN]).start()
        def load_up(n, blocks=range(CHIPS)):
            for k in range(COLOURS):
                for m in blocks:
                    copy(a1.at[n, k, m], w1.at[up_rows(k, m, GATHER)], local.at[W1_IN]).start()

        for s in range(2):
            for i in range(2):
                with jax.named_scope(f"ag0{s}{i}"):
                    ag_wait(0, s, (i,))
                ag_start(0, s + 1, (i,))
        wait_for(du_hbm.at[0, pl.ds(0, (nc - 1) * half)], local.at[OWN_1])
        wait_for(du_hbm.at[0, pl.ds(0, (nc - 1) * half)], pair_recv.at[3])
        ag_start(1, 0, (0,))
        ag_start(2, 0)
        with jax.named_scope("xr"):
            wait_for(xr_hbm, pair_recv.at[1])
        copy(xr_hbm, x.at[theirs], local.at[X_IN]).start()
        load_up(0, range(4))

        def load_down(n):
            for k in range(COLOURS):
                for m in range(CHIPS):
                    copy(a2.at[n, k, m], w2.at[down_rows(k, m, GATHER), down_cols(k)], local.at[W2_IN]).start()

        with jax.named_scope("ag020"):
            ag_wait(0, 2, (0,))
        load_up(0, range(4, CHIPS))
        with jax.named_scope("tokens"):
            wait_for(x, local.at[X_IN])
            wait_for(du_hbm.at[0, pl.ds(0, nc * half)], pair_send.at[0])

        def send_first(src, dst, n):
            for k in range(COLOURS):
                pltpu.make_async_remote_copy(
                    src_ref=src.at[n, k, pl.ds(4, 4)], dst_ref=dst.at[n, k], send_sem=rs_send.at[0, n],
                    recv_sem=rs_recv.at[0, n], device_id=(near[k],), device_id_type=MESH).start()

        def send_down(n):
            wait_for(p1.at[0], local.at[G1_OUT])
            wait_for(p2.at[0], local.at[G2_OUT])
            send_first(p2, ra2, n)

        def c_in(n):
            c_load(n, c1, c2, local.at[SUM_IN])

        def c_add(n):
            c_sum(c1, c2, co1, co2, local.at[SUM_IN])
            copy(co1, cb1.at[n], local.at[SUM_OUT]).start()
            copy(co2, cb2.at[n], local.at[SUM_OUT]).start()

        def c_go(n):
            wait_for(sized[1].at[0], local.at[SUM_OUT])
            for k in range(COLOURS):
                rs_start(n, 1, k, cb1.at[n, k], cb2.at[n, k])

        def early(slot):
            if slot > 1:
                c_go(slot - 2)
            if 0 < slot <= EARLY:
                c_add(slot - 1)
            if slot < EARLY:
                c_in(slot)

        up_tile = both // UP_TILES

        def chunk(n, carry):
            size = up_tile // PARTS
            strip = min(128, size)

            def use(first, u, da):
                for c in range(0, fc, 128):
                    lanes = slice(c, c + 128)
                    for r in range(0, size, strip):
                        at_r = pl.ds(pl.multiple_of(first + r, strip), strip)
                        a, slope = gelu_both(u(r, at_r, lanes).astype(F32))
                        ud[at_r, lanes] = (da[r:r + strip, lanes] * slope).astype(BF16)
                        at[lanes, at_r] = a.astype(BF16).T

            def da_of(at_t):
                return lax.dot_general(dy[at_t, :], w2[...], (((1,), (1,)), ((), ())), preferred_element_type=F32)

            with jax.named_scope("wait_w1"):
                wait_for(w1, local.at[W1_IN])

            @pl.when(n == 0)
            def _():
                def u_step(t, carry):
                    at_t = pl.ds(pl.multiple_of(t * 2 * up_tile, up_tile), 2 * up_tile)
                    ud[at_t, :] = jnp.dot(x[at_t, :], w1[...], preferred_element_type=F32).astype(BF16)

                    @pl.when(t == 1)
                    def _():
                        with jax.named_scope("dyr"):
                            wait_for(dyr_hbm, pair_recv.at[2])
                        copy(dyr_hbm, dy.at[theirs], local.at[DY_IN]).start()

                    @pl.when(t == 2)
                    def _():
                        with jax.named_scope("ag021"):
                            ag_wait(0, 2, (1,))
                        load_down(0)

                    return carry

                with jax.named_scope("u0"):
                    lax.fori_loop(0, UP_TILES // 2, u_step, 0)
                with jax.named_scope("wait_100"):
                    ag_wait(1, 0, (0,))
                ag_start(1, 1, (0,))
                with jax.named_scope("first_w2"):
                    wait_for(dy, local.at[DY_IN])
                    wait_for(w2, local.at[W2_IN])

                def da_step(t, carry):
                    for part in range(PARTS):
                        first = t * up_tile + part * size
                        da = da_of(pl.ds(pl.multiple_of(first, size), size))
                        use(first, lambda r, at_r, lanes: ud[at_r, lanes], da)

                    for when, s, i in ((0, 0, 1), (3, 1, 0), (6, 1, 1)):
                        @pl.when(t == when)
                        def _(s=s, i=i):
                            with jax.named_scope(f"wait_1{s}{i}"):
                                ag_wait(1, s, (i,))
                            ag_start(1, s + 1, (i,))

                    return carry

                with jax.named_scope("da0"):
                    lax.fori_loop(0, UP_TILES, da_step, 0)
                with jax.named_scope("wait_20"):
                    ag_wait(2, 0)
                ag_start(2, 1)
                ag_start(3, 0)

            def up_step(t, carry):
                for part in range(PARTS):
                    first = t * up_tile + part * size
                    at_t = pl.ds(pl.multiple_of(first, size), size)
                    u = jnp.dot(x[at_t, :], w1[...], preferred_element_type=F32).astype(BF16)
                    da = da_of(at_t)
                    use(first, lambda r, at_r, lanes, u=u: u[r:r + strip, lanes], da)

                @pl.when((t == 2) & (n == 1))
                def _():
                    with jax.named_scope("wait_30"):
                        ag_wait(3, 0)
                    ag_start(3, 1)
                    ag_start(4, 0)

                @pl.when(t == 2)
                def _():
                    send_down(n - 1)

                    @pl.when(n > nc - 4)
                    def _():
                        send_first(p1, ra1, n - 1)

                    @pl.when((n > 2) & (n < nc - 1))
                    def _():
                        send_first(p1, ra1, n - 3)

                @pl.when((t == 6) & (n == nc - 2))
                def _():
                    early(0)

                @pl.when((t == 6) & (n == nc - 1))
                def _():
                    early(3)

                return carry

            @pl.when(n > 0)
            def _():
                with jax.named_scope("wait_w2"):
                    wait_for(w2, local.at[W2_IN])
                with jax.named_scope("up"):
                    lax.fori_loop(0, UP_TILES, up_step, 0)

            copy(ud, du_hbm.at[n], local.at[DU_OUT]).start()

            @pl.when(n == nc - 1)
            def _():
                early(4)

            def down_grad(k, carry):
                part = pl.ds(pl.multiple_of(k * cols, cols), cols)
                s2[:, part] = jnp.dot(at[...], dy[:, part], preferred_element_type=F32).astype(BF16)
                return carry

            with jax.named_scope("down_grad"):
                lax.fori_loop(0, 3, down_grad, 0)
            for k in range(COLOURS):
                for m in range(CHIPS):
                    copy(s2.at[down_rows(k, m, REDUCE), down_cols(k)], p2.at[n, k, m], local.at[G2_OUT]).start()

            @pl.when((n > 0) & (n + 2 < nc))
            def _():
                with jax.named_scope("wait_ag1"):
                    ag_wait(n + 2, 1)
                ag_start(n + 2, 2)

            @pl.when((n > 0) & (n + 3 < nc))
            def _():
                with jax.named_scope("wait_ag0"):
                    ag_wait(n + 3, 0)
                ag_start(n + 3, 1)

            @pl.when((n > 0) & (n + 4 < nc))
            def _():
                ag_start(n + 4, 0)

            @pl.when(n == nc - 2)
            def _():
                early(1)

            @pl.when(n == nc - 1)
            def _():
                early(5)

            def up_grad(k, carry):
                part = pl.ds(pl.multiple_of(k * cols, cols), cols)

                @pl.when((k == 2) & (n + 1 < nc))
                def _():
                    with jax.named_scope("wait_ag2"):
                        ag_wait(n + 1, 2)
                    load_up(n + 1)
                    load_down(n + 1)

                s1[part, :] = lax.dot_general(
                    x[:, part], ud[...], (((0,), (0,)), ((), ())), preferred_element_type=F32).astype(BF16)
                return carry

            with jax.named_scope("up_grad"):
                lax.fori_loop(0, 3, up_grad, 0)
            for k in range(COLOURS):
                for m in range(CHIPS):
                    copy(s1.at[up_rows(k, m, REDUCE)], p1.at[n, k, m], local.at[G1_OUT]).start()

            @pl.when(n == 0)
            def _():
                with jax.named_scope("wait_21"):
                    ag_wait(2, 1)
                ag_start(2, 2)

            @pl.when(n == nc - 2)
            def _():
                early(2)

            wait_for(ud, local.at[DU_OUT])
            return carry

        lax.fori_loop(0, nc, chunk, 0)
        send_down(nc - 1)
        send_first(p1, ra1, nc - 1)

    pl.run_scoped(
        main,
        pltpu.VMEM((both, width), BF16), pltpu.VMEM((both, width), BF16),
        pltpu.VMEM((width, fc), BF16), pltpu.VMEM((fc, width), BF16),
        pltpu.VMEM((both, fc), BF16), pltpu.VMEM((fc, both), BF16),
        pltpu.VMEM((width, fc), BF16), pltpu.VMEM((fc, width), BF16),
        pltpu.VMEM((12, rows, fc), BF16), pltpu.VMEM((12, units, cols), BF16),
        pltpu.VMEM((3, 2, rows, fc), BF16), pltpu.VMEM((3, 2, units, cols), BF16))

    dx_tile = both // DX_TILES
    half_tiles = DX_TILES // 2
    steps = 3 * DX_TILES
    own_from = 3 * half_tiles
    hidden = nc * fc

    def last(w, du, wide, out16, res,
             co1, co2, do1, do2, e1, e2, eo1, eo2):
        def load_w(n, third_):
            for p in range(CHIPS):
                piece = CHIPS * third_ + p
                r, k = divmod(piece, COLOURS)
                m = 0
                for i in range(3):
                    d = (k + i) % 3
                    m = m + (1 << i) * ((1 - bits[d]) if (r >> d) & 1 else bits[d])
                copy(a1.at[n, k, m], w.at[pl.ds(piece * rows, rows), pl.ds(pl.multiple_of(n * fc, fc), fc)],
                     w_sem.at[third_]).start()

        def tokens_at(q):
            later = q // half_tiles
            owner = (1 - later) * (1 - core) + later * core
            return pl.multiple_of(owner * tokens + (q % half_tiles) * dx_tile, dx_tile)

        def load_du(q):
            slot = q % 2
            for n in range(nc):
                copy(du_hbm.at[n, pl.ds(tokens_at(q), dx_tile)], du.at[slot, :, pl.ds(n * fc, fc)], local.at[TILE_IN + slot]).start()

        for third_ in range(COLOURS):
            lax.fori_loop(0, nc, lambda n, carry, third_=third_: (load_w(n, third_), carry)[1], 0)
            if third_ == 0:
                load_du(0)

        def own_at(q, n):
            return (pl.ds(pl.multiple_of((q % half_tiles) * dx_tile, dx_tile), dx_tile), pl.ds(pl.multiple_of(n * cols, cols), cols))

        def c_in(n):
            c_load(n, e1, e2, local.at[C_IN])

        def c_send(n):
            to1, to2 = co1.at[n - EARLY], co2.at[n - EARLY]
            c_sum(e1, e2, to1, to2, local.at[C_IN])
            for k in range(COLOURS):
                rs_start(n, 1, k, to1.at[k], to2.at[k])

        def sum_of(e, k, terms):
            total = e[k].astype(F32)
            for i in range(1, terms):
                total = total + e[3 * i + k].astype(F32)
            return total.astype(BF16)

        def d_load(n):
            with jax.named_scope("wait_rs1"):
                rs_wait(n, 1)
            for i, (b1, b2) in enumerate(((p1, p2), (ra1, ra2), (rb1, rb2))):
                for k in range(COLOURS):
                    copy(b1.at[n, k, 1], e1.at[3 * i + k], local.at[D_IN]).start()
                    copy(b2.at[n, k, 1], e2.at[3 * i + k], local.at[D_IN]).start()

        def d_send(n):
            wait_for(e1.at[pl.ds(0, 9)], local.at[D_IN])
            wait_for(e2.at[pl.ds(0, 9)], local.at[D_IN])

            for k in range(COLOURS):
                do1[n, k] = sum_of(e1, k, 3)
                do2[n, k] = sum_of(e2, k, 3)
                rs_start(n, 2, k, do1.at[n, k], do2.at[n, k])

        def e_load(n):
            for i, (b1, b2) in enumerate(((p1, p2), (ra1, ra2), (rb1, rb2))):
                for k in range(COLOURS):
                    copy(b1.at[n, k, 0], e1.at[3 * i + k], local.at[E_IN]).start()
                    copy(b2.at[n, k, 0], e2.at[3 * i + k], local.at[E_IN]).start()
            with jax.named_scope("wait_rs2"):
                rs_wait(n, 2)
            copy(rc1.at[n], e1.at[pl.ds(9, 3)], local.at[E_IN]).start()
            copy(rc2.at[n], e2.at[pl.ds(9, 3)], local.at[E_IN]).start()

        keep = pl.ds(pl.multiple_of(core * half, 16), half)
        give = pl.ds(pl.multiple_of((1 - core) * half, 16), half)

        def e_wait_out(n):
            wait_for(gup_hbm.at[0, 0], local.at[GUP_OUT])
            wait_for(gdown_hbm.at[pl.ds(0, units)], local.at[GDOWN_OUT])
            wait_for(gup_hbm.at[0, 0], gup_send.at[n])

        def e_store(n):
            wait_for(e1, local.at[E_IN])
            wait_for(e2, local.at[E_IN])

            @pl.when(n > 0)
            def _():
                e_wait_out(n - 1)

            for k in range(COLOURS):
                eo1[k * rows:(k + 1) * rows, :] = sum_of(e1, k, 4)
                eo2[:, k * cols:(k + 1) * cols] = sum_of(e2, k, 4)
            copy(eo1.at[keep], gup_hbm.at[core, n], local.at[GUP_OUT]).start()
            copy(eo2, gdown_hbm.at[pl.ds(pl.multiple_of(n * units, 16), units)], local.at[GDOWN_OUT]).start()
            pltpu.make_async_remote_copy(
                src_ref=eo1.at[give], dst_ref=gup_hbm.at[core, n], send_sem=gup_send.at[n], recv_sem=gup_recv.at[n],
                device_id=(partner,), device_id_type=MESH).start()

        def pump(i):
            for start, low, high, load, finish_ in (
                    (0, EARLY, nc - 1, c_in, c_send), (6, nc - 1, nc, c_in, c_send), (7, 0, nc, d_load, d_send), (16, 0, nc, e_load, e_store)):
                n = i - start + low

                @pl.when((n > low) & (n <= high))
                def _(finish_=finish_, n=n):
                    finish_(n - 1)

                @pl.when((n >= low) & (n < high))
                def _(load=load, n=n):
                    load(n)

        def step(i, carry):
            q, n = i // 3, i % 3
            slot = i % 2

            @pl.when((i < steps) & (n == 0))
            def _():
                @pl.when(q + 1 < DX_TILES)
                def _():
                    load_du(q + 1)

                with jax.named_scope("wait_du"):
                    wait_for(du.at[0], local.at[TILE_IN + q % 2])

            @pl.when(i < 3)
            def _():
                with jax.named_scope("wait_wall"):
                    wait_for(w.at[pl.ds(0, cols)], w_sem.at[n])

            @pl.when((i >= own_from - 1) & (i < steps - 1))
            def _():
                here = own_at((i + 1) // 3, (i + 1) % 3)
                with jax.named_scope("wait_dxr"):
                    wait_for(dxr_hbm.at[here], dx_recv.at[i + 1 - own_from])

                @pl.when(i < own_from + 2)
                def _():
                    wait_for(wide.at[0], dx_send.at[i - 2])

                copy(dxr_hbm.at[here], wide.at[(i + 1) % 3], local.at[GOT_IN + 1 - slot]).start()
                copy(dy_hbm.at[here], res.at[1 - slot], local.at[RES_IN + 1 - slot]).start()

            @pl.when((i >= 3) & (i < own_from))
            def _():
                with jax.named_scope("wait_dxs"):
                    wait_for(wide.at[0], dx_send.at[i - 3])

            @pl.when((i >= own_from + 2) & (i < steps))
            def _():
                wait_for(out16.at[0], local.at[DX_OUT + slot])

            def dot():
                part = pl.ds(pl.multiple_of(n * cols, cols), cols)
                return lax.dot_general(du[q % 2], w[part, :], (((1,), (1,)), ((), ())), preferred_element_type=F32)

            @pl.when(i < own_from)
            def _():
                with jax.named_scope("dx_dot"):
                    wide[i % 3] = dot()
                pltpu.make_async_remote_copy(
                    src_ref=wide.at[i % 3], dst_ref=dxr_hbm.at[own_at(q, n)], send_sem=dx_send.at[i], recv_sem=dx_recv.at[i],
                    device_id=(partner,), device_id_type=MESH).start()

            @pl.when((i >= own_from) & (i < steps))
            def _():
                with jax.named_scope("wait_got"):
                    wait_for(wide.at[0], local.at[GOT_IN + slot])
                    wait_for(res.at[0], local.at[RES_IN + slot])
                with jax.named_scope("dx_dot2"):
                    out16[slot] = (res[slot].astype(F32) + (dot() + wide[i % 3])).astype(BF16)
                copy(out16.at[slot], dx_hbm.at[own_at(q, n)], local.at[DX_OUT + slot]).start()

            pump(i)
            return carry

        lax.fori_loop(0, max(steps, nc + 17), step, 0)
        for slot in range(2):
            wait_for(out16.at[0], local.at[DX_OUT + slot])
        e_wait_out(nc - 1)
        for n in range(nc):
            wait_for(sized[1].at[0], rs_send.at[1, n])
            wait_for(sized[0].at[0], rs_send.at[2, n])

    pl.run_scoped(
        last,
        pltpu.VMEM((width, hidden), BF16), pltpu.VMEM((2, dx_tile, hidden), BF16),
        pltpu.VMEM((3, dx_tile, cols), F32), pltpu.VMEM((2, dx_tile, cols), BF16), pltpu.VMEM((2, dx_tile, cols), BF16),
        pltpu.VMEM((nc - EARLY, 3, 2, rows, fc), BF16), pltpu.VMEM((nc - EARLY, 3, 2, units, cols), BF16),
        pltpu.VMEM((nc, 3, rows, fc), BF16), pltpu.VMEM((nc, 3, units, cols), BF16),
        pltpu.VMEM((12, rows, fc), BF16), pltpu.VMEM((12, units, cols), BF16),
        pltpu.VMEM((3 * rows, fc), BF16), pltpu.VMEM((units, width), BF16))

    def drain(n, carry):
        for s in range(3):
            for i in range(2):
                wait_for(one_array[s].at[n], ag_send.at[i, s, n])
        wait_for(sized[2].at[n], rs_send.at[0, n])
        wait_for(gup_hbm.at[0, 0], gup_recv.at[n])
        return carry

    with jax.named_scope("drain"):
        lax.fori_loop(0, nc, drain, 0)
    wait_for(xr_hbm, pair_send.at[1])
    wait_for(dyr_hbm, pair_send.at[2])


def finish(nc, units, gup, gdown, dx, gup_out, gdown_out, dx_out, v_in, v_out, v_down, v_dx, sem_in, sem_out):
    pieces = v_dx.shape[0]
    rows = v_dx.shape[1]
    copy(gup, v_in, sem_in.at[pieces]).start()
    copy(gdown, v_down, sem_in.at[pieces + 1]).start()
    for i in range(pieces):
        copy(dx.at[pl.ds(i * rows, rows)], v_dx.at[i], sem_in.at[i]).start()
    copy(gup, v_in, sem_in.at[pieces]).wait()
    per = 128 // math.gcd(128, units)
    for first in range(0, CHIPS * CORES * nc, per):
        parts = []
        for u in range(first, first + per):
            d, n = u // nc, u % nc
            r, c = d // CORES, d % CORES
            parts.append(v_in[c, n, :, r * units:(r + 1) * units])
        v_out[:, first * units:(first + per) * units] = jnp.concatenate(parts, axis=1)
    copy(v_out, gup_out, sem_out.at[pieces]).start()
    copy(gdown, v_down, sem_in.at[pieces + 1]).wait()
    copy(v_down, gdown_out, sem_out.at[pieces + 1]).start()
    for i in range(pieces):
        copy(dx.at[pl.ds(i * rows, rows)], v_dx.at[i], sem_in.at[i]).wait()
        copy(v_dx.at[i], dx_out.at[pl.ds(i * rows, rows)], sem_out.at[i]).start()
    copy(v_out, gup_out, sem_out.at[pieces]).wait()
    copy(v_down, gdown_out, sem_out.at[pieces + 1]).wait()
    for i in range(pieces):
        copy(v_dx.at[i], dx_out.at[pl.ds(i * rows, rows)], sem_out.at[i]).wait()


def solution(mesh):
    def device_fn(x_loc, dy_loc, up_loc, down_loc):
        width = x_loc.shape[-1]
        x = x_loc.reshape(-1, width)
        dy = dy_loc.reshape(-1, width)
        tokens = x.shape[0]
        down = down_loc[0]
        half, units_all = up_loc.shape[1], down.shape[0]
        nc = CHUNKS
        units = units_all // nc
        fc = CHIPS * units
        rows, cols = 2 * half // 3, width // 3
        up = up_loc[0]

        def hbm(*shape, dtype=BF16):
            return jax.ShapeDtypeStruct(shape, dtype)

        one, two = (rows, fc), (units, cols)
        outs = [
            hbm(CORES, nc, half, fc), hbm(units_all, width), hbm(tokens, width),
            hbm(tokens, width), hbm(tokens, width),
            *[hbm(nc, 3, blocks, *s) for blocks in (8, 8, 4, 2) for s in (one, two)],
            hbm(nc, 3, *one), hbm(nc, 3, *two), hbm(nc, 3, 2, *one), hbm(nc, 3, 2, *two),
            hbm(nc, 2 * tokens, fc), hbm(tokens, width, dtype=F32),
        ]
        dma = pltpu.SemaphoreType.DMA
        half_steps = 3 * DX_TILES // 2
        got = pl.pallas_call(
            functools.partial(kernel, nc),
            out_shape=outs,
            in_specs=[pl.BlockSpec(memory_space=pl.ANY)] * 4,
            out_specs=[pl.BlockSpec(memory_space=pl.ANY)] * len(outs),
            scratch_shapes=[
                dma((2, 3, nc)), dma((2, 3, nc)), dma((3, nc)), dma((3, nc)), dma((3,)), dma((4,)),
                dma((half_steps,)), dma((half_steps,)), dma((nc,)), dma((nc,)), dma((3,)), dma((13,)),
            ],
            compiler_params=pltpu.CompilerParams(
                collective_id=0, has_side_effects=True, vmem_limit_bytes=VMEM_BYTES),
        )(x, dy, up, down)
        pieces = 16
        g_up, g_down, dx = pl.pallas_call(
            functools.partial(finish, nc, units),
            out_shape=[hbm(half, up.shape[1]), hbm(units_all, width), hbm(tokens, width)],
            in_specs=[pl.BlockSpec(memory_space=pl.ANY)] * 3,
            out_specs=[pl.BlockSpec(memory_space=pl.ANY)] * 3,
            scratch_shapes=[
                pltpu.VMEM((CORES, nc, half, fc), BF16), pltpu.VMEM((half, up.shape[1]), BF16),
                pltpu.VMEM((units_all, width), BF16), pltpu.VMEM((pieces, tokens // pieces, width), BF16),
                dma((pieces + 2,)), dma((pieces + 2,)),
            ],
            compiler_params=pltpu.CompilerParams(vmem_limit_bytes=VMEM_BYTES),
        )(*got[:3])
        return g_up[None], g_down[None], dx.reshape(x_loc.shape)

    return jax.shard_map(
        device_fn, mesh=mesh, in_specs=(P("data"), P("data"), P(None, "data"), P(None, "data")),
        out_specs=(P(None, "data"), P(None, "data"), P("data")), check_vma=False)
```
